16 devices in a mesh: dp: 4 (over z, y), sp: 4 (over x, core).
Axes of the slice: x: 2, y: 2, z: 2, core: 2. Of those that a mesh axis runs over, the one named last changes fastest.
Arguments:
- patches: bfloat16 [8, 3072, 1536], P('dp', 'sp'), parts along dimension 0
- vis_mask: int32 [8, 3072], P('dp', 'sp'), parts along dimension 0
- enc_pos: bfloat16 [12288, 768], P(('dp', 'sp')), parts along dimension 0
- dec_pos: bfloat16 [12288, 384], P(('dp', 'sp')), parts along dimension 0
- w_pe: bfloat16 [1536, 768], replicated
- b_pe: bfloat16 [768], replicated
- enc_qkv: bfloat16 [2, 768, 3, 12, 64], replicated
- enc_proj: bfloat16 [2, 12, 64, 768], replicated
- enc_up: bfloat16 [2, 768, 3072], replicated
- enc_down: bfloat16 [2, 3072, 768], replicated
- w_ed: bfloat16 [768, 384], replicated
- mask_token: bfloat16 [384], replicated
- dec_qkv: bfloat16 [2, 384, 3, 6, 64], replicated
- dec_proj: bfloat16 [2, 6, 64, 384], replicated
- dec_up: bfloat16 [2, 384, 1536], replicated
- dec_down: bfloat16 [2, 1536, 384], replicated
- w_out: bfloat16 [384, 1536], replicated
Outputs:
- output: float32 [8, 3072, 1536], P('dp', 'sp'), parts along dimension 0
There are 4 independent parts. The reference program is written for one: setup_inputs(seed, part) draws one part's arguments, and reference() takes and returns one part's arrays. A program takes and returns all parts, laid end to end along the dimension named above; an argument that names none is the same for every part.
All inputs are finite; a program needn't handle non-finite values.
Results may differ from the reference program's by a relative error of at most 0.0157076.
Values are sent between devices in bfloat16 or wider.
A program may use at most 1 GiB of HBM per device.

```python
import jax
import jax.numpy as jnp
from jax import lax

P = 1536
D = 768
ENC_HEADS = 12
DD = 384
DEC_HEADS = 6
TOK_DEV = 768
SP = 4
KEEP_DIV = 8
CLIPS = 2
LAYERS = 2

SEQ = TOK_DEV * SP
VIS_SHARD = TOK_DEV // KEEP_DIV
VIS_ALL = VIS_SHARD * SP
ENC_HD = D // ENC_HEADS
DEC_HD = DD // DEC_HEADS


def shard_ranks(key):
    return jax.random.permutation(key, TOK_DEV)


def draw_mask(key):
    half_shard = VIS_SHARD // 2
    key_shift, key_pick, key_perm = jax.random.split(key, 3)
    inner_shift = jax.random.randint(key_shift, (CLIPS, SP - 1), -half_shard, half_shard + 1)
    pick_at = jax.random.randint(key_pick, (CLIPS, 1), 1, SP - 2)
    shard_idx = jnp.arange(1, SP)[None, :]
    inner_shift = jnp.where(shard_idx == pick_at, half_shard, inner_shift)
    inner_shift = jnp.where(shard_idx == pick_at + 1, -half_shard, inner_shift)
    inner_shift = jnp.where(shard_idx == pick_at + 2, half_shard, inner_shift)
    edge_zero = jnp.zeros((CLIPS, 1), jnp.int32)
    shift_all = jnp.concatenate([edge_zero, inner_shift, edge_zero], axis=1)
    shard_counts = VIS_SHARD + shift_all[:, 1:] - shift_all[:, :-1]
    tok_ranks = jax.vmap(shard_ranks)(jax.random.split(key_perm, CLIPS * SP))
    tok_ranks = tok_ranks.reshape(CLIPS, SP, TOK_DEV)
    return (tok_ranks < shard_counts[:, :, None]).astype(jnp.int32).reshape(CLIPS, SEQ)


def draw_normal(key, shape, scale):
    return (scale * jax.random.normal(key, shape, jnp.float32)).astype(jnp.bfloat16)


def setup_inputs(seed: int = 0, part: int = 0) -> dict:
    key_shared, key_local = jax.random.split(jax.random.key(seed))
    part_keys = jax.random.split(jax.random.fold_in(key_local, part), 4)
    weight_keys = jax.random.split(key_shared, 13)
    return {
        'patches': draw_normal(part_keys[0], (CLIPS, SEQ, P), 1.0),
        'vis_mask': draw_mask(part_keys[1]),
        'enc_pos': draw_normal(part_keys[2], (SEQ, D), 0.5),
        'dec_pos': draw_normal(part_keys[3], (SEQ, DD), 0.5),
        'w_pe': draw_normal(weight_keys[0], (P, D), P ** -0.5),
        'b_pe': draw_normal(weight_keys[1], (D,), 0.5),
        'enc_qkv': draw_normal(weight_keys[2], (LAYERS, D, 3, ENC_HEADS, ENC_HD), 1.5 * D ** -0.5),
        'enc_proj': draw_normal(weight_keys[3], (LAYERS, ENC_HEADS, ENC_HD, D), D ** -0.5),
        'enc_up': draw_normal(weight_keys[4], (LAYERS, D, 4 * D), D ** -0.5),
        'enc_down': draw_normal(weight_keys[5], (LAYERS, 4 * D, D), (4 * D) ** -0.5),
        'w_ed': draw_normal(weight_keys[6], (D, DD), D ** -0.5),
        'mask_token': draw_normal(weight_keys[7], (DD,), 1.0),
        'dec_qkv': draw_normal(weight_keys[8], (LAYERS, DD, 3, DEC_HEADS, DEC_HD), 1.5 * DD ** -0.5),
        'dec_proj': draw_normal(weight_keys[9], (LAYERS, DEC_HEADS, DEC_HD, DD), DD ** -0.5),
        'dec_up': draw_normal(weight_keys[10], (LAYERS, DD, 4 * DD), DD ** -0.5),
        'dec_down': draw_normal(weight_keys[11], (LAYERS, 4 * DD, DD), (4 * DD) ** -0.5),
        'w_out': draw_normal(weight_keys[12], (DD, P), DD ** -0.5),
    }


def layer_norm(hidden):
    hid_f32 = hidden.astype(jnp.float32)
    centred = hid_f32 - jnp.mean(hid_f32, axis=-1, keepdims=True)
    row_var = jnp.mean(centred * centred, axis=-1, keepdims=True)
    return (centred * lax.rsqrt(row_var + 1e-6)).astype(jnp.bfloat16)


def attend(queries, key_rows, value_rows):
    q_rows, n_heads, head_dim = queries.shape
    keys_f32 = key_rows.astype(jnp.float32)
    values_f32 = value_rows.astype(jnp.float32)

    def one_block(q_block):
        scores = jnp.einsum('qhk,shk->hqs', q_block.astype(jnp.float32), keys_f32) * head_dim ** -0.5
        attn_probs = jax.nn.softmax(scores, axis=-1).astype(jnp.bfloat16)
        return jnp.einsum('hqs,shk->qhk', attn_probs.astype(jnp.float32), values_f32).astype(jnp.bfloat16)

    q_blocks = queries.reshape(SP, q_rows // SP, n_heads, head_dim)
    return lax.map(one_block, q_blocks).reshape(q_rows, n_heads, head_dim)


def block(hidden, w_qkv, w_proj, w_up, w_down):
    proj_qkv = jnp.einsum('nd,dshk->snhk', layer_norm(hidden).astype(jnp.float32), w_qkv.astype(jnp.float32)).astype(jnp.bfloat16)
    attended = attend(proj_qkv[0], proj_qkv[1], proj_qkv[2])
    att_out = jnp.einsum('nhk,hkd->nd', attended.astype(jnp.float32), w_proj.astype(jnp.float32))
    mid_state = (hidden.astype(jnp.float32) + att_out).astype(jnp.bfloat16)
    up_act = jax.nn.gelu(jnp.dot(layer_norm(mid_state), w_up, preferred_element_type=jnp.float32), approximate=False).astype(jnp.bfloat16)
    return (mid_state.astype(jnp.float32) + jnp.dot(up_act, w_down, preferred_element_type=jnp.float32)).astype(jnp.bfloat16)


def run_stack(hidden, w_qkv, w_proj, w_up, w_down):
    def body(carry, layer_w):
        return block(carry, layer_w[0], layer_w[1], layer_w[2], layer_w[3]), None

    final_state, unused = lax.scan(body, hidden, (w_qkv, w_proj, w_up, w_down))
    return final_state


def reference(patches, vis_mask, enc_pos, dec_pos, w_pe, b_pe, enc_qkv, enc_proj, enc_up, enc_down, w_ed, mask_token, dec_qkv, dec_proj, dec_up, dec_down, w_out):
    def one_clip(clip_in):
        clip_patches, visible = clip_in
        vis_idx = jnp.nonzero(visible, size=VIS_ALL)[0]
        embedded = (jnp.dot(clip_patches[vis_idx], w_pe, preferred_element_type=jnp.float32)
                    + b_pe.astype(jnp.float32) + enc_pos[vis_idx].astype(jnp.float32)).astype(jnp.bfloat16)
        encoded = run_stack(embedded, enc_qkv, enc_proj, enc_up, enc_down)
        z_vis = jnp.dot(layer_norm(encoded), w_ed, preferred_element_type=jnp.float32).astype(jnp.bfloat16)
        vis_rank = jnp.clip(jnp.cumsum(visible) - visible, 0, VIS_ALL - 1)
        dec_tok = jnp.where(visible[:, None] == 1, z_vis[vis_rank], mask_token[None, :])
        dec_in = (dec_tok.astype(jnp.float32) + dec_pos.astype(jnp.float32)).astype(jnp.bfloat16)
        decoded = run_stack(dec_in, dec_qkv, dec_proj, dec_up, dec_down)
        return jnp.dot(layer_norm(decoded), w_out, preferred_element_type=jnp.float32)

    return lax.map(one_clip, (patches, vis_mask))
```

```python
import functools
import math

import jax
import jax.numpy as jnp
from jax import lax
from jax.experimental import pallas as pl
from jax.experimental.pallas import tpu as pltpu
from jax.sharding import PartitionSpec as P

F32 = jnp.float32
BF16 = jnp.bfloat16
MESH = pl.DeviceIdType.MESH
VMEM = pl.BlockSpec(memory_space=pltpu.VMEM)
ANY = pl.BlockSpec(memory_space=pl.ANY)

SP = 4
CLIPS = 2
TOK = 768
PATCH = 1536
DIM = 768
ENC_HEADS = 12
HEAD = 64
DDIM = 384
DEC_HEADS = 6
VIS = 96
WIN = 2 * VIS
ROWS = SP * VIS
OWN = 2 * TOK
SEQ = SP * TOK
LAYERS = 2
EXP_SCALE = HEAD ** -0.5 * math.log2(math.e)


def dot(lhs, rhs):
    return jnp.dot(lhs, rhs, preferred_element_type=F32)


def dot_nt(lhs, rhs):
    return lax.dot_general(lhs, rhs, (((1,), (1,)), ((), ())), preferred_element_type=F32)


def dot_tn(lhs, rhs):
    return lax.dot_general(lhs, rhs, (((0,), (0,)), ((), ())), preferred_element_type=F32)


def layer_norm(hidden):
    hid = hidden.astype(F32)
    centred = hid - jnp.mean(hid, axis=-1, keepdims=True)
    var = jnp.mean(centred * centred, axis=-1, keepdims=True)
    return (centred * lax.rsqrt(var + 1e-6)).astype(BF16)


def gelu(val):
    return (0.5 * val * (1.0 + lax.erf(val * math.sqrt(0.5)))).astype(BF16)


def col_max(val):
    return jnp.max(val, axis=0, keepdims=True)


def col_sum(val):
    return jnp.sum(val, axis=0, keepdims=True)


def embed_kernel(mask_ref, patch_ref, pos_ref, wpe_ref, bpe_ref, win_ref, rank_ref, masks, sendbuf, send_sem, recv_sem, mask_send, mask_recv):
    me = lax.axis_index('sp')
    chip = me // 2
    core = me - 2 * chip
    peer = lax.rem(me + 2, SP)
    sib = me + 1 - 2 * core
    diag = lax.rem(sib + 2, SP)

    barrier = pltpu.get_barrier_semaphore()
    for other in (peer, sib, diag):
        pl.semaphore_signal(barrier, inc=1, device_id={'sp': other}, device_id_type=MESH)
    pl.semaphore_wait(barrier, 3)

    mask_copies = []
    for step in range(1, SP):
        copy = pltpu.make_async_remote_copy(
            src_ref=mask_ref, dst_ref=masks.at[step - 1], send_sem=mask_send.at[step - 1], recv_sem=mask_recv.at[step - 1],
            device_id={'sp': lax.rem(me + step, SP)}, device_id_type=MESH)
        copy.start()
        mask_copies.append(copy)
    order_row = lax.broadcasted_iota(jnp.int32, (TOK, TOK), 0)
    order_col = lax.broadcasted_iota(jnp.int32, (TOK, TOK), 1)
    before = jnp.where(order_row < order_col, 1.0, 0.0).astype(BF16)
    for copy in mask_copies:
        copy.wait()

    mine = mask_ref[...].astype(F32)
    others = [masks[k].astype(F32) for k in range(SP - 1)]
    stacked = jnp.concatenate([mine] + others, axis=0)
    local = dot(stacked.astype(BF16), before)
    counts = jnp.sum(stacked, axis=1, keepdims=True)
    dist = lax.broadcasted_iota(jnp.int32, (CLIPS * SP, 1), 0) // CLIPS
    row_dev = lax.rem(me - dist + SP, SP)
    base = jnp.zeros((CLIPS * SP, 1), F32)
    for k in range(SP):
        dev_k = lax.rem(me - k + SP, SP)
        pair = counts[CLIPS * k:CLIPS * k + CLIPS]
        tiled = jnp.concatenate([pair] * SP, axis=0)
        base = base + jnp.where(dev_k < row_dev, tiled, 0.0)
    rank = jnp.where(stacked > 0.0, local + base, float(ROWS))
    rank_ref[...] = rank.astype(jnp.int32)

    def window(clip, mine_rank):
        dest = mine_rank - VIS * me + VIS // 2
        rows = lax.broadcasted_iota(jnp.int32, (WIN, TOK), 0)
        hit = (rows == dest) & (mine_rank < ROWS)
        hit_f32 = jnp.where(hit, 1.0, 0.0)
        select = hit_f32.astype(BF16)
        moved = dot(select, patch_ref[clip]).astype(BF16)
        occupied = jnp.sum(hit_f32, axis=1, keepdims=True)
        emb = dot(moved, wpe_ref[...]) + occupied * bpe_ref[...].astype(F32) + dot(select, pos_ref[...])
        return emb.astype(BF16)

    def send(src, dst, slot, dev):
        copy = pltpu.make_async_remote_copy(
            src_ref=src, dst_ref=dst, send_sem=send_sem.at[slot], recv_sem=recv_sem.at[slot],
            device_id={'sp': dev}, device_id_type=MESH)
        copy.start()
        return copy

    rank_i32 = rank.astype(jnp.int32)
    rank_clip = [rank_i32[0:1], rank_i32[1:2]]
    far = jnp.where(chip == 0, rank_clip[1], rank_clip[0])
    near = jnp.where(chip == 0, rank_clip[0], rank_clip[1])
    sendbuf[...] = window(1 - chip, far)
    to_peer = send(sendbuf, win_ref.at[peer * 0 + me], 0, peer)
    win_ref[me] = window(chip, near)
    to_sib = send(win_ref.at[me], win_ref.at[me], 1, sib)
    to_peer.wait_recv()
    relay = send(win_ref.at[peer], win_ref.at[peer], 2, sib)
    to_sib.wait_recv()
    relay.wait_recv()
    to_peer.wait_send()
    to_sib.wait_send()
    relay.wait_send()


def embed(mask, patches, pos, wpe, bpe):
    return pl.pallas_call(
        embed_kernel,
        out_shape=(jax.ShapeDtypeStruct((SP, WIN, DIM), BF16), jax.ShapeDtypeStruct((CLIPS * SP, TOK), jnp.int32)),
        in_specs=[VMEM] * 5,
        out_specs=(VMEM, VMEM),
        scratch_shapes=[
            pltpu.VMEM((SP - 1, CLIPS, TOK), jnp.int32),
            pltpu.VMEM((WIN, DIM), BF16),
            pltpu.SemaphoreType.DMA((3,)),
            pltpu.SemaphoreType.DMA((3,)),
            pltpu.SemaphoreType.DMA((SP - 1,)),
            pltpu.SemaphoreType.DMA((SP - 1,)),
        ],
        compiler_params=pltpu.CompilerParams(collective_id=0, has_side_effects=True, vmem_limit_bytes=40 * 2 ** 20),
        cost_estimate=pl.CostEstimate(flops=4 * 10 ** 9, bytes_accessed=10 ** 7, transcendentals=0),
        name='embed',
    )(mask, patches, pos, wpe, bpe)


def encoder_kernel(win_ref, token_ref, qkv_hbm, proj_hbm, up_hbm, down_hbm, wed_ref, z_ref, qkv, proj, up, down, hid, norm, q_t, k_n, v_t, o_t, sem):
    copies = []
    for layer in range(LAYERS):
        for idx, (src, dst) in enumerate(((qkv_hbm, qkv), (proj_hbm, proj), (up_hbm, up), (down_hbm, down))):
            copy = pltpu.make_async_copy(src.at[layer], dst.at[layer], sem.at[layer * 4 + idx])
            copy.start()
            copies.append(copy)
    half = VIS // 2
    for blk in range(SP):
        top = win_ref[blk, half:2 * half].astype(F32)
        bottom = win_ref[blk, 2 * half:3 * half].astype(F32)
        if blk > 0:
            top = top + win_ref[blk - 1, 3 * half:].astype(F32)
        if blk < SP - 1:
            bottom = bottom + win_ref[blk + 1, :half].astype(F32)
        hid[blk * VIS:blk * VIS + half] = top.astype(BF16)
        hid[blk * VIS + half:(blk + 1) * VIS] = bottom.astype(BF16)
    for layer in range(LAYERS):
        norm[...] = layer_norm(hid[...])
        copies[layer * 4].wait()
        for part, out in ((0, q_t), (2, v_t)):
            out[...] = dot_nt(qkv[layer, part * DIM:(part + 1) * DIM], norm[...]).astype(BF16)
        k_n[...] = dot_nt(norm[...], qkv[layer, DIM:2 * DIM]).astype(BF16)
        zero = jnp.zeros((HEAD, ROWS), BF16)

        def head_body(pair, carry, layer=layer):
            lanes = pl.ds(pl.multiple_of(pair * 2 * HEAD, 2 * HEAD), 2 * HEAD)
            keys = k_n[:, lanes]
            for odd in range(2):
                rows = pl.ds(pl.multiple_of((2 * pair + odd) * HEAD, HEAD), HEAD)
                q_head = q_t[rows, :]
                q_pad = jnp.concatenate([zero, q_head] if odd else [q_head, zero], axis=0)
                scores = dot(keys, q_pad)
                e = jnp.exp2(scores * EXP_SCALE - col_max(scores) * EXP_SCALE)
                o = dot(v_t[rows, :], e.astype(BF16))
                o_t[rows, :] = (o * (1.0 / col_sum(e))).astype(BF16)
            return carry

        lax.fori_loop(0, ENC_HEADS // 2, head_body, 0)
        copies[layer * 4 + 1].wait()
        mid = (hid[...].astype(F32) + dot_tn(o_t[...], proj[layer])).astype(BF16)
        hid[...] = mid
        norm[...] = layer_norm(mid)
        copies[layer * 4 + 2].wait()
        copies[layer * 4 + 3].wait()
        acc = None
        step = DIM
        for lo in range(0, 4 * DIM, step):
            act = gelu(dot(norm[...], up[layer, :, lo:lo + step]))
            part = dot(act, down[layer, lo:lo + step, :])
            acc = part if acc is None else acc + part
        hid[...] = (mid.astype(F32) + acc).astype(BF16)
    z_ref[:ROWS] = dot(layer_norm(hid[...]), wed_ref[...]).astype(BF16)
    first = lax.broadcasted_iota(jnp.int32, (2 * HEAD, DDIM), 0) == 0
    z_ref[ROWS:] = jnp.where(first, token_ref[...].astype(F32), 0.0).astype(BF16)


def encode(win, token, qkv_t, proj, up, down, wed):
    return pl.pallas_call(
        encoder_kernel,
        out_shape=jax.ShapeDtypeStruct((ROWS + 2 * HEAD, DDIM), BF16),
        in_specs=[VMEM, VMEM, ANY, ANY, ANY, ANY, VMEM],
        out_specs=VMEM,
        scratch_shapes=[
            pltpu.VMEM((LAYERS, 3 * DIM, DIM), BF16),
            pltpu.VMEM((LAYERS, DIM, DIM), BF16),
            pltpu.VMEM((LAYERS, DIM, 4 * DIM), BF16),
            pltpu.VMEM((LAYERS, 4 * DIM, DIM), BF16),
            pltpu.VMEM((ROWS, DIM), BF16),
            pltpu.VMEM((ROWS, DIM), BF16),
            pltpu.VMEM((DIM, ROWS), BF16),
            pltpu.VMEM((ROWS, DIM), BF16),
            pltpu.VMEM((DIM, ROWS), BF16),
            pltpu.VMEM((DIM, ROWS), BF16),
            pltpu.SemaphoreType.DMA((LAYERS * 4,)),
        ],
        compiler_params=pltpu.CompilerParams(vmem_limit_bytes=56 * 2 ** 20),
        cost_estimate=pl.CostEstimate(flops=12 * 10 ** 9, bytes_accessed=3 * 10 ** 7, transcendentals=0),
        name='encoder',
    )(win, token, qkv_t, proj, up, down, wed)


Q_BLK = 256
K_BLK = 128
CHUNK = 256
Q_BLKS = OWN // Q_BLK
UNITS = DEC_HEADS * Q_BLKS


def decoder_layer(hid, other_norm, wqkv, wproj, wup, wdown, norm, q_z, k_n, v_t, o_t, s_even, s_odd, finish):
    def norm_body(i, carry):
        rows = pl.ds(pl.multiple_of(i * CHUNK, CHUNK), CHUNK)
        norm[rows, :] = layer_norm(hid[rows, :])
        return carry

    lax.fori_loop(0, OWN // CHUNK, norm_body, 0)
    other_norm()

    def q_body(i, carry):
        rows = pl.ds(pl.multiple_of(i * CHUNK, CHUNK), CHUNK)
        q = dot_nt(wqkv[0:DDIM], norm[rows, :]).astype(BF16)
        zero = jnp.zeros((HEAD, CHUNK), BF16)
        for head in range(DEC_HEADS):
            q_head = q[head * HEAD:(head + 1) * HEAD]
            lo, hi = (q_head, zero) if head % 2 == 0 else (zero, q_head)
            q_z[head, 0:HEAD, rows] = lo
            q_z[head, HEAD:2 * HEAD, rows] = hi
        return carry

    lax.fori_loop(0, OWN // CHUNK, q_body, 0)

    def kv_body(i, carry):
        rows = pl.ds(pl.multiple_of(i * CHUNK, CHUNK), CHUNK)
        a = norm[rows, :]
        k_n[rows, :] = dot_nt(a, wqkv[DDIM:2 * DDIM]).astype(BF16)
        v_t[:, rows] = dot_nt(wqkv[2 * DDIM:3 * DDIM], a).astype(BF16)
        return carry

    lax.fori_loop(0, SEQ // CHUNK, kv_body, 0)

    def place(unit):
        head = unit // Q_BLKS
        return head, pl.ds(pl.multiple_of((unit - head * Q_BLKS) * Q_BLK, Q_BLK), Q_BLK)

    def mixed(unit_q, s_q, unit_p, s_p, max8):
        if unit_q is not None:
            head_q, cols_q = place(unit_q)
            q = q_z[head_q, :, cols_q]
            lanes = pl.ds(pl.multiple_of((head_q // 2) * 2 * HEAD, 2 * HEAD), 2 * HEAD)
        if unit_p is not None:
            head_p, cols_p = place(unit_p)
            shift = col_max(max8) * EXP_SCALE
            v_rows = pl.ds(pl.multiple_of(head_p * HEAD, HEAD), HEAD)
        new_max = total = acc = None
        for lo in range(0, SEQ, K_BLK):
            if unit_q is not None:
                s = dot(k_n[lo:lo + K_BLK, lanes], q)
                s_q[lo:lo + K_BLK, :] = s
                m = jnp.max(s.reshape(K_BLK // 8, 8, Q_BLK), axis=0)
                new_max = m if new_max is None else jnp.maximum(new_max, m)
            if unit_p is not None:
                e = jnp.exp2(s_p[lo:lo + K_BLK, :] * EXP_SCALE - shift)
                t = jnp.sum(e.reshape(K_BLK // 8, 8, Q_BLK), axis=0)
                total = t if total is None else total + t
                o = dot(v_t[v_rows, lo:lo + K_BLK], e.astype(BF16))
                acc = o if acc is None else acc + o
        if unit_p is not None:
            o_t[v_rows, cols_p] = (acc * (1.0 / col_sum(total))).astype(BF16)
        return new_max

    first = mixed(0, s_even, None, None, None)

    def attn_body(i, max8):
        unit = 2 * i
        max_odd = mixed(unit + 1, s_odd, unit, s_even, max8)
        return mixed(jnp.minimum(unit + 2, UNITS - 1), s_even, unit + 1, s_odd, max_odd)

    lax.fori_loop(0, UNITS // 2, attn_body, first)

    def mlp_body(i, carry):
        rows = pl.ds(pl.multiple_of(i * CHUNK, CHUNK), CHUNK)
        mid = (hid[rows, :].astype(F32) + dot_tn(o_t[:, rows], wproj[...])).astype(BF16)
        act = gelu(dot(layer_norm(mid), wup[...]))
        finish(rows, (mid.astype(F32) + dot(act, wdown[...])).astype(BF16))
        return carry

    lax.fori_loop(0, OWN // CHUNK, mlp_body, 0)


def first_layer_kernel(z_ref, rank_ref, pos_ref, wqkv, wproj, wup, wdown, out_ref, hid, norm, *scratch):
    me = lax.axis_index('sp')
    chip = me // 2
    core = me - 2 * chip
    peer = lax.rem(me + 2, SP)
    sib = me + 1 - 2 * core
    diag = lax.rem(sib + 2, SP)

    def tokens(dev):
        slot = lax.rem(me - dev + SP, SP)
        rank = rank_ref[pl.ds(2 * slot + chip, 1), :]
        rank_col = jnp.transpose(jnp.broadcast_to(rank.astype(F32), (8, TOK)))[:, 0:1]
        lanes = lax.broadcasted_iota(jnp.int32, (TOK, ROWS + 2 * HEAD), 1).astype(F32)
        select = jnp.where(lanes == rank_col, 1.0, 0.0).astype(BF16)
        return (dot(select, z_ref[...]) + pos_ref[slot].astype(F32)).astype(BF16)

    hid[0:TOK] = tokens(peer)
    hid[TOK:OWN] = tokens(me)

    def other_norm():
        norm[OWN:OWN + TOK] = layer_norm(tokens(diag))
        norm[OWN + TOK:SEQ] = layer_norm(tokens(sib))

    def finish(rows, val):
        out_ref[rows, :] = val

    decoder_layer(hid, other_norm, wqkv, wproj, wup, wdown, norm, *scratch, finish)


def last_layer_kernel(hid, other, wqkv, wproj, wup, wdown, out_ref, norm, *scratch):
    def other_norm():
        def body(i, carry):
            rows = pl.ds(pl.multiple_of(i * CHUNK, CHUNK), CHUNK)
            norm[pl.ds(pl.multiple_of(OWN + i * CHUNK, CHUNK), CHUNK), :] = layer_norm(other[rows, :])
            return carry

        lax.fori_loop(0, OWN // CHUNK, body, 0)

    def finish(rows, val):
        out_ref[rows, :] = layer_norm(val)

    decoder_layer(hid, other_norm, wqkv, wproj, wup, wdown, norm, *scratch, finish)


LAYER_SCRATCH = [
    pltpu.VMEM((SEQ, DDIM), BF16),
    pltpu.VMEM((DEC_HEADS, 2 * HEAD, OWN), BF16),
    pltpu.VMEM((SEQ, DDIM), BF16),
    pltpu.VMEM((DDIM, SEQ), BF16),
    pltpu.VMEM((DDIM, OWN), BF16),
    pltpu.VMEM((SEQ, Q_BLK), F32),
    pltpu.VMEM((SEQ, Q_BLK), F32),
]
LAYER_COST = pl.CostEstimate(flops=30 * 10 ** 9, bytes_accessed=10 ** 7, transcendentals=3 * 10 ** 7)


def first_layer(z, rank, pos, wqkv, wproj, wup, wdown):
    return pl.pallas_call(
        first_layer_kernel,
        out_shape=jax.ShapeDtypeStruct((OWN, DDIM), BF16),
        in_specs=[VMEM] * 7,
        out_specs=VMEM,
        scratch_shapes=[pltpu.VMEM((OWN, DDIM), BF16)] + LAYER_SCRATCH,
        compiler_params=pltpu.CompilerParams(vmem_limit_bytes=50 * 2 ** 20),
        cost_estimate=LAYER_COST,
        name='decoder_first',
    )(z, rank, pos, wqkv, wproj, wup, wdown)


def last_layer(hid, other, wqkv, wproj, wup, wdown):
    return pl.pallas_call(
        last_layer_kernel,
        out_shape=jax.ShapeDtypeStruct((OWN, DDIM), BF16),
        in_specs=[VMEM] * 6,
        out_specs=VMEM,
        scratch_shapes=LAYER_SCRATCH,
        compiler_params=pltpu.CompilerParams(vmem_limit_bytes=50 * 2 ** 20),
        cost_estimate=LAYER_COST,
        name='decoder_last',
    )(hid, other, wqkv, wproj, wup, wdown)


def solution(mesh):
    across = [(0, 2), (1, 3), (2, 0), (3, 1)]
    beside = [(0, 1), (1, 0), (2, 3), (3, 2)]

    def local_program(patches, vis_mask, enc_pos, dec_pos, w_pe, b_pe, enc_qkv, enc_proj, enc_up, enc_down, w_ed, mask_token, dec_qkv, dec_proj, dec_up, dec_down, w_out):
        me = lax.axis_index('sp')
        chip = me // 2
        enc_qkv_t = jnp.transpose(enc_qkv, (0, 2, 3, 4, 1)).reshape(LAYERS, 3 * DIM, DIM)
        dec_qkv_t = jnp.transpose(dec_qkv, (0, 2, 3, 4, 1)).reshape(LAYERS, 3 * DDIM, DDIM)
        enc_proj2 = enc_proj.reshape(LAYERS, DIM, DIM)
        dec_proj2 = dec_proj.reshape(LAYERS, DDIM, DDIM)
        win, rank = embed(vis_mask, patches, enc_pos, w_pe, b_pe.reshape(1, DIM))
        dec_pos, win = lax.optimization_barrier((dec_pos, win))
        pos_peer = lax.ppermute(dec_pos, 'sp', across)
        pos_sib = lax.ppermute(dec_pos, 'sp', beside)
        pos_diag = lax.ppermute(pos_peer, 'sp', beside)
        even = me == 2 * chip
        pos = jnp.stack([dec_pos, jnp.where(even, pos_diag, pos_sib), pos_peer, jnp.where(even, pos_sib, pos_diag)])
        z = encode(win, mask_token.reshape(1, DDIM), enc_qkv_t, enc_proj2, enc_up, enc_down, w_ed)
        hid = first_layer(z, rank, pos, dec_qkv_t[0], dec_proj2[0], dec_up[0], dec_down[0])
        other = lax.ppermute(hid, 'sp', beside)
        final = last_layer(hid, other, dec_qkv_t[1], dec_proj2[1], dec_up[1], dec_down[1])
        back = lax.ppermute(final[:TOK], 'sp', across)
        here = final[TOK:]
        both = jnp.stack([jnp.where(chip == 0, here, back), jnp.where(chip == 0, back, here)])
        return jnp.einsum('cne,ep->cnp', both, w_out, preferred_element_type=F32)

    row_spec = P('dp', 'sp', None)
    pos_spec = P(('dp', 'sp'), None)
    arg_specs = (row_spec, P('dp', 'sp'), pos_spec, pos_spec) + (P(),) * 13
    return jax.shard_map(local_program, mesh=mesh, in_specs=arg_specs, out_specs=row_spec, check_vma=False)
```

```python
import functools
import math

import jax
import jax.numpy as jnp
from jax import lax
from jax.experimental import pallas as pl
from jax.experimental.pallas import tpu as pltpu
from jax.sharding import PartitionSpec as P

F32 = jnp.float32
BF16 = jnp.bfloat16
MESH = pl.DeviceIdType.MESH
VMEM = pl.BlockSpec(memory_space=pltpu.VMEM)
ANY = pl.BlockSpec(memory_space=pl.ANY)

SP = 4
CLIPS = 2
TOK = 768
PATCH = 1536
DIM = 768
ENC_HEADS = 12
HEAD = 64
DDIM = 384
DEC_HEADS = 6
VIS = 96
WIN = 2 * VIS
ROWS = SP * VIS
OWN = 2 * TOK
SEQ = SP * TOK
LAYERS = 2
EXP_SCALE = HEAD ** -0.5 * math.log2(math.e)


def dot(lhs, rhs):
    return jnp.dot(lhs, rhs, preferred_element_type=F32)


def dot_nt(lhs, rhs):
    return lax.dot_general(lhs, rhs, (((1,), (1,)), ((), ())), preferred_element_type=F32)


def dot_tn(lhs, rhs):
    return lax.dot_general(lhs, rhs, (((0,), (0,)), ((), ())), preferred_element_type=F32)


def layer_norm(hidden):
    hid = hidden.astype(F32)
    centred = hid - jnp.mean(hid, axis=-1, keepdims=True)
    var = jnp.mean(centred * centred, axis=-1, keepdims=True)
    return (centred * lax.rsqrt(var + 1e-6)).astype(BF16)


def gelu(val):
    return (0.5 * val * (1.0 + lax.erf(val * math.sqrt(0.5)))).astype(BF16)


def col_max(val):
    return jnp.max(val, axis=0, keepdims=True)


def col_sum(val):
    return jnp.sum(val, axis=0, keepdims=True)


def embed_kernel(mask_ref, patch_ref, pos_ref, wpe_ref, bpe_ref, win_ref, rank_ref, masks, sendbuf, send_sem, recv_sem, mask_send, mask_recv):
    me = lax.axis_index('sp')
    chip = me // 2
    core = me - 2 * chip
    peer = lax.rem(me + 2, SP)
    sib = me + 1 - 2 * core
    diag = lax.rem(sib + 2, SP)

    barrier = pltpu.get_barrier_semaphore()
    for other in (peer, sib, diag):
        pl.semaphore_signal(barrier, inc=1, device_id={'sp': other}, device_id_type=MESH)
    pl.semaphore_wait(barrier, 3)

    mask_copies = []
    for step in range(1, SP):
        copy = pltpu.make_async_remote_copy(
            src_ref=mask_ref, dst_ref=masks.at[step - 1], send_sem=mask_send.at[step - 1], recv_sem=mask_recv.at[step - 1],
            device_id={'sp': lax.rem(me + step, SP)}, device_id_type=MESH)
        copy.start()
        mask_copies.append(copy)
    order_row = lax.broadcasted_iota(jnp.int32, (TOK, TOK), 0)
    order_col = lax.broadcasted_iota(jnp.int32, (TOK, TOK), 1)
    before = jnp.where(order_row < order_col, 1.0, 0.0).astype(BF16)
    for copy in mask_copies:
        copy.wait()

    mine = mask_ref[...].astype(F32)
    others = [masks[k].astype(F32) for k in range(SP - 1)]
    stacked = jnp.concatenate([mine] + others, axis=0)
    local = dot(stacked.astype(BF16), before)
    counts = jnp.sum(stacked, axis=1, keepdims=True)
    dist = lax.broadcasted_iota(jnp.int32, (CLIPS * SP, 1), 0) // CLIPS
    row_dev = lax.rem(me - dist + SP, SP)
    base = jnp.zeros((CLIPS * SP, 1), F32)
    for k in range(SP):
        dev_k = lax.rem(me - k + SP, SP)
        pair = counts[CLIPS * k:CLIPS * k + CLIPS]
        tiled = jnp.concatenate([pair] * SP, axis=0)
        base = base + jnp.where(dev_k < row_dev, tiled, 0.0)
    rank = jnp.where(stacked > 0.0, local + base, float(ROWS))
    rank_ref[...] = rank.astype(jnp.int32)

    def window(clip, mine_rank):
        dest = mine_rank - VIS * me + VIS // 2
        rows = lax.broadcasted_iota(jnp.int32, (WIN, TOK), 0)
        hit = (rows == dest) & (mine_rank < ROWS)
        hit_f32 = jnp.where(hit, 1.0, 0.0)
        select = hit_f32.astype(BF16)
        moved = dot(select, patch_ref[clip]).astype(BF16)
        occupied = jnp.sum(hit_f32, axis=1, keepdims=True)
        emb = dot(moved, wpe_ref[...]) + occupied * bpe_ref[...].astype(F32) + dot(select, pos_ref[...])
        return emb.astype(BF16)

    def send(src, dst, slot, dev):
        copy = pltpu.make_async_remote_copy(
            src_ref=src, dst_ref=dst, send_sem=send_sem.at[slot], recv_sem=recv_sem.at[slot],
            device_id={'sp': dev}, device_id_type=MESH)
        copy.start()
        return copy

    rank_i32 = rank.astype(jnp.int32)
    rank_clip = [rank_i32[0:1], rank_i32[1:2]]
    far = jnp.where(chip == 0, rank_clip[1], rank_clip[0])
    near = jnp.where(chip == 0, rank_clip[0], rank_clip[1])
    sendbuf[...] = window(1 - chip, far)
    to_peer = send(sendbuf, win_ref.at[peer * 0 + me], 0, peer)
    win_ref[me] = window(chip, near)
    to_sib = send(win_ref.at[me], win_ref.at[me], 1, sib)
    to_peer.wait_recv()
    relay = send(win_ref.at[peer], win_ref.at[peer], 2, sib)
    to_sib.wait_recv()
    relay.wait_recv()
    to_peer.wait_send()
    to_sib.wait_send()
    relay.wait_send()


def embed(mask, patches, pos, wpe, bpe):
    return pl.pallas_call(
        embed_kernel,
        out_shape=(jax.ShapeDtypeStruct((SP, WIN, DIM), BF16), jax.ShapeDtypeStruct((CLIPS * SP, TOK), jnp.int32)),
        in_specs=[VMEM] * 5,
        out_specs=(VMEM, VMEM),
        scratch_shapes=[
            pltpu.VMEM((SP - 1, CLIPS, TOK), jnp.int32),
            pltpu.VMEM((WIN, DIM), BF16),
            pltpu.SemaphoreType.DMA((3,)),
            pltpu.SemaphoreType.DMA((3,)),
            pltpu.SemaphoreType.DMA((SP - 1,)),
            pltpu.SemaphoreType.DMA((SP - 1,)),
        ],
        compiler_params=pltpu.CompilerParams(collective_id=0, has_side_effects=True, vmem_limit_bytes=40 * 2 ** 20),
        cost_estimate=pl.CostEstimate(flops=4 * 10 ** 9, bytes_accessed=10 ** 7, transcendentals=0),
        name='embed',
    )(mask, patches, pos, wpe, bpe)


def encoder_kernel(win_ref, token_ref, qkv_hbm, proj_hbm, up_hbm, down_hbm, wed_ref, z_ref, qkv, proj, up, down, hid, norm, q_t, k_n, v_t, o_t, sem):
    copies = []
    for layer in range(LAYERS):
        for idx, (src, dst) in enumerate(((qkv_hbm, qkv), (proj_hbm, proj), (up_hbm, up), (down_hbm, down))):
            copy = pltpu.make_async_copy(src.at[layer], dst.at[layer], sem.at[layer * 4 + idx])
            copy.start()
            copies.append(copy)
    half = VIS // 2
    for blk in range(SP):
        top = win_ref[blk, half:2 * half].astype(F32)
        bottom = win_ref[blk, 2 * half:3 * half].astype(F32)
        if blk > 0:
            top = top + win_ref[blk - 1, 3 * half:].astype(F32)
        if blk < SP - 1:
            bottom = bottom + win_ref[blk + 1, :half].astype(F32)
        hid[blk * VIS:blk * VIS + half] = top.astype(BF16)
        hid[blk * VIS + half:(blk + 1) * VIS] = bottom.astype(BF16)
    for layer in range(LAYERS):
        norm[...] = layer_norm(hid[...])
        copies[layer * 4].wait()
        for part, out in ((0, q_t), (2, v_t)):
            out[...] = dot_nt(qkv[layer, part * DIM:(part + 1) * DIM], norm[...]).astype(BF16)
        k_n[...] = dot_nt(norm[...], qkv[layer, DIM:2 * DIM]).astype(BF16)
        zero = jnp.zeros((HEAD, ROWS), BF16)

        def head_body(pair, carry, layer=layer):
            lanes = pl.ds(pl.multiple_of(pair * 2 * HEAD, 2 * HEAD), 2 * HEAD)
            keys = k_n[:, lanes]
            for odd in range(2):
                rows = pl.ds(pl.multiple_of((2 * pair + odd) * HEAD, HEAD), HEAD)
                q_head = q_t[rows, :]
                q_pad = jnp.concatenate([zero, q_head] if odd else [q_head, zero], axis=0)
                scores = dot(keys, q_pad)
                e = jnp.exp2(scores * EXP_SCALE - col_max(scores) * EXP_SCALE)
                o = dot(v_t[rows, :], e.astype(BF16))
                o_t[rows, :] = (o * (1.0 / col_sum(e))).astype(BF16)
            return carry

        lax.fori_loop(0, ENC_HEADS // 2, head_body, 0)
        copies[layer * 4 + 1].wait()
        mid = (hid[...].astype(F32) + dot_tn(o_t[...], proj[layer])).astype(BF16)
        hid[...] = mid
        norm[...] = layer_norm(mid)
        copies[layer * 4 + 2].wait()
        copies[layer * 4 + 3].wait()
        acc = None
        step = DIM
        for lo in range(0, 4 * DIM, step):
            act = gelu(dot(norm[...], up[layer, :, lo:lo + step]))
            part = dot(act, down[layer, lo:lo + step, :])
            acc = part if acc is None else acc + part
        hid[...] = (mid.astype(F32) + acc).astype(BF16)
    z_ref[:ROWS] = dot(layer_norm(hid[...]), wed_ref[...]).astype(BF16)
    first = lax.broadcasted_iota(jnp.int32, (2 * HEAD, DDIM), 0) == 0
    z_ref[ROWS:] = jnp.where(first, token_ref[...].astype(F32), 0.0).astype(BF16)


def encode(win, token, qkv_t, proj, up, down, wed):
    return pl.pallas_call(
        encoder_kernel,
        out_shape=jax.ShapeDtypeStruct((ROWS + 2 * HEAD, DDIM), BF16),
        in_specs=[VMEM, VMEM, ANY, ANY, ANY, ANY, VMEM],
        out_specs=VMEM,
        scratch_shapes=[
            pltpu.VMEM((LAYERS, 3 * DIM, DIM), BF16),
            pltpu.VMEM((LAYERS, DIM, DIM), BF16),
            pltpu.VMEM((LAYERS, DIM, 4 * DIM), BF16),
            pltpu.VMEM((LAYERS, 4 * DIM, DIM), BF16),
            pltpu.VMEM((ROWS, DIM), BF16),
            pltpu.VMEM((ROWS, DIM), BF16),
            pltpu.VMEM((DIM, ROWS), BF16),
            pltpu.VMEM((ROWS, DIM), BF16),
            pltpu.VMEM((DIM, ROWS), BF16),
            pltpu.VMEM((DIM, ROWS), BF16),
            pltpu.SemaphoreType.DMA((LAYERS * 4,)),
        ],
        compiler_params=pltpu.CompilerParams(vmem_limit_bytes=56 * 2 ** 20),
        cost_estimate=pl.CostEstimate(flops=12 * 10 ** 9, bytes_accessed=3 * 10 ** 7, transcendentals=0),
        name='encoder',
    )(win, token, qkv_t, proj, up, down, wed)


Q_BLK = 512
K_BLK = 256
CHUNK = 256
WIDE = 512
PAIR = 2 * HEAD


def fill_rows(start, count, step, body):
    def run(i, carry):
        body(pl.ds(pl.multiple_of(start + i * step, step), step))
        return carry

    lax.fori_loop(0, count // step, run, 0)


def make_queries(rows, norm, w_q, q_3):
    q = dot_nt(w_q, norm[rows, :]).astype(BF16).astype(F32) * EXP_SCALE
    hi = q.astype(BF16)
    rest = q - hi.astype(F32)
    mid = rest.astype(BF16)
    low = (rest - mid.astype(F32)).astype(BF16)
    zero = jnp.zeros((HEAD, q.shape[1]), BF16)
    for head in range(DEC_HEADS):
        part = slice(head * HEAD, (head + 1) * HEAD)
        tail = (low[part], zero) if head % 2 == 0 else (zero, low[part])
        for idx, val in enumerate((hi[part], mid[part]) + tail):
            q_3[head, idx * HEAD:(idx + 1) * HEAD, rows] = val


def make_keys(rows, norm, w_k, w_v, k_n, k_dup, v_t):
    a = norm[rows, :]
    k = dot_nt(a, w_k)
    k_n[rows, :] = k.astype(BF16)
    first = lax.broadcasted_iota(jnp.int32, (k.shape[0], PAIR), 1) < HEAD
    for pair in range(DEC_HEADS // 2):
        both = k[:, pair * PAIR:(pair + 1) * PAIR]
        turned = pltpu.roll(both, HEAD, axis=1)
        k_dup[rows, 2 * pair * PAIR:(2 * pair + 1) * PAIR] = jnp.where(first, both, turned).astype(BF16)
        k_dup[rows, (2 * pair + 1) * PAIR:(2 * pair + 2) * PAIR] = jnp.where(first, turned, both).astype(BF16)
    v_t[:, rows] = dot_nt(w_v, a).astype(BF16)


def attention(start, count, q_3, k_n, k_dup, v_t, o_t, s_even, s_odd):
    blocks = count // Q_BLK
    units = DEC_HEADS * blocks

    def place(unit):
        head = unit // blocks
        return head, pl.ds(pl.multiple_of(start + (unit - head * blocks) * Q_BLK, Q_BLK), Q_BLK)

    def mixed(unit_q, s_q, unit_p, s_p, max8):
        if unit_q is not None:
            head_q, cols_q = place(unit_q)
            q = q_3[head_q, :, cols_q]
            lanes = pl.ds(pl.multiple_of((head_q // 2) * PAIR, PAIR), PAIR)
            lanes_dup = pl.ds(pl.multiple_of(head_q * PAIR, PAIR), PAIR)
        if unit_p is not None:
            head_p, cols_p = place(unit_p)
            shift = col_max(max8)
            v_rows = pl.ds(pl.multiple_of(head_p * HEAD, HEAD), HEAD)
        new_max = total = late = None
        accs = [None, None]

        def weigh(idx, weights):
            o = dot(v_t[v_rows, idx * K_BLK:(idx + 1) * K_BLK], weights)
            accs[idx % 2] = o if accs[idx % 2] is None else accs[idx % 2] + o

        for idx in range(SEQ // K_BLK):
            rows = slice(idx * K_BLK, (idx + 1) * K_BLK)
            if unit_p is not None:
                e = jnp.exp2(s_p[rows, :] - shift)
                t = jnp.sum(e.reshape(K_BLK // 8, 8, Q_BLK), axis=0)
                total = t if total is None else total + t
                if late is not None:
                    weigh(*late)
                late = (idx, e.astype(BF16))
            if unit_q is not None:
                keys = jnp.concatenate([k_dup[rows, lanes_dup], k_n[rows, lanes]], axis=1)
                s = dot(keys, q)
                s_q[rows, :] = s
                m = jnp.max(s.reshape(K_BLK // 8, 8, Q_BLK), axis=0)
                new_max = m if new_max is None else jnp.maximum(new_max, m)
        if unit_p is not None:
            weigh(*late)
            o_t[v_rows, cols_p] = ((accs[0] + accs[1]) * (1.0 / col_sum(total))).astype(BF16)
        return new_max

    first = mixed(0, s_even, None, None, None)

    def body(i, max8):
        unit = 2 * i
        max_odd = mixed(unit + 1, s_odd, unit, s_even, max8)
        return mixed(jnp.minimum(unit + 2, units - 1), s_even, unit + 1, s_odd, max_odd)

    lax.fori_loop(0, units // 2, body, first)


def mlp(rows, hid, o_t, w_proj, w_up, w_down):
    mid = (hid[rows, :].astype(F32) + dot_tn(o_t[:, rows], w_proj)).astype(BF16)
    act = gelu(dot(layer_norm(mid), w_up))
    return (mid.astype(F32) + dot(act, w_down)).astype(BF16)


def decoder_kernel(z_ref, rank_ref, pos_me, pos_peer, pos_sib, pos_diag, qkv_hbm, proj_hbm, up_hbm, down_hbm, both_ref,
                   qkv, proj, up, down, hid, norm, fin, q_3, k_n, k_dup, v_t, o_t, s_even, s_odd, w_sem, ready, row_send, row_recv, fin_send, fin_recv):
    me = lax.axis_index('sp')
    chip = me // 2
    core = me - 2 * chip
    peer = lax.rem(me + 2, SP)
    sib = me + 1 - 2 * core
    diag = lax.rem(sib + 2, SP)

    copies = []
    for layer in range(LAYERS):
        for idx, (src, dst) in enumerate(((qkv_hbm, qkv), (proj_hbm, proj), (up_hbm, up), (down_hbm, down))):
            copy = pltpu.make_async_copy(src.at[layer], dst.at[layer], w_sem.at[layer * 4 + idx])
            copy.start()
            copies.append(copy)
    barrier = pltpu.get_barrier_semaphore()
    for other in (peer, sib):
        pl.semaphore_signal(barrier, inc=1, device_id={'sp': other}, device_id_type=MESH)
    pl.semaphore_wait(barrier, 2)

    def tokens(dev, pos_ref):
        slot = lax.rem(me - dev + SP, SP)
        rank = rank_ref[pl.ds(2 * slot + chip, 1), :]
        rank_col = jnp.transpose(jnp.broadcast_to(rank.astype(F32), (8, TOK)))[:, 0:1]
        lanes = lax.broadcasted_iota(jnp.int32, (TOK, ROWS + 2 * HEAD), 1).astype(F32)
        select = jnp.where(lanes == rank_col, 1.0, 0.0).astype(BF16)
        return (dot(select, z_ref[...]) + pos_ref[...].astype(F32)).astype(BF16)

    hid[0:TOK] = tokens(peer, pos_peer)
    hid[TOK:OWN] = tokens(me, pos_me)
    norm[OWN:OWN + TOK] = layer_norm(tokens(diag, pos_diag))
    norm[OWN + TOK:SEQ] = layer_norm(tokens(sib, pos_sib))

    def own_norm(rows):
        norm[rows, :] = layer_norm(hid[rows, :])

    fill_rows(0, OWN, CHUNK, own_norm)

    def queries(layer):
        fill_rows(0, OWN, WIDE, lambda rows: make_queries(rows, norm, qkv[layer, 0:DDIM], q_3))

    def keys(layer, start, count):
        fill_rows(start, count, WIDE, lambda rows: make_keys(
            rows, norm, qkv[layer, DDIM:2 * DDIM], qkv[layer, 2 * DDIM:3 * DDIM], k_n, k_dup, v_t))

    for copy in copies:
        copy.wait()
    queries(0)
    keys(0, 0, SEQ)
    pl.semaphore_signal(ready, inc=1, device_id={'sp': sib}, device_id_type=MESH)
    attention(0, OWN, q_3, k_n, k_dup, v_t, o_t, s_even, s_odd)
    pl.semaphore_wait(ready, 1)
    steps = OWN // CHUNK

    def row_copy(i):
        src = pl.ds(pl.multiple_of(i * CHUNK, CHUNK), CHUNK)
        dst = pl.ds(pl.multiple_of(OWN + i * CHUNK, CHUNK), CHUNK)
        return pltpu.make_async_remote_copy(
            src_ref=norm.at[src], dst_ref=norm.at[dst], send_sem=row_send.at[i], recv_sem=row_recv.at[i],
            device_id={'sp': sib}, device_id_type=MESH)

    def first_mlp(i, carry):
        rows = pl.ds(pl.multiple_of(i * CHUNK, CHUNK), CHUNK)
        val = mlp(rows, hid, o_t, proj[0], up[0], down[0])
        hid[rows, :] = val
        norm[rows, :] = layer_norm(val)

        @pl.when(i > 0)
        def _():
            row_copy(i - 1).start()

        return carry

    lax.fori_loop(0, steps, first_mlp, 0)
    queries(1)
    row_copy(steps - 1).start()
    keys(1, 0, OWN)
    for i in range(steps):
        row_copy(i).wait()
    keys(1, OWN, OWN)

    early = 2 * Q_BLK
    attention(0, early, q_3, k_n, k_dup, v_t, o_t, s_even, s_odd)

    def last_rows(rows):
        fin[rows, :] = layer_norm(mlp(rows, hid, o_t, proj[1], up[1], down[1]))

    fill_rows(0, early, CHUNK, last_rows)
    send = pltpu.make_async_remote_copy(
        src_ref=fin.at[pl.ds(0, TOK)], dst_ref=both_ref.at[chip], send_sem=fin_send, recv_sem=fin_recv,
        device_id={'sp': peer}, device_id_type=MESH)
    send.start()
    attention(early, OWN - early, q_3, k_n, k_dup, v_t, o_t, s_even, s_odd)
    fill_rows(early, OWN - early, CHUNK, last_rows)
    both_ref[chip] = fin[TOK:OWN]
    send.wait()


def decode(z, rank, pos, wqkv, wproj, wup, wdown):
    return pl.pallas_call(
        decoder_kernel,
        out_shape=jax.ShapeDtypeStruct((CLIPS, TOK, DDIM), BF16),
        in_specs=[VMEM] * 6 + [ANY] * 4,
        out_specs=VMEM,
        scratch_shapes=[
            pltpu.VMEM((LAYERS, 3 * DDIM, DDIM), BF16),
            pltpu.VMEM((LAYERS, DDIM, DDIM), BF16),
            pltpu.VMEM((LAYERS, DDIM, 4 * DDIM), BF16),
            pltpu.VMEM((LAYERS, 4 * DDIM, DDIM), BF16),
            pltpu.VMEM((OWN, DDIM), BF16),
            pltpu.VMEM((SEQ, DDIM), BF16),
            pltpu.VMEM((OWN, DDIM), BF16),
            pltpu.VMEM((DEC_HEADS, 4 * HEAD, OWN), BF16),
            pltpu.VMEM((SEQ, DDIM), BF16),
            pltpu.VMEM((SEQ, 2 * DDIM), BF16),
            pltpu.VMEM((DDIM, SEQ), BF16),
            pltpu.VMEM((DDIM, OWN), BF16),
            pltpu.VMEM((SEQ, Q_BLK), F32),
            pltpu.VMEM((SEQ, Q_BLK), F32),
            pltpu.SemaphoreType.DMA((LAYERS * 4,)),
            pltpu.SemaphoreType.REGULAR,
            pltpu.SemaphoreType.DMA((OWN // CHUNK,)),
            pltpu.SemaphoreType.DMA((OWN // CHUNK,)),
            pltpu.SemaphoreType.DMA,
            pltpu.SemaphoreType.DMA,
        ],
        compiler_params=pltpu.CompilerParams(collective_id=1, has_side_effects=True, vmem_limit_bytes=58 * 2 ** 20),
        cost_estimate=pl.CostEstimate(flops=60 * 10 ** 9, bytes_accessed=2 * 10 ** 7, transcendentals=6 * 10 ** 7),
        name='decoder',
    )(z, rank, *pos, wqkv, wproj, wup, wdown)


def solution(mesh):
    across = [(0, 2), (1, 3), (2, 0), (3, 1)]
    beside = [(0, 1), (1, 0), (2, 3), (3, 2)]

    def local_program(patches, vis_mask, enc_pos, dec_pos, w_pe, b_pe, enc_qkv, enc_proj, enc_up, enc_down, w_ed, mask_token, dec_qkv, dec_proj, dec_up, dec_down, w_out):
        enc_qkv_t = jnp.transpose(enc_qkv, (0, 2, 3, 4, 1)).reshape(LAYERS, 3 * DIM, DIM)
        dec_qkv_t = jnp.transpose(dec_qkv, (0, 2, 3, 4, 1)).reshape(LAYERS, 3 * DDIM, DDIM)
        enc_proj2 = enc_proj.reshape(LAYERS, DIM, DIM)
        dec_proj2 = dec_proj.reshape(LAYERS, DDIM, DDIM)
        win, rank = embed(vis_mask, patches, enc_pos, w_pe, b_pe.reshape(1, DIM))
        dec_pos, win = lax.optimization_barrier((dec_pos, win))
        pos_peer = lax.ppermute(dec_pos, 'sp', across)
        pos_sib = lax.ppermute(dec_pos, 'sp', beside)
        pos_diag = lax.ppermute(pos_peer, 'sp', beside)
        z = encode(win, mask_token.reshape(1, DDIM), enc_qkv_t, enc_proj2, enc_up, enc_down, w_ed)
        both = decode(z, rank, (dec_pos, pos_peer, pos_sib, pos_diag), dec_qkv_t, dec_proj2, dec_up, dec_down)
        return jnp.einsum('cne,ep->cnp', both, w_out, preferred_element_type=F32)

    row_spec = P('dp', 'sp', None)
    pos_spec = P(('dp', 'sp'), None)
    arg_specs = (row_spec, P('dp', 'sp'), pos_spec, pos_spec) + (P(),) * 13
    return jax.shard_map(local_program, mesh=mesh, in_specs=arg_specs, out_specs=row_spec, check_vma=False)
```

```python
import functools
import math

import jax
import jax.numpy as jnp
from jax import lax
from jax.experimental import pallas as pl
from jax.experimental.pallas import tpu as pltpu
from jax.sharding import PartitionSpec as P

F32 = jnp.float32
BF16 = jnp.bfloat16
MESH = pl.DeviceIdType.MESH
VMEM = pl.BlockSpec(memory_space=pltpu.VMEM)
ANY = pl.BlockSpec(memory_space=pl.ANY)

SP = 4
CLIPS = 2
TOK = 768
PATCH = 1536
DIM = 768
ENC_HEADS = 12
HEAD = 64
DDIM = 384
DEC_HEADS = 6
VIS = 96
WIN = 2 * VIS
ROWS = SP * VIS
OWN = 2 * TOK
SEQ = SP * TOK
LAYERS = 2
EXP_SCALE = HEAD ** -0.5 * math.log2(math.e)


def dot(lhs, rhs):
    return jnp.dot(lhs, rhs, preferred_element_type=F32)


def dot_nt(lhs, rhs):
    return lax.dot_general(lhs, rhs, (((1,), (1,)), ((), ())), preferred_element_type=F32)


def dot_tn(lhs, rhs):
    return lax.dot_general(lhs, rhs, (((0,), (0,)), ((), ())), preferred_element_type=F32)


def layer_norm(hidden):
    hid = hidden.astype(F32)
    centred = hid - jnp.mean(hid, axis=-1, keepdims=True)
    var = jnp.mean(centred * centred, axis=-1, keepdims=True)
    return (centred * lax.rsqrt(var + 1e-6)).astype(BF16)


def gelu(val):
    return (0.5 * val * (1.0 + lax.erf(val * math.sqrt(0.5)))).astype(BF16)


def col_max(val):
    return jnp.max(val, axis=0, keepdims=True)


def col_sum(val):
    return jnp.sum(val, axis=0, keepdims=True)


MINE = ROWS // 2
Q_PAD = 256


def encoder_kernel(mask_ref, bpe_ref, token_ref, patch_hbm, pos_hbm, wpe_hbm, dec_pos_hbm, wed_ref, qkv_hbm, proj_hbm, up_hbm, down_hbm,
                   z_ref, rank_ref, pos_out,
                   patch, pos, wpe, qkv, proj, up, down, masks, sendbuf, win, hall, hid, norm, norm_q, q_t, k_n, v_t, o_t,
                   in_sem, w_sem, mask_send, mask_recv, win_send, win_recv, pos_send, pos_recv, row_send, row_recv):
    me = lax.axis_index('sp')
    chip = me // 2
    core = me - 2 * chip
    peer = lax.rem(me + 2, SP)
    sib = me + 1 - 2 * core
    diag = lax.rem(sib + 2, SP)

    loads = [pltpu.make_async_copy(src, dst, in_sem.at[idx])
             for idx, (src, dst) in enumerate(((patch_hbm, patch), (wpe_hbm, wpe), (pos_hbm, pos)))]
    for copy in loads:
        copy.start()
    barrier = pltpu.get_barrier_semaphore()
    for other in (peer, sib, diag):
        pl.semaphore_signal(barrier, inc=1, device_id={'sp': other}, device_id_type=MESH)
    order_row = lax.broadcasted_iota(jnp.int32, (TOK, TOK), 0)
    order_col = lax.broadcasted_iota(jnp.int32, (TOK, TOK), 1)
    before = jnp.where(order_row < order_col, 1.0, 0.0).astype(BF16)
    mine = mask_ref[...].astype(F32)
    mine_rank = dot(jnp.concatenate([mine] * SP, axis=0).astype(BF16), before)[0:CLIPS]
    slot_of = jnp.where(mine > 0.0, mine_rank, -1.0)
    pl.semaphore_wait(barrier, 3)

    def send(src, dst, send_sem, recv_sem, dev):
        copy = pltpu.make_async_remote_copy(
            src_ref=src, dst_ref=dst, send_sem=send_sem, recv_sem=recv_sem, device_id={'sp': dev}, device_id_type=MESH)
        copy.start()
        return copy

    mask_copies = [send(mask_ref, masks.at[step - 1], mask_send.at[step - 1], mask_recv.at[step - 1], lax.rem(me + step, SP))
                   for step in range(1, SP)]
    for copy in loads:
        copy.wait()
    copies = []
    for layer in range(LAYERS):
        for idx, (src, dst) in enumerate(((qkv_hbm, qkv), (proj_hbm, proj), (up_hbm, up), (down_hbm, down))):
            copy = pltpu.make_async_copy(src.at[layer], dst.at[layer], w_sem.at[layer * 4 + idx])
            copy.start()
            copies.append(copy)

    def window(clip, slots):
        rows = lax.broadcasted_iota(jnp.int32, (WIN, TOK), 0).astype(F32)
        hit = jnp.where(rows == slots, 1.0, 0.0)
        select = hit.astype(BF16)
        moved = dot(select, patch[clip]).astype(BF16)
        occupied = jnp.sum(hit, axis=1, keepdims=True)
        emb = dot(moved, wpe[...]) + occupied * bpe_ref[...].astype(F32) + dot(select, pos[...])
        return emb.astype(BF16)

    far = jnp.where(chip == 0, slot_of[1:2], slot_of[0:1])
    near = jnp.where(chip == 0, slot_of[0:1], slot_of[1:2])
    sendbuf[...] = window(1 - chip, far)
    to_peer = send(sendbuf, win.at[1], win_send.at[0], win_recv.at[0], peer)
    win[0] = window(chip, near)
    to_sib = send(win.at[0], win.at[2], win_send.at[1], win_recv.at[1], sib)

    for copy in mask_copies:
        copy.wait()
    stacked = jnp.concatenate([mine] + [masks[k].astype(F32) for k in range(SP - 1)], axis=0)
    local = dot(stacked.astype(BF16), before)
    counts = jnp.sum(stacked, axis=1, keepdims=True)
    row_dev = lax.rem(me - lax.broadcasted_iota(jnp.int32, (CLIPS * SP, 1), 0) // CLIPS + SP, SP)
    base = jnp.zeros((CLIPS * SP, 1), F32)
    for k in range(SP):
        dev_k = lax.rem(me - k + SP, SP)
        tiled = jnp.concatenate([counts[CLIPS * k:CLIPS * k + CLIPS]] * SP, axis=0)
        base = base + jnp.where(dev_k < row_dev, tiled, 0.0)
    rank_ref[...] = jnp.where(stacked > 0.0, local + base, float(ROWS)).astype(jnp.int32)

    def placement(slot):
        def pick(val):
            two = val[CLIPS * slot:CLIPS * slot + CLIPS]
            return jnp.where(chip == 0, two[0:1], two[1:2])

        start, size = pick(base), pick(counts)
        rows = lax.broadcasted_iota(jnp.int32, (ROWS, WIN), 0).astype(F32)
        cols = lax.broadcasted_iota(jnp.int32, (ROWS, WIN), 1).astype(F32)
        return jnp.where((rows == cols + start) & (cols < size), 1.0, 0.0)

    even = core == 0
    left, right = placement(1), placement(3)
    place = [placement(0), placement(2), jnp.where(even, right, left), jnp.where(even, left, right)]
    to_peer.wait_recv()
    relay = send(win.at[1], win.at[3], win_send.at[2], win_recv.at[2], sib)
    pos_peer = send(dec_pos_hbm, pos_out.at[0], pos_send.at[0], pos_recv.at[0], peer)
    pos_sib = send(dec_pos_hbm, pos_out.at[1], pos_send.at[1], pos_recv.at[1], sib)
    total = dot(place[0].astype(BF16), win[0]) + dot(place[1].astype(BF16), win[1])
    to_sib.wait_recv()
    total = total + dot(place[2].astype(BF16), win[2])
    relay.wait_recv()
    total = total + dot(place[3].astype(BF16), win[3])
    hall[...] = total.astype(BF16)
    own = pl.ds(pl.multiple_of(core * MINE, MINE), MINE)
    hid[...] = hall[own, :]
    norm[0] = layer_norm(hall[...])
    norm_q[MINE:] = jnp.zeros((Q_PAD - MINE, DIM), BF16)
    zero = jnp.zeros((HEAD, Q_PAD), BF16)
    pos_diag = swap = None

    for layer in range(LAYERS):
        copies[layer * 4].wait()
        norm_q[0:MINE] = norm[layer, own, :]
        q_t[...] = dot_nt(qkv[layer, 0:DIM], norm_q[...]).astype(BF16)
        if swap is not None:
            swap.wait()
        k_n[...] = dot_nt(norm[layer], qkv[layer, DIM:2 * DIM]).astype(BF16)
        v_t[...] = dot_nt(qkv[layer, 2 * DIM:3 * DIM], norm[layer]).astype(BF16)

        def heads(group, carry):
            scores, weights = [], []
            for pair in range(2):
                lanes = pl.ds(pl.multiple_of((2 * group + pair) * 2 * HEAD, 2 * HEAD), 2 * HEAD)
                for odd in range(2):
                    rows = pl.ds(pl.multiple_of((4 * group + 2 * pair + odd) * HEAD, HEAD), HEAD)
                    q_head = q_t[rows, :]
                    q_both = jnp.concatenate([zero, q_head] if odd else [q_head, zero], axis=0)
                    scores.append(dot(k_n[:, lanes], q_both))
            for s in scores:
                e = jnp.exp2(s * EXP_SCALE - col_max(s) * EXP_SCALE)
                weights.append((e.astype(BF16), 1.0 / col_sum(e)))
            for idx, (e, scale) in enumerate(weights):
                rows = pl.ds(pl.multiple_of((4 * group + idx) * HEAD, HEAD), HEAD)
                o_t[rows, :] = (dot(v_t[rows, :], e) * scale).astype(BF16)
            return carry

        lax.fori_loop(0, ENC_HEADS // 4, heads, 0)
        if layer == 0:
            pos_peer.wait_recv()
            pos_diag = send(pos_out.at[0], pos_out.at[2], pos_send.at[2], pos_recv.at[2], sib)
        copies[layer * 4 + 1].wait()
        mid = (hid[...].astype(F32) + dot_tn(o_t[...], proj[layer])[0:MINE]).astype(BF16)
        rows_norm = layer_norm(mid)
        copies[layer * 4 + 2].wait()
        copies[layer * 4 + 3].wait()
        acc = None
        for lo in range(0, 4 * DIM, DIM):
            act = gelu(dot(rows_norm, up[layer, :, lo:lo + DIM]))
            part = dot(act, down[layer, lo:lo + DIM, :])
            acc = part if acc is None else acc + part
        out = (mid.astype(F32) + acc).astype(BF16)
        if layer < LAYERS - 1:
            hid[...] = out
            norm[layer + 1, own, :] = layer_norm(out)
            swap = send(norm.at[layer + 1, own], norm.at[layer + 1, own], row_send.at[layer], row_recv.at[layer], sib)
    z_ref[own, :] = dot(layer_norm(out), wed_ref[...]).astype(BF16)
    first = lax.broadcasted_iota(jnp.int32, (2 * HEAD, DDIM), 0) == 0
    z_ref[ROWS:] = jnp.where(first, token_ref[...].astype(F32), 0.0).astype(BF16)
    last = send(z_ref.at[own], z_ref.at[own], row_send.at[LAYERS - 1], row_recv.at[LAYERS - 1], sib)
    to_peer.wait_send()
    to_sib.wait_send()
    relay.wait_send()
    pos_peer.wait_send()
    pos_sib.wait()
    pos_diag.wait()
    last.wait()


def encode(mask, bpe, token, patches, enc_pos, wpe, dec_pos, wed, qkv_t, proj, up, down):
    return pl.pallas_call(
        encoder_kernel,
        out_shape=(
            jax.ShapeDtypeStruct((ROWS + 2 * HEAD, DDIM), BF16),
            jax.ShapeDtypeStruct((CLIPS * SP, TOK), jnp.int32),
            jax.ShapeDtypeStruct((SP - 1, TOK, DDIM), BF16),
        ),
        in_specs=[VMEM] * 3 + [ANY] * 4 + [VMEM] + [ANY] * 4,
        out_specs=(VMEM, VMEM, ANY),
        scratch_shapes=[
            pltpu.VMEM((CLIPS, TOK, PATCH), BF16),
            pltpu.VMEM((TOK, DIM), BF16),
            pltpu.VMEM((PATCH, DIM), BF16),
            pltpu.VMEM((LAYERS, 3 * DIM, DIM), BF16),
            pltpu.VMEM((LAYERS, DIM, DIM), BF16),
            pltpu.VMEM((LAYERS, DIM, 4 * DIM), BF16),
            pltpu.VMEM((LAYERS, 4 * DIM, DIM), BF16),
            pltpu.VMEM((SP - 1, CLIPS, TOK), jnp.int32),
            pltpu.VMEM((WIN, DIM), BF16),
            pltpu.VMEM((SP, WIN, DIM), BF16),
            pltpu.VMEM((ROWS, DIM), BF16),
            pltpu.VMEM((MINE, DIM), BF16),
            pltpu.VMEM((LAYERS, ROWS, DIM), BF16),
            pltpu.VMEM((Q_PAD, DIM), BF16),
            pltpu.VMEM((DIM, Q_PAD), BF16),
            pltpu.VMEM((ROWS, DIM), BF16),
            pltpu.VMEM((DIM, ROWS), BF16),
            pltpu.VMEM((DIM, Q_PAD), BF16),
            pltpu.SemaphoreType.DMA((3,)),
            pltpu.SemaphoreType.DMA((LAYERS * 4,)),
            pltpu.SemaphoreType.DMA((SP - 1,)),
            pltpu.SemaphoreType.DMA((SP - 1,)),
            pltpu.SemaphoreType.DMA((3,)),
            pltpu.SemaphoreType.DMA((3,)),
            pltpu.SemaphoreType.DMA((3,)),
            pltpu.SemaphoreType.DMA((3,)),
            pltpu.SemaphoreType.DMA((LAYERS,)),
            pltpu.SemaphoreType.DMA((LAYERS,)),
        ],
        compiler_params=pltpu.CompilerParams(collective_id=0, has_side_effects=True, vmem_limit_bytes=58 * 2 ** 20),
        cost_estimate=pl.CostEstimate(flops=12 * 10 ** 9, bytes_accessed=4 * 10 ** 7, transcendentals=0),
        name='encoder',
    )(mask, bpe, token, patches, enc_pos, wpe, dec_pos, wed, qkv_t, proj, up, down)


Q_BLK = 512
K_BLK = 256
CHUNK = 256
WIDE = 512
PAIR = 2 * HEAD


def fill_rows(start, count, step, body):
    def run(i, carry):
        body(pl.ds(pl.multiple_of(start + i * step, step), step))
        return carry

    lax.fori_loop(0, count // step, run, 0)


def make_queries(rows, norm, w_q, q_3):
    q = dot_nt(w_q, norm[rows, :]).astype(BF16).astype(F32) * EXP_SCALE
    hi = q.astype(BF16)
    rest = q - hi.astype(F32)
    mid = rest.astype(BF16)
    low = (rest - mid.astype(F32)).astype(BF16)
    zero = jnp.zeros((HEAD, q.shape[1]), BF16)
    for head in range(DEC_HEADS):
        part = slice(head * HEAD, (head + 1) * HEAD)
        tail = (low[part], zero) if head % 2 == 0 else (zero, low[part])
        for idx, val in enumerate((hi[part], mid[part]) + tail):
            q_3[head, idx * HEAD:(idx + 1) * HEAD, rows] = val


def make_keys(rows, norm, w_k, w_v, k_n, k_dup, v_t):
    a = norm[rows, :]
    k = dot_nt(a, w_k)
    k_n[rows, :] = k.astype(BF16)
    first = lax.broadcasted_iota(jnp.int32, (k.shape[0], PAIR), 1) < HEAD
    for pair in range(DEC_HEADS // 2):
        both = k[:, pair * PAIR:(pair + 1) * PAIR]
        turned = pltpu.roll(both, HEAD, axis=1)
        k_dup[rows, 2 * pair * PAIR:(2 * pair + 1) * PAIR] = jnp.where(first, both, turned).astype(BF16)
        k_dup[rows, (2 * pair + 1) * PAIR:(2 * pair + 2) * PAIR] = jnp.where(first, turned, both).astype(BF16)
    v_t[:, rows] = dot_nt(w_v, a).astype(BF16)


def attention(start, count, q_3, k_n, k_dup, v_t, o_t, s_even, s_odd):
    blocks = count // Q_BLK
    units = DEC_HEADS * blocks

    def place(unit):
        head = unit // blocks
        return head, pl.ds(pl.multiple_of(start + (unit - head * blocks) * Q_BLK, Q_BLK), Q_BLK)

    def mixed(unit_q, s_q, unit_p, s_p, max8):
        if unit_q is not None:
            head_q, cols_q = place(unit_q)
            q = q_3[head_q, :, cols_q]
            lanes = pl.ds(pl.multiple_of((head_q // 2) * PAIR, PAIR), PAIR)
            lanes_dup = pl.ds(pl.multiple_of(head_q * PAIR, PAIR), PAIR)
        if unit_p is not None:
            head_p, cols_p = place(unit_p)
            shift = col_max(max8)
            v_rows = pl.ds(pl.multiple_of(head_p * HEAD, HEAD), HEAD)
        new_max = total = late = None
        accs = [None, None]

        def weigh(idx, weights):
            o = dot(v_t[v_rows, idx * K_BLK:(idx + 1) * K_BLK], weights)
            accs[idx % 2] = o if accs[idx % 2] is None else accs[idx % 2] + o

        for idx in range(SEQ // K_BLK):
            rows = slice(idx * K_BLK, (idx + 1) * K_BLK)
            if unit_p is not None:
                e = jnp.exp2(s_p[rows, :] - shift)
                t = jnp.sum(e.reshape(K_BLK // 8, 8, Q_BLK), axis=0)
                total = t if total is None else total + t
                if late is not None:
                    weigh(*late)
                late = (idx, e.astype(BF16))
            if unit_q is not None:
                keys = jnp.concatenate([k_dup[rows, lanes_dup], k_n[rows, lanes]], axis=1)
                s = dot(keys, q)
                s_q[rows, :] = s
                m = jnp.max(s.reshape(K_BLK // 8, 8, Q_BLK), axis=0)
                new_max = m if new_max is None else jnp.maximum(new_max, m)
        if unit_p is not None:
            weigh(*late)
            o_t[v_rows, cols_p] = ((accs[0] + accs[1]) * (1.0 / col_sum(total))).astype(BF16)
        return new_max

    first = mixed(0, s_even, None, None, None)

    def body(i, max8):
        unit = 2 * i
        max_odd = mixed(unit + 1, s_odd, unit, s_even, max8)
        return mixed(jnp.minimum(unit + 2, units - 1), s_even, unit + 1, s_odd, max_odd)

    lax.fori_loop(0, units // 2, body, first)


def mlp(rows, hid, o_t, w_proj, w_up, w_down):
    mid = (hid[rows, :].astype(F32) + dot_tn(o_t[:, rows], w_proj)).astype(BF16)
    act = gelu(dot(layer_norm(mid), w_up))
    return (mid.astype(F32) + dot(act, w_down)).astype(BF16)


def decoder_kernel(z_ref, rank_ref, pos_me, pos_x, qkv_hbm, proj_hbm, up_hbm, down_hbm, both_ref,
                   qkv, proj, up, down, hid, norm, fin, q_3, k_n, k_dup, v_t, o_t, s_even, s_odd, w_sem, ready, row_send, row_recv, fin_send, fin_recv):
    me = lax.axis_index('sp')
    chip = me // 2
    core = me - 2 * chip
    peer = lax.rem(me + 2, SP)
    sib = me + 1 - 2 * core
    diag = lax.rem(sib + 2, SP)

    copies = []
    for layer in range(LAYERS):
        for idx, (src, dst) in enumerate(((qkv_hbm, qkv), (proj_hbm, proj), (up_hbm, up), (down_hbm, down))):
            copy = pltpu.make_async_copy(src.at[layer], dst.at[layer], w_sem.at[layer * 4 + idx])
            copy.start()
            copies.append(copy)
    barrier = pltpu.get_barrier_semaphore()
    for other in (peer, sib):
        pl.semaphore_signal(barrier, inc=1, device_id={'sp': other}, device_id_type=MESH)
    pl.semaphore_wait(barrier, 2)

    def tokens(dev, pos):
        slot = lax.rem(me - dev + SP, SP)
        rank = rank_ref[pl.ds(2 * slot + chip, 1), :]
        rank_col = jnp.transpose(jnp.broadcast_to(rank.astype(F32), (8, TOK)))[:, 0:1]
        lanes = lax.broadcasted_iota(jnp.int32, (TOK, ROWS + 2 * HEAD), 1).astype(F32)
        select = jnp.where(lanes == rank_col, 1.0, 0.0).astype(BF16)
        return (dot(select, z_ref[...]) + pos.astype(F32)).astype(BF16)

    hid[0:TOK] = tokens(peer, pos_x[0])
    hid[TOK:OWN] = tokens(me, pos_me[...])
    norm[OWN:OWN + TOK] = layer_norm(tokens(diag, pos_x[2]))
    norm[OWN + TOK:SEQ] = layer_norm(tokens(sib, pos_x[1]))

    def own_norm(rows):
        norm[rows, :] = layer_norm(hid[rows, :])

    fill_rows(0, OWN, CHUNK, own_norm)

    def queries(layer):
        fill_rows(0, OWN, WIDE, lambda rows: make_queries(rows, norm, qkv[layer, 0:DDIM], q_3))

    def keys(layer, start, count):
        fill_rows(start, count, WIDE, lambda rows: make_keys(
            rows, norm, qkv[layer, DDIM:2 * DDIM], qkv[layer, 2 * DDIM:3 * DDIM], k_n, k_dup, v_t))

    for copy in copies:
        copy.wait()
    queries(0)
    keys(0, 0, SEQ)
    pl.semaphore_signal(ready, inc=1, device_id={'sp': sib}, device_id_type=MESH)
    attention(0, OWN, q_3, k_n, k_dup, v_t, o_t, s_even, s_odd)
    pl.semaphore_wait(ready, 1)
    steps = OWN // CHUNK

    def row_copy(i):
        src = pl.ds(pl.multiple_of(i * CHUNK, CHUNK), CHUNK)
        dst = pl.ds(pl.multiple_of(OWN + i * CHUNK, CHUNK), CHUNK)
        return pltpu.make_async_remote_copy(
            src_ref=norm.at[src], dst_ref=norm.at[dst], send_sem=row_send.at[i], recv_sem=row_recv.at[i],
            device_id={'sp': sib}, device_id_type=MESH)

    def first_mlp(i, carry):
        rows = pl.ds(pl.multiple_of(i * CHUNK, CHUNK), CHUNK)
        val = mlp(rows, hid, o_t, proj[0], up[0], down[0])
        hid[rows, :] = val
        norm[rows, :] = layer_norm(val)

        @pl.when(i > 0)
        def _():
            row_copy(i - 1).start()

        return carry

    lax.fori_loop(0, steps, first_mlp, 0)
    queries(1)
    row_copy(steps - 1).start()
    keys(1, 0, OWN)
    for i in range(steps):
        row_copy(i).wait()
    keys(1, OWN, OWN)

    early = 2 * Q_BLK
    attention(0, early, q_3, k_n, k_dup, v_t, o_t, s_even, s_odd)

    def last_rows(rows):
        fin[rows, :] = layer_norm(mlp(rows, hid, o_t, proj[1], up[1], down[1]))

    fill_rows(0, early, CHUNK, last_rows)
    send = pltpu.make_async_remote_copy(
        src_ref=fin.at[pl.ds(0, TOK)], dst_ref=both_ref.at[chip], send_sem=fin_send, recv_sem=fin_recv,
        device_id={'sp': peer}, device_id_type=MESH)
    send.start()
    attention(early, OWN - early, q_3, k_n, k_dup, v_t, o_t, s_even, s_odd)
    fill_rows(early, OWN - early, CHUNK, last_rows)
    both_ref[chip] = fin[TOK:OWN]
    send.wait()


def decode(z, rank, pos, pos_x, wqkv, wproj, wup, wdown):
    return pl.pallas_call(
        decoder_kernel,
        out_shape=jax.ShapeDtypeStruct((CLIPS, TOK, DDIM), BF16),
        in_specs=[VMEM] * 4 + [ANY] * 4,
        out_specs=VMEM,
        scratch_shapes=[
            pltpu.VMEM((LAYERS, 3 * DDIM, DDIM), BF16),
            pltpu.VMEM((LAYERS, DDIM, DDIM), BF16),
            pltpu.VMEM((LAYERS, DDIM, 4 * DDIM), BF16),
            pltpu.VMEM((LAYERS, 4 * DDIM, DDIM), BF16),
            pltpu.VMEM((OWN, DDIM), BF16),
            pltpu.VMEM((SEQ, DDIM), BF16),
            pltpu.VMEM((OWN, DDIM), BF16),
            pltpu.VMEM((DEC_HEADS, 4 * HEAD, OWN), BF16),
            pltpu.VMEM((SEQ, DDIM), BF16),
            pltpu.VMEM((SEQ, 2 * DDIM), BF16),
            pltpu.VMEM((DDIM, SEQ), BF16),
            pltpu.VMEM((DDIM, OWN), BF16),
            pltpu.VMEM((SEQ, Q_BLK), F32),
            pltpu.VMEM((SEQ, Q_BLK), F32),
            pltpu.SemaphoreType.DMA((LAYERS * 4,)),
            pltpu.SemaphoreType.REGULAR,
            pltpu.SemaphoreType.DMA((OWN // CHUNK,)),
            pltpu.SemaphoreType.DMA((OWN // CHUNK,)),
            pltpu.SemaphoreType.DMA,
            pltpu.SemaphoreType.DMA,
        ],
        compiler_params=pltpu.CompilerParams(collective_id=1, has_side_effects=True, vmem_limit_bytes=58 * 2 ** 20),
        cost_estimate=pl.CostEstimate(flops=60 * 10 ** 9, bytes_accessed=2 * 10 ** 7, transcendentals=6 * 10 ** 7),
        name='decoder',
    )(z, rank, pos, pos_x, wqkv, wproj, wup, wdown)


def solution(mesh):
    def local_program(patches, vis_mask, enc_pos, dec_pos, w_pe, b_pe, enc_qkv, enc_proj, enc_up, enc_down, w_ed, mask_token, dec_qkv, dec_proj, dec_up, dec_down, w_out):
        enc_qkv_t = jnp.transpose(enc_qkv, (0, 2, 3, 4, 1)).reshape(LAYERS, 3 * DIM, DIM)
        dec_qkv_t = jnp.transpose(dec_qkv, (0, 2, 3, 4, 1)).reshape(LAYERS, 3 * DDIM, DDIM)
        enc_proj2 = enc_proj.reshape(LAYERS, DIM, DIM)
        dec_proj2 = dec_proj.reshape(LAYERS, DDIM, DDIM)
        z, rank, pos_x = encode(vis_mask, b_pe.reshape(1, DIM), mask_token.reshape(1, DDIM), patches, enc_pos, w_pe, dec_pos, w_ed,
                                enc_qkv_t, enc_proj2, enc_up, enc_down)
        both = decode(z, rank, dec_pos, pos_x, dec_qkv_t, dec_proj2, dec_up, dec_down)
        return jnp.einsum('cne,ep->cnp', both, w_out, preferred_element_type=F32)

    row_spec = P('dp', 'sp', None)
    pos_spec = P(('dp', 'sp'), None)
    arg_specs = (row_spec, P('dp', 'sp'), pos_spec, pos_spec) + (P(),) * 13
    return jax.shard_map(local_program, mesh=mesh, in_specs=arg_specs, out_specs=row_spec, check_vma=False)
```

```python
import functools
import math

import jax
import jax.numpy as jnp
from jax import lax
from jax.experimental import pallas as pl
from jax.experimental.pallas import tpu as pltpu
from jax.sharding import PartitionSpec as P

F32 = jnp.float32
BF16 = jnp.bfloat16
MESH = pl.DeviceIdType.MESH
VMEM = pl.BlockSpec(memory_space=pltpu.VMEM)
ANY = pl.BlockSpec(memory_space=pl.ANY)

SP = 4
CLIPS = 2
TOK = 768
PATCH = 1536
DIM = 768
ENC_HEADS = 12
HEAD = 64
DDIM = 384
DEC_HEADS = 6
VIS = 96
WIN = 2 * VIS
ROWS = SP * VIS
OWN = 2 * TOK
SEQ = SP * TOK
LAYERS = 2
EXP_SCALE = HEAD ** -0.5 * math.log2(math.e)


def dot(lhs, rhs):
    return jnp.dot(lhs, rhs, preferred_element_type=F32)


def dot_nt(lhs, rhs):
    return lax.dot_general(lhs, rhs, (((1,), (1,)), ((), ())), preferred_element_type=F32)


def dot_tn(lhs, rhs):
    return lax.dot_general(lhs, rhs, (((0,), (0,)), ((), ())), preferred_element_type=F32)


def layer_norm(hidden):
    hid = hidden.astype(F32)
    centred = hid - jnp.mean(hid, axis=-1, keepdims=True)
    var = jnp.mean(centred * centred, axis=-1, keepdims=True)
    return (centred * lax.rsqrt(var + 1e-6)).astype(BF16)


def gelu(val):
    return (0.5 * val * (1.0 + lax.erf(val * math.sqrt(0.5)))).astype(BF16)


def col_max(val):
    return jnp.max(val, axis=0, keepdims=True)


def col_sum(val):
    return jnp.sum(val, axis=0, keepdims=True)


MINE = ROWS // 2
Q_PAD = 256


def encoder_kernel(mask_ref, bpe_ref, token_ref, patch_hbm, pos_hbm, wpe_hbm, dec_pos_hbm, wed_ref, qkv_hbm, proj_hbm, up_hbm, down_hbm,
                   z_ref, rank_ref, pos_out,
                   patch, pos, wpe, qkv, proj, up, down, masks, sendbuf, win, hall, hid, norm, norm_q, q_t, k_n, v_t, o_t,
                   in_sem, w_sem, mask_send, mask_recv, win_send, win_recv, pos_send, pos_recv, row_send, row_recv):
    me = lax.axis_index('sp')
    chip = me // 2
    core = me - 2 * chip
    peer = lax.rem(me + 2, SP)
    sib = me + 1 - 2 * core
    diag = lax.rem(sib + 2, SP)

    loads = [pltpu.make_async_copy(src, dst, in_sem.at[idx])
             for idx, (src, dst) in enumerate(((patch_hbm, patch), (wpe_hbm, wpe), (pos_hbm, pos)))]
    for copy in loads:
        copy.start()
    barrier = pltpu.get_barrier_semaphore()
    for other in (peer, sib, diag):
        pl.semaphore_signal(barrier, inc=1, device_id={'sp': other}, device_id_type=MESH)
    order_row = lax.broadcasted_iota(jnp.int32, (TOK, TOK), 0)
    order_col = lax.broadcasted_iota(jnp.int32, (TOK, TOK), 1)
    before = jnp.where(order_row < order_col, 1.0, 0.0).astype(BF16)
    mine = mask_ref[...].astype(F32)
    mine_rank = dot(jnp.concatenate([mine] * SP, axis=0).astype(BF16), before)[0:CLIPS]
    slot_of = jnp.where(mine > 0.0, mine_rank, -1.0)
    pl.semaphore_wait(barrier, 3)

    def send(src, dst, send_sem, recv_sem, dev):
        copy = pltpu.make_async_remote_copy(
            src_ref=src, dst_ref=dst, send_sem=send_sem, recv_sem=recv_sem, device_id={'sp': dev}, device_id_type=MESH)
        copy.start()
        return copy

    mask_copies = [send(mask_ref, masks.at[step - 1], mask_send.at[step - 1], mask_recv.at[step - 1], lax.rem(me + step, SP))
                   for step in range(1, SP)]
    for copy in loads:
        copy.wait()
    copies = []
    for layer in range(LAYERS):
        for idx, (src, dst) in enumerate(((qkv_hbm, qkv), (proj_hbm, proj), (up_hbm, up), (down_hbm, down))):
            copy = pltpu.make_async_copy(src.at[layer], dst.at[layer], w_sem.at[layer * 4 + idx])
            copy.start()
            copies.append(copy)

    bias = bpe_ref[...].astype(F32).reshape(1, DIM)

    def window(clip, slots):
        rows = lax.broadcasted_iota(jnp.int32, (WIN, TOK), 0).astype(F32)
        hit = jnp.where(rows == slots, 1.0, 0.0)
        select = hit.astype(BF16)
        moved = dot(select, patch[clip]).astype(BF16)
        occupied = jnp.sum(hit, axis=1, keepdims=True)
        emb = dot(moved, wpe[...]) + occupied * bias + dot(select, pos[...])
        return emb.astype(BF16)

    far = jnp.where(chip == 0, slot_of[1:2], slot_of[0:1])
    near = jnp.where(chip == 0, slot_of[0:1], slot_of[1:2])
    sendbuf[...] = window(1 - chip, far)
    to_peer = send(sendbuf, win.at[1], win_send.at[0], win_recv.at[0], peer)
    win[0] = window(chip, near)
    to_sib = send(win.at[0], win.at[2], win_send.at[1], win_recv.at[1], sib)

    for copy in mask_copies:
        copy.wait()
    stacked = jnp.concatenate([mine] + [masks[k].astype(F32) for k in range(SP - 1)], axis=0)
    local = dot(stacked.astype(BF16), before)
    counts = jnp.sum(stacked, axis=1, keepdims=True)
    row_dev = lax.rem(me - lax.broadcasted_iota(jnp.int32, (CLIPS * SP, 1), 0) // CLIPS + SP, SP)
    base = jnp.zeros((CLIPS * SP, 1), F32)
    for k in range(SP):
        dev_k = lax.rem(me - k + SP, SP)
        tiled = jnp.concatenate([counts[CLIPS * k:CLIPS * k + CLIPS]] * SP, axis=0)
        base = base + jnp.where(dev_k < row_dev, tiled, 0.0)
    rank_ref[...] = jnp.where(stacked > 0.0, local + base, float(ROWS)).astype(jnp.int32)

    def placement(slot):
        def pick(val):
            two = val[CLIPS * slot:CLIPS * slot + CLIPS]
            return jnp.where(chip == 0, two[0:1], two[1:2])

        start, size = pick(base), pick(counts)
        rows = lax.broadcasted_iota(jnp.int32, (ROWS, WIN), 0).astype(F32)
        cols = lax.broadcasted_iota(jnp.int32, (ROWS, WIN), 1).astype(F32)
        return jnp.where((rows == cols + start) & (cols < size), 1.0, 0.0)

    even = core == 0
    left, right = placement(1), placement(3)
    place = [placement(0), placement(2), jnp.where(even, right, left), jnp.where(even, left, right)]
    to_peer.wait_recv()
    relay = send(win.at[1], win.at[3], win_send.at[2], win_recv.at[2], sib)
    pos_peer = send(dec_pos_hbm, pos_out.at[0], pos_send.at[0], pos_recv.at[0], peer)
    pos_sib = send(dec_pos_hbm, pos_out.at[1], pos_send.at[1], pos_recv.at[1], sib)
    total = dot(place[0].astype(BF16), win[0]) + dot(place[1].astype(BF16), win[1])
    to_sib.wait_recv()
    total = total + dot(place[2].astype(BF16), win[2])
    relay.wait_recv()
    total = total + dot(place[3].astype(BF16), win[3])
    hall[...] = total.astype(BF16)
    own = pl.ds(pl.multiple_of(core * MINE, MINE), MINE)
    hid[...] = hall[own, :]
    norm[0] = layer_norm(hall[...])
    norm_q[MINE:] = jnp.zeros((Q_PAD - MINE, DIM), BF16)
    zero = jnp.zeros((HEAD, Q_PAD), BF16)
    pos_diag = swap = None

    for layer in range(LAYERS):
        copies[layer * 4].wait()
        norm_q[0:MINE] = norm[layer, own, :]
        q_t[...] = dot_nt(qkv[layer, 0:DIM], norm_q[...]).astype(BF16)
        if swap is not None:
            swap.wait()
        k_n[...] = dot_nt(norm[layer], qkv[layer, DIM:2 * DIM]).astype(BF16)
        v_t[...] = dot_nt(qkv[layer, 2 * DIM:3 * DIM], norm[layer]).astype(BF16)

        def heads(group, carry):
            scores, weights = [], []
            for pair in range(2):
                lanes = pl.ds(pl.multiple_of((2 * group + pair) * 2 * HEAD, 2 * HEAD), 2 * HEAD)
                for odd in range(2):
                    rows = pl.ds(pl.multiple_of((4 * group + 2 * pair + odd) * HEAD, HEAD), HEAD)
                    q_head = q_t[rows, :]
                    q_both = jnp.concatenate([zero, q_head] if odd else [q_head, zero], axis=0)
                    scores.append(dot(k_n[:, lanes], q_both))
            for s in scores:
                e = jnp.exp2(s * EXP_SCALE - col_max(s) * EXP_SCALE)
                weights.append((e.astype(BF16), 1.0 / col_sum(e)))
            for idx, (e, scale) in enumerate(weights):
                rows = pl.ds(pl.multiple_of((4 * group + idx) * HEAD, HEAD), HEAD)
                o_t[rows, :] = (dot(v_t[rows, :], e) * scale).astype(BF16)
            return carry

        lax.fori_loop(0, ENC_HEADS // 4, heads, 0)
        copies[layer * 4 + 1].wait()
        mid = (hid[...].astype(F32) + dot_tn(o_t[...], proj[layer])[0:MINE]).astype(BF16)
        rows_norm = layer_norm(mid)
        copies[layer * 4 + 2].wait()
        copies[layer * 4 + 3].wait()
        if layer == LAYERS - 1:
            pos_peer.wait_recv()
            pos_diag = send(pos_out.at[0], pos_out.at[2], pos_send.at[2], pos_recv.at[2], sib)
        acc = None
        for lo in range(0, 4 * DIM, DIM):
            act = gelu(dot(rows_norm, up[layer, :, lo:lo + DIM]))
            part = dot(act, down[layer, lo:lo + DIM, :])
            acc = part if acc is None else acc + part
        out = (mid.astype(F32) + acc).astype(BF16)
        if layer < LAYERS - 1:
            hid[...] = out
            norm[layer + 1, own, :] = layer_norm(out)
            swap = send(norm.at[layer + 1, own], norm.at[layer + 1, own], row_send.at[layer], row_recv.at[layer], sib)
    z_ref[own, :] = dot(layer_norm(out), wed_ref[...]).astype(BF16)
    first = lax.broadcasted_iota(jnp.int32, (2 * HEAD, DDIM), 0) == 0
    z_ref[ROWS:] = jnp.where(first, token_ref[...].astype(F32).reshape(1, DDIM), 0.0).astype(BF16)
    last = send(z_ref.at[own], z_ref.at[own], row_send.at[LAYERS - 1], row_recv.at[LAYERS - 1], sib)
    to_peer.wait_send()
    to_sib.wait_send()
    relay.wait_send()
    pos_peer.wait_send()
    pos_sib.wait()
    pos_diag.wait()
    last.wait()


def encode(mask, bpe, token, patches, enc_pos, wpe, dec_pos, wed, qkv_t, proj, up, down):
    return pl.pallas_call(
        encoder_kernel,
        out_shape=(
            jax.ShapeDtypeStruct((ROWS + 2 * HEAD, DDIM), BF16),
            jax.ShapeDtypeStruct((CLIPS * SP, TOK), jnp.int32),
            jax.ShapeDtypeStruct((SP - 1, TOK, DDIM), BF16),
        ),
        in_specs=[VMEM] * 3 + [ANY] * 4 + [VMEM] + [ANY] * 4,
        out_specs=(VMEM, VMEM, ANY),
        scratch_shapes=[
            pltpu.VMEM((CLIPS, TOK, PATCH), BF16),
            pltpu.VMEM((TOK, DIM), BF16),
            pltpu.VMEM((PATCH, DIM), BF16),
            pltpu.VMEM((LAYERS, 3 * DIM, DIM), BF16),
            pltpu.VMEM((LAYERS, DIM, DIM), BF16),
            pltpu.VMEM((LAYERS, DIM, 4 * DIM), BF16),
            pltpu.VMEM((LAYERS, 4 * DIM, DIM), BF16),
            pltpu.VMEM((SP - 1, CLIPS, TOK), jnp.int32),
            pltpu.VMEM((WIN, DIM), BF16),
            pltpu.VMEM((SP, WIN, DIM), BF16),
            pltpu.VMEM((ROWS, DIM), BF16),
            pltpu.VMEM((MINE, DIM), BF16),
            pltpu.VMEM((LAYERS, ROWS, DIM), BF16),
            pltpu.VMEM((Q_PAD, DIM), BF16),
            pltpu.VMEM((DIM, Q_PAD), BF16),
            pltpu.VMEM((ROWS, DIM), BF16),
            pltpu.VMEM((DIM, ROWS), BF16),
            pltpu.VMEM((DIM, Q_PAD), BF16),
            pltpu.SemaphoreType.DMA((3,)),
            pltpu.SemaphoreType.DMA((LAYERS * 4,)),
            pltpu.SemaphoreType.DMA((SP - 1,)),
            pltpu.SemaphoreType.DMA((SP - 1,)),
            pltpu.SemaphoreType.DMA((3,)),
            pltpu.SemaphoreType.DMA((3,)),
            pltpu.SemaphoreType.DMA((3,)),
            pltpu.SemaphoreType.DMA((3,)),
            pltpu.SemaphoreType.DMA((LAYERS,)),
            pltpu.SemaphoreType.DMA((LAYERS,)),
        ],
        compiler_params=pltpu.CompilerParams(collective_id=0, has_side_effects=True, vmem_limit_bytes=58 * 2 ** 20),
        cost_estimate=pl.CostEstimate(flops=12 * 10 ** 9, bytes_accessed=4 * 10 ** 7, transcendentals=0),
        name='encoder',
    )(mask, bpe, token, patches, enc_pos, wpe, dec_pos, wed, qkv_t, proj, up, down)


Q_BLK = 512
K_BLK = 256
CHUNK = 256
WIDE = 512
PAIR = 2 * HEAD


def fill_rows(start, count, step, body):
    def run(i, carry):
        body(pl.ds(pl.multiple_of(start + i * step, step), step))
        return carry

    lax.fori_loop(0, count // step, run, 0)


def make_queries(rows, norm, w_q, q_3):
    q = dot_nt(w_q, norm[rows, :]).astype(BF16).astype(F32) * EXP_SCALE
    hi = q.astype(BF16)
    rest = q - hi.astype(F32)
    mid = rest.astype(BF16)
    low = (rest - mid.astype(F32)).astype(BF16)
    zero = jnp.zeros((HEAD, q.shape[1]), BF16)
    for head in range(DEC_HEADS):
        part = slice(head * HEAD, (head + 1) * HEAD)
        tail = (low[part], zero) if head % 2 == 0 else (zero, low[part])
        for idx, val in enumerate((hi[part], mid[part]) + tail):
            q_3[head, idx * HEAD:(idx + 1) * HEAD, rows] = val


def make_keys(rows, norm, w_k, w_v, k_n, k_dup, v_t):
    a = norm[rows, :]
    k = dot_nt(a, w_k)
    k_n[rows, :] = k.astype(BF16)
    first = lax.broadcasted_iota(jnp.int32, (k.shape[0], PAIR), 1) < HEAD
    for pair in range(DEC_HEADS // 2):
        both = k[:, pair * PAIR:(pair + 1) * PAIR]
        turned = pltpu.roll(both, HEAD, axis=1)
        k_dup[rows, 2 * pair * PAIR:(2 * pair + 1) * PAIR] = jnp.where(first, both, turned).astype(BF16)
        k_dup[rows, (2 * pair + 1) * PAIR:(2 * pair + 2) * PAIR] = jnp.where(first, turned, both).astype(BF16)
    v_t[:, rows] = dot_nt(w_v, a).astype(BF16)


def attention(start, count, q_3, k_n, k_dup, v_t, o_t, s_even, s_odd):
    blocks = count // Q_BLK
    units = DEC_HEADS * blocks

    def place(unit):
        head = unit // blocks
        return head, pl.ds(pl.multiple_of(start + (unit - head * blocks) * Q_BLK, Q_BLK), Q_BLK)

    def mixed(unit_q, s_q, unit_p, s_p, max8):
        if unit_q is not None:
            head_q, cols_q = place(unit_q)
            q = q_3[head_q, :, cols_q]
            lanes = pl.ds(pl.multiple_of((head_q // 2) * PAIR, PAIR), PAIR)
            lanes_dup = pl.ds(pl.multiple_of(head_q * PAIR, PAIR), PAIR)
        if unit_p is not None:
            head_p, cols_p = place(unit_p)
            shift = col_max(max8)
            v_rows = pl.ds(pl.multiple_of(head_p * HEAD, HEAD), HEAD)
        new_max = total = late = None
        accs = [None, None]

        def weigh(idx, weights):
            o = dot(v_t[v_rows, idx * K_BLK:(idx + 1) * K_BLK], weights)
            accs[idx % 2] = o if accs[idx % 2] is None else accs[idx % 2] + o

        for idx in range(SEQ // K_BLK):
            rows = slice(idx * K_BLK, (idx + 1) * K_BLK)
            if unit_p is not None:
                e = jnp.exp2(s_p[rows, :] - shift)
                t = jnp.sum(e.reshape(K_BLK // 8, 8, Q_BLK), axis=0)
                total = t if total is None else total + t
                if late is not None:
                    weigh(*late)
                late = (idx, e.astype(BF16))
            if unit_q is not None:
                keys = jnp.concatenate([k_dup[rows, lanes_dup], k_n[rows, lanes]], axis=1)
                s = dot(keys, q)
                s_q[rows, :] = s
                m = jnp.max(s.reshape(K_BLK // 8, 8, Q_BLK), axis=0)
                new_max = m if new_max is None else jnp.maximum(new_max, m)
        if unit_p is not None:
            weigh(*late)
            o_t[v_rows, cols_p] = ((accs[0] + accs[1]) * (1.0 / col_sum(total))).astype(BF16)
        return new_max

    first = mixed(0, s_even, None, None, None)

    def body(i, max8):
        unit = 2 * i
        max_odd = mixed(unit + 1, s_odd, unit, s_even, max8)
        return mixed(jnp.minimum(unit + 2, units - 1), s_even, unit + 1, s_odd, max_odd)

    lax.fori_loop(0, units // 2, body, first)


def mlp(rows, hid, o_t, w_proj, w_up, w_down):
    mid = (hid[rows, :].astype(F32) + dot_tn(o_t[:, rows], w_proj)).astype(BF16)
    act = gelu(dot(layer_norm(mid), w_up))
    return (mid.astype(F32) + dot(act, w_down)).astype(BF16)


def decoder_kernel(z_ref, rank_ref, pos_me, pos_x, qkv_hbm, proj_hbm, up_hbm, down_hbm, both_ref,
                   qkv, proj, up, down, hid, norm, fin, q_3, k_n, k_dup, v_t, o_t, s_even, s_odd, w_sem, ready, row_send, row_recv, fin_send, fin_recv):
    me = lax.axis_index('sp')
    chip = me // 2
    core = me - 2 * chip
    peer = lax.rem(me + 2, SP)
    sib = me + 1 - 2 * core
    diag = lax.rem(sib + 2, SP)

    copies = []
    for layer in range(LAYERS):
        for idx, (src, dst) in enumerate(((qkv_hbm, qkv), (proj_hbm, proj), (up_hbm, up), (down_hbm, down))):
            copy = pltpu.make_async_copy(src.at[layer], dst.at[layer], w_sem.at[layer * 4 + idx])
            copy.start()
            copies.append(copy)
    barrier = pltpu.get_barrier_semaphore()
    for other in (peer, sib):
        pl.semaphore_signal(barrier, inc=1, device_id={'sp': other}, device_id_type=MESH)
    pl.semaphore_wait(barrier, 2)

    def tokens(dev, pos):
        slot = lax.rem(me - dev + SP, SP)
        rank = rank_ref[pl.ds(2 * slot + chip, 1), :]
        rank_col = jnp.transpose(jnp.broadcast_to(rank.astype(F32), (8, TOK)))[:, 0:1]
        lanes = lax.broadcasted_iota(jnp.int32, (TOK, ROWS + 2 * HEAD), 1).astype(F32)
        select = jnp.where(lanes == rank_col, 1.0, 0.0).astype(BF16)
        return (dot(select, z_ref[...]) + pos.astype(F32)).astype(BF16)

    hid[0:TOK] = tokens(peer, pos_x[0])
    hid[TOK:OWN] = tokens(me, pos_me[...])
    norm[OWN:OWN + TOK] = layer_norm(tokens(diag, pos_x[2]))
    norm[OWN + TOK:SEQ] = layer_norm(tokens(sib, pos_x[1]))

    def own_norm(rows):
        norm[rows, :] = layer_norm(hid[rows, :])

    fill_rows(0, OWN, CHUNK, own_norm)

    def queries(layer):
        fill_rows(0, OWN, WIDE, lambda rows: make_queries(rows, norm, qkv[layer, 0:DDIM], q_3))

    def keys(layer, start, count):
        fill_rows(start, count, WIDE, lambda rows: make_keys(
            rows, norm, qkv[layer, DDIM:2 * DDIM], qkv[layer, 2 * DDIM:3 * DDIM], k_n, k_dup, v_t))

    copies[0].wait()
    queries(0)
    keys(0, 0, SEQ)
    pl.semaphore_signal(ready, inc=1, device_id={'sp': sib}, device_id_type=MESH)
    attention(0, OWN, q_3, k_n, k_dup, v_t, o_t, s_even, s_odd)
    pl.semaphore_wait(ready, 1)
    for copy in copies[1:]:
        copy.wait()
    steps = OWN // CHUNK

    def row_copy(i):
        src = pl.ds(pl.multiple_of(i * CHUNK, CHUNK), CHUNK)
        dst = pl.ds(pl.multiple_of(OWN + i * CHUNK, CHUNK), CHUNK)
        return pltpu.make_async_remote_copy(
            src_ref=norm.at[src], dst_ref=norm.at[dst], send_sem=row_send.at[i], recv_sem=row_recv.at[i],
            device_id={'sp': sib}, device_id_type=MESH)

    def first_mlp(i, carry):
        rows = pl.ds(pl.multiple_of(i * CHUNK, CHUNK), CHUNK)
        val = mlp(rows, hid, o_t, proj[0], up[0], down[0])
        hid[rows, :] = val
        norm[rows, :] = layer_norm(val)

        @pl.when(i > 0)
        def _():
            row_copy(i - 1).start()

        return carry

    lax.fori_loop(0, steps, first_mlp, 0)
    queries(1)
    row_copy(steps - 1).start()
    keys(1, 0, OWN)
    for i in range(steps):
        row_copy(i).wait()
    keys(1, OWN, OWN)

    early = 2 * Q_BLK
    attention(0, early, q_3, k_n, k_dup, v_t, o_t, s_even, s_odd)

    def last_rows(rows):
        fin[rows, :] = layer_norm(mlp(rows, hid, o_t, proj[1], up[1], down[1]))

    fill_rows(0, early, CHUNK, last_rows)
    send = pltpu.make_async_remote_copy(
        src_ref=fin.at[pl.ds(0, TOK)], dst_ref=both_ref.at[chip], send_sem=fin_send, recv_sem=fin_recv,
        device_id={'sp': peer}, device_id_type=MESH)
    send.start()
    attention(early, OWN - early, q_3, k_n, k_dup, v_t, o_t, s_even, s_odd)
    fill_rows(early, OWN - early, CHUNK, last_rows)
    both_ref[chip] = fin[TOK:OWN]
    send.wait()


def decode(z, rank, pos, pos_x, wqkv, wproj, wup, wdown):
    return pl.pallas_call(
        decoder_kernel,
        out_shape=jax.ShapeDtypeStruct((CLIPS, TOK, DDIM), BF16),
        in_specs=[VMEM] * 4 + [ANY] * 4,
        out_specs=VMEM,
        scratch_shapes=[
            pltpu.VMEM((LAYERS, 3 * DDIM, DDIM), BF16),
            pltpu.VMEM((LAYERS, DDIM, DDIM), BF16),
            pltpu.VMEM((LAYERS, DDIM, 4 * DDIM), BF16),
            pltpu.VMEM((LAYERS, 4 * DDIM, DDIM), BF16),
            pltpu.VMEM((OWN, DDIM), BF16),
            pltpu.VMEM((SEQ, DDIM), BF16),
            pltpu.VMEM((OWN, DDIM), BF16),
            pltpu.VMEM((DEC_HEADS, 4 * HEAD, OWN), BF16),
            pltpu.VMEM((SEQ, DDIM), BF16),
            pltpu.VMEM((SEQ, 2 * DDIM), BF16),
            pltpu.VMEM((DDIM, SEQ), BF16),
            pltpu.VMEM((DDIM, OWN), BF16),
            pltpu.VMEM((SEQ, Q_BLK), F32),
            pltpu.VMEM((SEQ, Q_BLK), F32),
            pltpu.SemaphoreType.DMA((LAYERS * 4,)),
            pltpu.SemaphoreType.REGULAR,
            pltpu.SemaphoreType.DMA((OWN // CHUNK,)),
            pltpu.SemaphoreType.DMA((OWN // CHUNK,)),
            pltpu.SemaphoreType.DMA,
            pltpu.SemaphoreType.DMA,
        ],
        compiler_params=pltpu.CompilerParams(collective_id=1, has_side_effects=True, vmem_limit_bytes=58 * 2 ** 20),
        cost_estimate=pl.CostEstimate(flops=60 * 10 ** 9, bytes_accessed=2 * 10 ** 7, transcendentals=6 * 10 ** 7),
        name='decoder',
    )(z, rank, pos, pos_x, wqkv, wproj, wup, wdown)


OUT_ROWS = 256


def output_kernel(both_ref, w_ref, out_ref):
    out_ref[...] = dot(both_ref[...], w_ref[...])


def project(both, w_out):
    rows = both.reshape(CLIPS * TOK, DDIM)
    out = pl.pallas_call(
        output_kernel,
        grid=(CLIPS * TOK // OUT_ROWS,),
        out_shape=jax.ShapeDtypeStruct((CLIPS * TOK, PATCH), F32),
        in_specs=[pl.BlockSpec((OUT_ROWS, DDIM), lambda i: (i, 0)), pl.BlockSpec((DDIM, PATCH), lambda i: (0, 0))],
        out_specs=pl.BlockSpec((OUT_ROWS, PATCH), lambda i: (i, 0)),
        cost_estimate=pl.CostEstimate(flops=2 * 10 ** 9, bytes_accessed=12 * 10 ** 6, transcendentals=0),
        name='output',
    )(rows, w_out)
    return out.reshape(CLIPS, TOK, PATCH)


def solution(mesh):
    def local_program(patches, vis_mask, enc_pos, dec_pos, w_pe, b_pe, enc_qkv, enc_proj, enc_up, enc_down, w_ed, mask_token, dec_qkv, dec_proj, dec_up, dec_down, w_out):
        enc_qkv_t = jnp.transpose(enc_qkv, (0, 2, 3, 4, 1)).reshape(LAYERS, 3 * DIM, DIM)
        dec_qkv_t = jnp.transpose(dec_qkv, (0, 2, 3, 4, 1)).reshape(LAYERS, 3 * DDIM, DDIM)
        enc_proj2 = enc_proj.reshape(LAYERS, DIM, DIM)
        dec_proj2 = dec_proj.reshape(LAYERS, DDIM, DDIM)
        z, rank, pos_x = encode(vis_mask, b_pe, mask_token, patches, enc_pos, w_pe, dec_pos, w_ed,
                                enc_qkv_t, enc_proj2, enc_up, enc_down)
        both = decode(z, rank, dec_pos, pos_x, dec_qkv_t, dec_proj2, dec_up, dec_down)
        return project(both, w_out)

    row_spec = P('dp', 'sp', None)
    pos_spec = P(('dp', 'sp'), None)
    arg_specs = (row_spec, P('dp', 'sp'), pos_spec, pos_spec) + (P(),) * 13
    return jax.shard_map(local_program, mesh=mesh, in_specs=arg_specs, out_specs=row_spec, check_vma=False)
```

```python
import functools
import math

import jax
import jax.numpy as jnp
from jax import lax
from jax.experimental import pallas as pl
from jax.experimental.pallas import tpu as pltpu
from jax.sharding import PartitionSpec as P

F32 = jnp.float32
BF16 = jnp.bfloat16
MESH = pl.DeviceIdType.MESH
VMEM = pl.BlockSpec(memory_space=pltpu.VMEM)
ANY = pl.BlockSpec(memory_space=pl.ANY)

SP = 4
CLIPS = 2
TOK = 768
PATCH = 1536
DIM = 768
ENC_HEADS = 12
HEAD = 64
DDIM = 384
DEC_HEADS = 6
VIS = 96
WIN = 2 * VIS
ROWS = SP * VIS
OWN = 2 * TOK
SEQ = SP * TOK
LAYERS = 2
EXP_SCALE = HEAD ** -0.5 * math.log2(math.e)


def dot(lhs, rhs):
    return jnp.dot(lhs, rhs, preferred_element_type=F32)


def dot_nt(lhs, rhs):
    return lax.dot_general(lhs, rhs, (((1,), (1,)), ((), ())), preferred_element_type=F32)


def dot_tn(lhs, rhs):
    return lax.dot_general(lhs, rhs, (((0,), (0,)), ((), ())), preferred_element_type=F32)


def layer_norm(hidden):
    hid = hidden.astype(F32)
    centred = hid - jnp.mean(hid, axis=-1, keepdims=True)
    var = jnp.mean(centred * centred, axis=-1, keepdims=True)
    return (centred * lax.rsqrt(var + 1e-6)).astype(BF16)


def gelu(val):
    return (0.5 * val * (1.0 + lax.erf(val * math.sqrt(0.5)))).astype(BF16)


def col_max(val):
    return jnp.max(val, axis=0, keepdims=True)


def col_sum(val):
    return jnp.sum(val, axis=0, keepdims=True)


MINE = ROWS // 2
Q_PAD = 256


def encoder_kernel(mask_ref, bpe_ref, token_ref, patch_hbm, pos_hbm, wpe_hbm, dec_pos_hbm, wed_ref, qkv_hbm, proj_hbm, up_hbm, down_hbm,
                   z_ref, rank_ref, pos_out,
                   patch, pos, wpe, qkv, proj, up, down, masks, sendbuf, win, hall, hid, norm, norm_q, q_t, k_n, v_t, o_t,
                   in_sem, w_sem, mask_send, mask_recv, win_send, win_recv, pos_send, pos_recv, row_send, row_recv):
    me = lax.axis_index('sp')
    chip = me // 2
    core = me - 2 * chip
    peer = lax.rem(me + 2, SP)
    sib = me + 1 - 2 * core
    diag = lax.rem(sib + 2, SP)

    loads = [pltpu.make_async_copy(src, dst, in_sem.at[idx])
             for idx, (src, dst) in enumerate(((patch_hbm, patch), (wpe_hbm, wpe), (pos_hbm, pos)))]
    for copy in loads:
        copy.start()
    barrier = pltpu.get_barrier_semaphore()
    for other in (peer, sib, diag):
        pl.semaphore_signal(barrier, inc=1, device_id={'sp': other}, device_id_type=MESH)
    order_row = lax.broadcasted_iota(jnp.int32, (TOK, TOK), 0)
    order_col = lax.broadcasted_iota(jnp.int32, (TOK, TOK), 1)
    before = jnp.where(order_row < order_col, 1.0, 0.0).astype(BF16)
    mine = mask_ref[...].astype(F32)
    mine_rank = dot(jnp.concatenate([mine] * SP, axis=0).astype(BF16), before)[0:CLIPS]
    slot_of = jnp.where(mine > 0.0, mine_rank, -1.0)
    pl.semaphore_wait(barrier, 3)

    def send(src, dst, send_sem, recv_sem, dev):
        copy = pltpu.make_async_remote_copy(
            src_ref=src, dst_ref=dst, send_sem=send_sem, recv_sem=recv_sem, device_id={'sp': dev}, device_id_type=MESH)
        copy.start()
        return copy

    mask_copies = [send(mask_ref, masks.at[step - 1], mask_send.at[step - 1], mask_recv.at[step - 1], lax.rem(me + step, SP))
                   for step in range(1, SP)]
    for copy in loads:
        copy.wait()
    copies = []
    for layer in range(LAYERS):
        for idx, (src, dst) in enumerate(((qkv_hbm, qkv), (proj_hbm, proj), (up_hbm, up), (down_hbm, down))):
            copy = pltpu.make_async_copy(src.at[layer], dst.at[layer], w_sem.at[layer * 4 + idx])
            copy.start()
            copies.append(copy)

    bias = bpe_ref[...].astype(F32).reshape(1, DIM)

    def window(clip, slots):
        rows = lax.broadcasted_iota(jnp.int32, (WIN, TOK), 0).astype(F32)
        hit = jnp.where(rows == slots, 1.0, 0.0)
        select = hit.astype(BF16)
        moved = dot(select, patch[clip]).astype(BF16)
        occupied = jnp.sum(hit, axis=1, keepdims=True)
        emb = dot(moved, wpe[...]) + occupied * bias + dot(select, pos[...])
        return emb.astype(BF16)

    far = jnp.where(chip == 0, slot_of[1:2], slot_of[0:1])
    near = jnp.where(chip == 0, slot_of[0:1], slot_of[1:2])
    sendbuf[...] = window(1 - chip, far)
    to_peer = send(sendbuf, win.at[1], win_send.at[0], win_recv.at[0], peer)
    win[0] = window(chip, near)
    to_sib = send(win.at[0], win.at[2], win_send.at[1], win_recv.at[1], sib)

    for copy in mask_copies:
        copy.wait()
    stacked = jnp.concatenate([mine] + [masks[k].astype(F32) for k in range(SP - 1)], axis=0)
    local = dot(stacked.astype(BF16), before)
    counts = jnp.sum(stacked, axis=1, keepdims=True)
    row_dev = lax.rem(me - lax.broadcasted_iota(jnp.int32, (CLIPS * SP, 1), 0) // CLIPS + SP, SP)
    base = jnp.zeros((CLIPS * SP, 1), F32)
    for k in range(SP):
        dev_k = lax.rem(me - k + SP, SP)
        tiled = jnp.concatenate([counts[CLIPS * k:CLIPS * k + CLIPS]] * SP, axis=0)
        base = base + jnp.where(dev_k < row_dev, tiled, 0.0)
    rank_ref[...] = jnp.where(stacked > 0.0, local + base, float(ROWS)).astype(jnp.int32)

    def placement(slot):
        def pick(val):
            two = val[CLIPS * slot:CLIPS * slot + CLIPS]
            return jnp.where(chip == 0, two[0:1], two[1:2])

        start, size = pick(base), pick(counts)
        rows = lax.broadcasted_iota(jnp.int32, (ROWS, WIN), 0).astype(F32)
        cols = lax.broadcasted_iota(jnp.int32, (ROWS, WIN), 1).astype(F32)
        return jnp.where((rows == cols + start) & (cols < size), 1.0, 0.0)

    even = core == 0
    left, right = placement(1), placement(3)
    place = [placement(0), placement(2), jnp.where(even, right, left), jnp.where(even, left, right)]
    to_peer.wait_recv()
    relay = send(win.at[1], win.at[3], win_send.at[2], win_recv.at[2], sib)
    pos_peer = send(dec_pos_hbm, pos_out.at[0], pos_send.at[0], pos_recv.at[0], peer)
    pos_sib = send(dec_pos_hbm, pos_out.at[1], pos_send.at[1], pos_recv.at[1], sib)
    total = dot(place[0].astype(BF16), win[0]) + dot(place[1].astype(BF16), win[1])
    to_sib.wait_recv()
    total = total + dot(place[2].astype(BF16), win[2])
    relay.wait_recv()
    total = total + dot(place[3].astype(BF16), win[3])
    hall[...] = total.astype(BF16)
    own = pl.ds(pl.multiple_of(core * MINE, MINE), MINE)
    hid[...] = hall[own, :]
    norm[0] = layer_norm(hall[...])
    norm_q[MINE:] = jnp.zeros((Q_PAD - MINE, DIM), BF16)
    zero = jnp.zeros((HEAD, Q_PAD), BF16)
    pos_diag = swap = None

    for layer in range(LAYERS):
        copies[layer * 4].wait()
        norm_q[0:MINE] = norm[layer, own, :]
        q_t[...] = dot_nt(qkv[layer, 0:DIM], norm_q[...]).astype(BF16)
        if swap is not None:
            swap.wait()
        k_n[...] = dot_nt(norm[layer], qkv[layer, DIM:2 * DIM]).astype(BF16)
        v_t[...] = dot_nt(qkv[layer, 2 * DIM:3 * DIM], norm[layer]).astype(BF16)

        def heads(group, carry):
            scores, weights = [], []
            for pair in range(2):
                lanes = pl.ds(pl.multiple_of((2 * group + pair) * 2 * HEAD, 2 * HEAD), 2 * HEAD)
                for odd in range(2):
                    rows = pl.ds(pl.multiple_of((4 * group + 2 * pair + odd) * HEAD, HEAD), HEAD)
                    q_head = q_t[rows, :]
                    q_both = jnp.concatenate([zero, q_head] if odd else [q_head, zero], axis=0)
                    scores.append(dot(k_n[:, lanes], q_both))
            for s in scores:
                e = jnp.exp2(s * EXP_SCALE - col_max(s) * EXP_SCALE)
                weights.append((e.astype(BF16), 1.0 / col_sum(e)))
            for idx, (e, scale) in enumerate(weights):
                rows = pl.ds(pl.multiple_of((4 * group + idx) * HEAD, HEAD), HEAD)
                o_t[rows, :] = (dot(v_t[rows, :], e) * scale).astype(BF16)
            return carry

        lax.fori_loop(0, ENC_HEADS // 4, heads, 0)
        copies[layer * 4 + 1].wait()
        mid = (hid[...].astype(F32) + dot_tn(o_t[...], proj[layer])[0:MINE]).astype(BF16)
        rows_norm = layer_norm(mid)
        copies[layer * 4 + 2].wait()
        copies[layer * 4 + 3].wait()
        if layer == LAYERS - 1:
            pos_peer.wait_recv()
            pos_diag = send(pos_out.at[0], pos_out.at[2], pos_send.at[2], pos_recv.at[2], sib)
        acc = None
        for lo in range(0, 4 * DIM, DIM):
            act = gelu(dot(rows_norm, up[layer, :, lo:lo + DIM]))
            part = dot(act, down[layer, lo:lo + DIM, :])
            acc = part if acc is None else acc + part
        out = (mid.astype(F32) + acc).astype(BF16)
        if layer < LAYERS - 1:
            hid[...] = out
            norm[layer + 1, own, :] = layer_norm(out)
            swap = send(norm.at[layer + 1, own], norm.at[layer + 1, own], row_send.at[layer], row_recv.at[layer], sib)
    z_ref[own, :] = dot(layer_norm(out), wed_ref[...]).astype(BF16)
    first = lax.broadcasted_iota(jnp.int32, (2 * HEAD, DDIM), 0) == 0
    z_ref[ROWS:] = jnp.where(first, token_ref[...].astype(F32).reshape(1, DDIM), 0.0).astype(BF16)
    last = send(z_ref.at[own], z_ref.at[own], row_send.at[LAYERS - 1], row_recv.at[LAYERS - 1], sib)
    to_peer.wait_send()
    to_sib.wait_send()
    relay.wait_send()
    pos_peer.wait_send()
    pos_sib.wait()
    pos_diag.wait()
    last.wait()


def encode(mask, bpe, token, patches, enc_pos, wpe, dec_pos, wed, qkv_t, proj, up, down):
    return pl.pallas_call(
        encoder_kernel,
        out_shape=(
            jax.ShapeDtypeStruct((ROWS + 2 * HEAD, DDIM), BF16),
            jax.ShapeDtypeStruct((CLIPS * SP, TOK), jnp.int32),
            jax.ShapeDtypeStruct((SP - 1, TOK, DDIM), BF16),
        ),
        in_specs=[VMEM] * 3 + [ANY] * 4 + [VMEM] + [ANY] * 4,
        out_specs=(VMEM, VMEM, ANY),
        scratch_shapes=[
            pltpu.VMEM((CLIPS, TOK, PATCH), BF16),
            pltpu.VMEM((TOK, DIM), BF16),
            pltpu.VMEM((PATCH, DIM), BF16),
            pltpu.VMEM((LAYERS, 3 * DIM, DIM), BF16),
            pltpu.VMEM((LAYERS, DIM, DIM), BF16),
            pltpu.VMEM((LAYERS, DIM, 4 * DIM), BF16),
            pltpu.VMEM((LAYERS, 4 * DIM, DIM), BF16),
            pltpu.VMEM((SP - 1, CLIPS, TOK), jnp.int32),
            pltpu.VMEM((WIN, DIM), BF16),
            pltpu.VMEM((SP, WIN, DIM), BF16),
            pltpu.VMEM((ROWS, DIM), BF16),
            pltpu.VMEM((MINE, DIM), BF16),
            pltpu.VMEM((LAYERS, ROWS, DIM), BF16),
            pltpu.VMEM((Q_PAD, DIM), BF16),
            pltpu.VMEM((DIM, Q_PAD), BF16),
            pltpu.VMEM((ROWS, DIM), BF16),
            pltpu.VMEM((DIM, ROWS), BF16),
            pltpu.VMEM((DIM, Q_PAD), BF16),
            pltpu.SemaphoreType.DMA((3,)),
            pltpu.SemaphoreType.DMA((LAYERS * 4,)),
            pltpu.SemaphoreType.DMA((SP - 1,)),
            pltpu.SemaphoreType.DMA((SP - 1,)),
            pltpu.SemaphoreType.DMA((3,)),
            pltpu.SemaphoreType.DMA((3,)),
            pltpu.SemaphoreType.DMA((3,)),
            pltpu.SemaphoreType.DMA((3,)),
            pltpu.SemaphoreType.DMA((LAYERS,)),
            pltpu.SemaphoreType.DMA((LAYERS,)),
        ],
        compiler_params=pltpu.CompilerParams(collective_id=0, has_side_effects=True, vmem_limit_bytes=58 * 2 ** 20),
        cost_estimate=pl.CostEstimate(flops=12 * 10 ** 9, bytes_accessed=4 * 10 ** 7, transcendentals=0),
        name='encoder',
    )(mask, bpe, token, patches, enc_pos, wpe, dec_pos, wed, qkv_t, proj, up, down)


Q_BLK = 512
K_BLK = 256
CHUNK = 256
WIDE = 512
PAIR = 2 * HEAD


def fill_rows(start, count, step, body):
    def run(i, carry):
        body(pl.ds(pl.multiple_of(start + i * step, step), step))
        return carry

    lax.fori_loop(0, count // step, run, 0)


def make_queries(rows, norm, w_q, q_3):
    q = dot_nt(w_q, norm[rows, :]).astype(BF16).astype(F32) * EXP_SCALE
    hi = q.astype(BF16)
    rest = q - hi.astype(F32)
    mid = rest.astype(BF16)
    low = (rest - mid.astype(F32)).astype(BF16)
    zero = jnp.zeros((HEAD, q.shape[1]), BF16)
    for head in range(DEC_HEADS):
        part = slice(head * HEAD, (head + 1) * HEAD)
        tail = (low[part], zero) if head % 2 == 0 else (zero, low[part])
        for idx, val in enumerate((hi[part], mid[part]) + tail):
            q_3[head, idx * HEAD:(idx + 1) * HEAD, rows] = val


def make_keys(rows, norm, w_k, w_v, k_n, k_dup, v_t):
    a = norm[rows, :]
    k = dot_nt(a, w_k)
    first = lax.broadcasted_iota(jnp.int32, (k.shape[0], PAIR), 1) < HEAD
    for pair in range(DEC_HEADS // 2):
        both = k[:, pair * PAIR:(pair + 1) * PAIR]
        turned = pltpu.roll(both, HEAD, axis=1)
        k_n[pair, rows, :] = both.astype(BF16)
        k_dup[2 * pair, rows, :] = jnp.where(first, both, turned).astype(BF16)
        k_dup[2 * pair + 1, rows, :] = jnp.where(first, turned, both).astype(BF16)
    v_t[:, rows] = dot_nt(w_v, a).astype(BF16)


def attention(start, count, q_3, k_n, k_dup, v_t, o_t, s_even, s_odd):
    blocks = count // Q_BLK
    units = DEC_HEADS * blocks

    def place(unit):
        head = unit // blocks
        return head, pl.ds(pl.multiple_of(start + (unit - head * blocks) * Q_BLK, Q_BLK), Q_BLK)

    def mixed(unit_q, s_q, unit_p, s_p, max8):
        if unit_q is not None:
            head_q, cols_q = place(unit_q)
            q = q_3[head_q, :, cols_q]
        if unit_p is not None:
            head_p, cols_p = place(unit_p)
            shift = col_max(max8)
            v_rows = pl.ds(pl.multiple_of(head_p * HEAD, HEAD), HEAD)
        new_max = total = late = None
        accs = [None, None]

        def weigh(idx, weights):
            o = dot(v_t[v_rows, idx * K_BLK:(idx + 1) * K_BLK], weights)
            accs[idx % 2] = o if accs[idx % 2] is None else accs[idx % 2] + o

        for idx in range(SEQ // K_BLK):
            rows = slice(idx * K_BLK, (idx + 1) * K_BLK)
            if unit_p is not None:
                e = jnp.exp2(s_p[rows, :] - shift)
                t = jnp.sum(e.reshape(K_BLK // 8, 8, Q_BLK), axis=0)
                total = t if total is None else total + t
                if late is not None:
                    weigh(*late)
                late = (idx, e.astype(BF16))
            if unit_q is not None:
                keys = jnp.concatenate([k_dup[head_q, rows, :], k_n[head_q // 2, rows, :]], axis=1)
                s = dot(keys, q)
                s_q[rows, :] = s
                m = jnp.max(s.reshape(K_BLK // 8, 8, Q_BLK), axis=0)
                new_max = m if new_max is None else jnp.maximum(new_max, m)
        if unit_p is not None:
            weigh(*late)
            o_t[v_rows, cols_p] = ((accs[0] + accs[1]) * (1.0 / col_sum(total))).astype(BF16)
        return new_max

    first = mixed(0, s_even, None, None, None)

    def body(i, max8):
        unit = 2 * i
        max_odd = mixed(unit + 1, s_odd, unit, s_even, max8)
        return mixed(jnp.minimum(unit + 2, units - 1), s_even, unit + 1, s_odd, max_odd)

    lax.fori_loop(0, units // 2, body, first)


def mlp(rows, hid, o_t, w_proj, w_up, w_down):
    mid = (hid[rows, :].astype(F32) + dot_tn(o_t[:, rows], w_proj)).astype(BF16)
    act = gelu(dot(layer_norm(mid), w_up))
    return (mid.astype(F32) + dot(act, w_down)).astype(BF16)


def decoder_kernel(z_ref, rank_ref, pos_me, pos_x, qkv_hbm, proj_hbm, up_hbm, down_hbm, far_ref, hid_out, o_out,
                   qkv, proj, up, down, hid, norm, fin, q_3, k_n, k_dup, v_t, o_t, s_even, s_odd, w_sem, ready, row_send, row_recv, fin_send, fin_recv, out_sem):
    me = lax.axis_index('sp')
    chip = me // 2
    core = me - 2 * chip
    peer = lax.rem(me + 2, SP)
    sib = me + 1 - 2 * core
    diag = lax.rem(sib + 2, SP)

    copies = []
    for layer in range(LAYERS):
        for idx, (src, dst) in enumerate(((qkv_hbm, qkv), (proj_hbm, proj), (up_hbm, up), (down_hbm, down))):
            copy = pltpu.make_async_copy(src.at[layer], dst.at[layer], w_sem.at[layer * 4 + idx])
            copy.start()
            copies.append(copy)
    barrier = pltpu.get_barrier_semaphore()
    for other in (peer, sib):
        pl.semaphore_signal(barrier, inc=1, device_id={'sp': other}, device_id_type=MESH)
    pl.semaphore_wait(barrier, 2)

    def tokens(dev, pos):
        slot = lax.rem(me - dev + SP, SP)
        rank = rank_ref[pl.ds(2 * slot + chip, 1), :]
        rank_col = jnp.transpose(jnp.broadcast_to(rank.astype(F32), (8, TOK)))[:, 0:1]
        lanes = lax.broadcasted_iota(jnp.int32, (TOK, ROWS + 2 * HEAD), 1).astype(F32)
        select = jnp.where(lanes == rank_col, 1.0, 0.0).astype(BF16)
        return (dot(select, z_ref[...]) + pos.astype(F32)).astype(BF16)

    hid[0:TOK] = tokens(peer, pos_x[0])
    hid[TOK:OWN] = tokens(me, pos_me[...])
    norm[OWN:OWN + TOK] = layer_norm(tokens(diag, pos_x[2]))
    norm[OWN + TOK:SEQ] = layer_norm(tokens(sib, pos_x[1]))

    def own_norm(rows):
        norm[rows, :] = layer_norm(hid[rows, :])

    fill_rows(0, OWN, CHUNK, own_norm)

    def queries(layer):
        fill_rows(0, OWN, WIDE, lambda rows: make_queries(rows, norm, qkv[layer, 0:DDIM], q_3))

    def keys(layer, start, count):
        fill_rows(start, count, WIDE, lambda rows: make_keys(
            rows, norm, qkv[layer, DDIM:2 * DDIM], qkv[layer, 2 * DDIM:3 * DDIM], k_n, k_dup, v_t))

    copies[0].wait()
    queries(0)
    keys(0, 0, SEQ)
    pl.semaphore_signal(ready, inc=1, device_id={'sp': sib}, device_id_type=MESH)
    attention(0, OWN, q_3, k_n, k_dup, v_t, o_t, s_even, s_odd)
    pl.semaphore_wait(ready, 1)
    for copy in copies[1:]:
        copy.wait()
    steps = OWN // CHUNK

    def row_copy(i):
        src = pl.ds(pl.multiple_of(i * CHUNK, CHUNK), CHUNK)
        dst = pl.ds(pl.multiple_of(OWN + i * CHUNK, CHUNK), CHUNK)
        return pltpu.make_async_remote_copy(
            src_ref=norm.at[src], dst_ref=norm.at[dst], send_sem=row_send.at[i], recv_sem=row_recv.at[i],
            device_id={'sp': sib}, device_id_type=MESH)

    def first_mlp(i, carry):
        rows = pl.ds(pl.multiple_of(i * CHUNK, CHUNK), CHUNK)
        val = mlp(rows, hid, o_t, proj[0], up[0], down[0])
        hid[rows, :] = val
        norm[rows, :] = layer_norm(val)

        @pl.when(i > 0)
        def _():
            row_copy(i - 1).start()

        return carry

    lax.fori_loop(0, steps, first_mlp, 0)
    queries(1)
    row_copy(steps - 1).start()
    keys(1, 0, OWN)
    for i in range(steps):
        row_copy(i).wait()
    keys(1, OWN, OWN)

    keep = pltpu.make_async_copy(hid.at[pl.ds(TOK, TOK)], hid_out, out_sem.at[0])
    keep.start()
    early = 2 * Q_BLK
    attention(0, early, q_3, k_n, k_dup, v_t, o_t, s_even, s_odd)
    pieces = TOK // CHUNK

    def fin_copy(i):
        rows = pl.ds(pl.multiple_of(i * CHUNK, CHUNK), CHUNK)
        return pltpu.make_async_remote_copy(
            src_ref=fin.at[rows], dst_ref=far_ref.at[rows], send_sem=fin_send.at[i], recv_sem=fin_recv.at[i],
            device_id={'sp': peer}, device_id_type=MESH)

    def peer_mlp(i, carry):
        rows = pl.ds(pl.multiple_of(i * CHUNK, CHUNK), CHUNK)
        fin[rows, :] = layer_norm(mlp(rows, hid, o_t, proj[1], up[1], down[1]))

        @pl.when(i > 0)
        def _():
            fin_copy(i - 1).start()

        return carry

    lax.fori_loop(0, pieces, peer_mlp, 0)
    fin_copy(pieces - 1).start()
    attention(early, OWN - early, q_3, k_n, k_dup, v_t, o_t, s_even, s_odd)
    give = pltpu.make_async_copy(o_t.at[:, pl.ds(TOK, TOK)], o_out, out_sem.at[1])
    give.start()
    for i in range(pieces):
        fin_copy(i).wait()
    keep.wait()
    give.wait()


def decode(z, rank, pos, pos_x, wqkv, wproj, wup, wdown):
    return pl.pallas_call(
        decoder_kernel,
        out_shape=(
            jax.ShapeDtypeStruct((TOK, DDIM), BF16),
            jax.ShapeDtypeStruct((TOK, DDIM), BF16),
            jax.ShapeDtypeStruct((DDIM, TOK), BF16),
        ),
        in_specs=[VMEM] * 4 + [ANY] * 4,
        out_specs=(VMEM, ANY, ANY),
        scratch_shapes=[
            pltpu.VMEM((LAYERS, 3 * DDIM, DDIM), BF16),
            pltpu.VMEM((LAYERS, DDIM, DDIM), BF16),
            pltpu.VMEM((LAYERS, DDIM, 4 * DDIM), BF16),
            pltpu.VMEM((LAYERS, 4 * DDIM, DDIM), BF16),
            pltpu.VMEM((OWN, DDIM), BF16),
            pltpu.VMEM((SEQ, DDIM), BF16),
            pltpu.VMEM((TOK, DDIM), BF16),
            pltpu.VMEM((DEC_HEADS, 4 * HEAD, OWN), BF16),
            pltpu.VMEM((DEC_HEADS // 2, SEQ, PAIR), BF16),
            pltpu.VMEM((DEC_HEADS, SEQ, PAIR), BF16),
            pltpu.VMEM((DDIM, SEQ), BF16),
            pltpu.VMEM((DDIM, OWN), BF16),
            pltpu.VMEM((SEQ, Q_BLK), F32),
            pltpu.VMEM((SEQ, Q_BLK), F32),
            pltpu.SemaphoreType.DMA((LAYERS * 4,)),
            pltpu.SemaphoreType.REGULAR,
            pltpu.SemaphoreType.DMA((OWN // CHUNK,)),
            pltpu.SemaphoreType.DMA((OWN // CHUNK,)),
            pltpu.SemaphoreType.DMA((TOK // CHUNK,)),
            pltpu.SemaphoreType.DMA((TOK // CHUNK,)),
            pltpu.SemaphoreType.DMA((2,)),
        ],
        compiler_params=pltpu.CompilerParams(collective_id=1, has_side_effects=True, vmem_limit_bytes=58 * 2 ** 20),
        cost_estimate=pl.CostEstimate(flops=60 * 10 ** 9, bytes_accessed=2 * 10 ** 7, transcendentals=6 * 10 ** 7),
        name='decoder',
    )(z, rank, pos, pos_x, wqkv, wproj, wup, wdown)


def output_kernel(far_ref, hid, o_t, w_ref, proj_hbm, up_hbm, down_hbm, out_hbm, proj, up, down, buf, w_sem, out_sem):
    chip = lax.axis_index('sp') // 2
    loads = [pltpu.make_async_copy(src.at[LAYERS - 1], dst, w_sem.at[idx])
             for idx, (src, dst) in enumerate(((proj_hbm, proj), (up_hbm, up), (down_hbm, down)))]
    for copy in loads:
        copy.start()
    pieces = TOK // CHUNK

    def out_copy(slot, clip, i):
        rows = pl.ds(pl.multiple_of(i * CHUNK, CHUNK), CHUNK)
        return pltpu.make_async_copy(buf.at[slot], out_hbm.at[clip, rows], out_sem.at[slot])

    def far_rows(i, carry):
        buf[i] = dot(far_ref[pl.ds(pl.multiple_of(i * CHUNK, CHUNK), CHUNK), :], w_ref[...])
        out_copy(i, 1 - chip, i).start()
        return carry

    def near_rows(i, carry):
        rows = pl.ds(pl.multiple_of(i * CHUNK, CHUNK), CHUNK)
        buf[pieces + i] = dot(layer_norm(mlp(rows, hid, o_t, proj[...], up[...], down[...])), w_ref[...])
        out_copy(pieces + i, chip, i).start()
        return carry

    lax.fori_loop(0, pieces, far_rows, 0)
    for copy in loads:
        copy.wait()
    lax.fori_loop(0, pieces, near_rows, 0)
    for i in range(pieces):
        out_copy(i, 1 - chip, i).wait()
        out_copy(pieces + i, chip, i).wait()


def project(far, hid, o_t, w_out, proj, up, down):
    return pl.pallas_call(
        output_kernel,
        out_shape=jax.ShapeDtypeStruct((CLIPS, TOK, PATCH), F32),
        in_specs=[VMEM] * 4 + [ANY] * 3,
        out_specs=ANY,
        scratch_shapes=[
            pltpu.VMEM((DDIM, DDIM), BF16),
            pltpu.VMEM((DDIM, 4 * DDIM), BF16),
            pltpu.VMEM((4 * DDIM, DDIM), BF16),
            pltpu.VMEM((CLIPS * TOK // CHUNK, CHUNK, PATCH), F32),
            pltpu.SemaphoreType.DMA((3,)),
            pltpu.SemaphoreType.DMA((CLIPS * TOK // CHUNK,)),
        ],
        compiler_params=pltpu.CompilerParams(vmem_limit_bytes=62 * 2 ** 20),
        cost_estimate=pl.CostEstimate(flops=5 * 10 ** 9, bytes_accessed=15 * 10 ** 6, transcendentals=0),
        name='output',
    )(far, hid, o_t, w_out, proj, up, down)


def solution(mesh):
    def local_program(patches, vis_mask, enc_pos, dec_pos, w_pe, b_pe, enc_qkv, enc_proj, enc_up, enc_down, w_ed, mask_token, dec_qkv, dec_proj, dec_up, dec_down, w_out):
        enc_qkv_t = jnp.transpose(enc_qkv, (0, 2, 3, 4, 1)).reshape(LAYERS, 3 * DIM, DIM)
        dec_qkv_t = jnp.transpose(dec_qkv, (0, 2, 3, 4, 1)).reshape(LAYERS, 3 * DDIM, DDIM)
        enc_proj2 = enc_proj.reshape(LAYERS, DIM, DIM)
        dec_proj2 = dec_proj.reshape(LAYERS, DDIM, DDIM)
        z, rank, pos_x = encode(vis_mask, b_pe, mask_token, patches, enc_pos, w_pe, dec_pos, w_ed,
                                enc_qkv_t, enc_proj2, enc_up, enc_down)
        far, hid, o_t = decode(z, rank, dec_pos, pos_x, dec_qkv_t, dec_proj2, dec_up, dec_down)
        return project(far, hid, o_t, w_out, dec_proj2, dec_up, dec_down)

    row_spec = P('dp', 'sp', None)
    pos_spec = P(('dp', 'sp'), None)
    arg_specs = (row_spec, P('dp', 'sp'), pos_spec, pos_spec) + (P(),) * 13
    return jax.shard_map(local_program, mesh=mesh, in_specs=arg_specs, out_specs=row_spec, check_vma=False)
```

```python
import functools
import math

import jax
import jax.numpy as jnp
from jax import lax
from jax.experimental import pallas as pl
from jax.experimental.pallas import tpu as pltpu
from jax.sharding import PartitionSpec as P

F32 = jnp.float32
BF16 = jnp.bfloat16
MESH = pl.DeviceIdType.MESH
VMEM = pl.BlockSpec(memory_space=pltpu.VMEM)
ANY = pl.BlockSpec(memory_space=pl.ANY)

SP = 4
CLIPS = 2
TOK = 768
PATCH = 1536
DIM = 768
ENC_HEADS = 12
HEAD = 64
DDIM = 384
DEC_HEADS = 6
VIS = 96
WIN = 2 * VIS
ROWS = SP * VIS
OWN = 2 * TOK
SEQ = SP * TOK
LAYERS = 2
EXP_SCALE = HEAD ** -0.5 * math.log2(math.e)


def dot(lhs, rhs):
    return jnp.dot(lhs, rhs, preferred_element_type=F32)


def dot_nt(lhs, rhs):
    return lax.dot_general(lhs, rhs, (((1,), (1,)), ((), ())), preferred_element_type=F32)


def dot_tn(lhs, rhs):
    return lax.dot_general(lhs, rhs, (((0,), (0,)), ((), ())), preferred_element_type=F32)


def layer_norm(hidden):
    hid = hidden.astype(F32)
    centred = hid - jnp.mean(hid, axis=-1, keepdims=True)
    var = jnp.mean(centred * centred, axis=-1, keepdims=True)
    return (centred * lax.rsqrt(var + 1e-6)).astype(BF16)


def gelu(val):
    return (0.5 * val * (1.0 + lax.erf(val * math.sqrt(0.5)))).astype(BF16)


def col_max(val):
    return jnp.max(val, axis=0, keepdims=True)


def col_sum(val):
    return jnp.sum(val, axis=0, keepdims=True)


MINE = ROWS // 2
Q_PAD = 256


def encoder_kernel(mask_ref, bpe_ref, token_ref, patch_hbm, pos_hbm, wpe_hbm, dec_pos_hbm, wed_ref, qkv_hbm, proj_hbm, up_hbm, down_hbm,
                   z_ref, rank_ref, pos_out,
                   patch, pos, wpe, qkv, proj, up, down, masks, sendbuf, win, hall, hid, norm, norm_q, q_t, k_n, v_t, o_t,
                   in_sem, w_sem, mask_send, mask_recv, win_send, win_recv, pos_send, pos_recv, row_send, row_recv):
    me = lax.axis_index('sp')
    chip = me // 2
    core = me - 2 * chip
    peer = lax.rem(me + 2, SP)
    sib = me + 1 - 2 * core
    diag = lax.rem(sib + 2, SP)

    loads = [pltpu.make_async_copy(src, dst, in_sem.at[idx])
             for idx, (src, dst) in enumerate(((patch_hbm, patch), (wpe_hbm, wpe), (pos_hbm, pos)))]
    for copy in loads:
        copy.start()
    barrier = pltpu.get_barrier_semaphore()
    for other in (peer, sib, diag):
        pl.semaphore_signal(barrier, inc=1, device_id={'sp': other}, device_id_type=MESH)
    order_row = lax.broadcasted_iota(jnp.int32, (TOK, TOK), 0)
    order_col = lax.broadcasted_iota(jnp.int32, (TOK, TOK), 1)
    before = jnp.where(order_row < order_col, 1.0, 0.0).astype(BF16)
    mine = mask_ref[...].astype(F32)
    mine_rank = dot(jnp.concatenate([mine] * SP, axis=0).astype(BF16), before)[0:CLIPS]
    slot_of = jnp.where(mine > 0.0, mine_rank, -1.0)
    pl.semaphore_wait(barrier, 3)

    def send(src, dst, send_sem, recv_sem, dev):
        copy = pltpu.make_async_remote_copy(
            src_ref=src, dst_ref=dst, send_sem=send_sem, recv_sem=recv_sem, device_id={'sp': dev}, device_id_type=MESH)
        copy.start()
        return copy

    mask_copies = [send(mask_ref, masks.at[step - 1], mask_send.at[step - 1], mask_recv.at[step - 1], lax.rem(me + step, SP))
                   for step in range(1, SP)]
    for copy in loads:
        copy.wait()
    copies = []
    for layer in range(LAYERS):
        for idx, (src, dst) in enumerate(((qkv_hbm, qkv), (proj_hbm, proj), (up_hbm, up), (down_hbm, down))):
            copy = pltpu.make_async_copy(src.at[layer], dst.at[layer], w_sem.at[layer * 4 + idx])
            copy.start()
            copies.append(copy)

    bias = bpe_ref[...].astype(F32).reshape(1, DIM)

    def window(clip, slots):
        rows = lax.broadcasted_iota(jnp.int32, (WIN, TOK), 0).astype(F32)
        hit = jnp.where(rows == slots, 1.0, 0.0)
        select = hit.astype(BF16)
        moved = dot(select, patch[clip]).astype(BF16)
        occupied = jnp.sum(hit, axis=1, keepdims=True)
        emb = dot(moved, wpe[...]) + occupied * bias + dot(select, pos[...])
        return emb.astype(BF16)

    far = jnp.where(chip == 0, slot_of[1:2], slot_of[0:1])
    near = jnp.where(chip == 0, slot_of[0:1], slot_of[1:2])
    sendbuf[...] = window(1 - chip, far)
    to_peer = send(sendbuf, win.at[1], win_send.at[0], win_recv.at[0], peer)
    win[0] = window(chip, near)
    to_sib = send(win.at[0], win.at[2], win_send.at[1], win_recv.at[1], sib)

    for copy in mask_copies:
        copy.wait()
    stacked = jnp.concatenate([mine] + [masks[k].astype(F32) for k in range(SP - 1)], axis=0)
    local = dot(stacked.astype(BF16), before)
    counts = jnp.sum(stacked, axis=1, keepdims=True)
    row_dev = lax.rem(me - lax.broadcasted_iota(jnp.int32, (CLIPS * SP, 1), 0) // CLIPS + SP, SP)
    base = jnp.zeros((CLIPS * SP, 1), F32)
    for k in range(SP):
        dev_k = lax.rem(me - k + SP, SP)
        tiled = jnp.concatenate([counts[CLIPS * k:CLIPS * k + CLIPS]] * SP, axis=0)
        base = base + jnp.where(dev_k < row_dev, tiled, 0.0)
    rank_ref[...] = jnp.where(stacked > 0.0, local + base, float(ROWS)).astype(jnp.int32)

    def placement(slot):
        def pick(val):
            two = val[CLIPS * slot:CLIPS * slot + CLIPS]
            return jnp.where(chip == 0, two[0:1], two[1:2])

        start, size = pick(base), pick(counts)
        rows = lax.broadcasted_iota(jnp.int32, (ROWS, WIN), 0).astype(F32)
        cols = lax.broadcasted_iota(jnp.int32, (ROWS, WIN), 1).astype(F32)
        return jnp.where((rows == cols + start) & (cols < size), 1.0, 0.0)

    even = core == 0
    left, right = placement(1), placement(3)
    place = [placement(0), placement(2), jnp.where(even, right, left), jnp.where(even, left, right)]
    to_peer.wait_recv()
    relay = send(win.at[1], win.at[3], win_send.at[2], win_recv.at[2], sib)
    pos_peer = send(dec_pos_hbm, pos_out.at[0], pos_send.at[0], pos_recv.at[0], peer)
    pos_sib = send(dec_pos_hbm, pos_out.at[1], pos_send.at[1], pos_recv.at[1], sib)
    total = dot(place[0].astype(BF16), win[0]) + dot(place[1].astype(BF16), win[1])
    to_sib.wait_recv()
    total = total + dot(place[2].astype(BF16), win[2])
    relay.wait_recv()
    total = total + dot(place[3].astype(BF16), win[3])
    hall[...] = total.astype(BF16)
    own = pl.ds(pl.multiple_of(core * MINE, MINE), MINE)
    hid[...] = hall[own, :]
    norm[0] = layer_norm(hall[...])
    norm_q[MINE:] = jnp.zeros((Q_PAD - MINE, DIM), BF16)
    zero = jnp.zeros((HEAD, Q_PAD), BF16)
    pos_diag = swap = None

    for layer in range(LAYERS):
        copies[layer * 4].wait()
        norm_q[0:MINE] = norm[layer, own, :]
        q_t[...] = dot_nt(qkv[layer, 0:DIM], norm_q[...]).astype(BF16)
        if swap is not None:
            swap.wait()
        k_n[...] = dot_nt(norm[layer], qkv[layer, DIM:2 * DIM]).astype(BF16)
        v_t[...] = dot_nt(qkv[layer, 2 * DIM:3 * DIM], norm[layer]).astype(BF16)

        def heads(group, carry):
            scores, weights = [], []
            for pair in range(2):
                lanes = pl.ds(pl.multiple_of((2 * group + pair) * 2 * HEAD, 2 * HEAD), 2 * HEAD)
                for odd in range(2):
                    rows = pl.ds(pl.multiple_of((4 * group + 2 * pair + odd) * HEAD, HEAD), HEAD)
                    q_head = q_t[rows, :]
                    q_both = jnp.concatenate([zero, q_head] if odd else [q_head, zero], axis=0)
                    scores.append(dot(k_n[:, lanes], q_both))
            for s in scores:
                e = jnp.exp2(s * EXP_SCALE - col_max(s) * EXP_SCALE)
                weights.append((e.astype(BF16), 1.0 / col_sum(e)))
            for idx, (e, scale) in enumerate(weights):
                rows = pl.ds(pl.multiple_of((4 * group + idx) * HEAD, HEAD), HEAD)
                o_t[rows, :] = (dot(v_t[rows, :], e) * scale).astype(BF16)
            return carry

        lax.fori_loop(0, ENC_HEADS // 4, heads, 0)
        copies[layer * 4 + 1].wait()
        mid = (hid[...].astype(F32) + dot_tn(o_t[...], proj[layer])[0:MINE]).astype(BF16)
        rows_norm = layer_norm(mid)
        copies[layer * 4 + 2].wait()
        copies[layer * 4 + 3].wait()
        if layer == LAYERS - 1:
            pos_peer.wait_recv()
            pos_diag = send(pos_out.at[0], pos_out.at[2], pos_send.at[2], pos_recv.at[2], sib)
        acc = None
        for lo in range(0, 4 * DIM, DIM):
            act = gelu(dot(rows_norm, up[layer, :, lo:lo + DIM]))
            part = dot(act, down[layer, lo:lo + DIM, :])
            acc = part if acc is None else acc + part
        out = (mid.astype(F32) + acc).astype(BF16)
        if layer < LAYERS - 1:
            hid[...] = out
            norm[layer + 1, own, :] = layer_norm(out)
            swap = send(norm.at[layer + 1, own], norm.at[layer + 1, own], row_send.at[layer], row_recv.at[layer], sib)
    z_ref[own, :] = dot(layer_norm(out), wed_ref[...]).astype(BF16)
    first = lax.broadcasted_iota(jnp.int32, (2 * HEAD, DDIM), 0) == 0
    z_ref[ROWS:] = jnp.where(first, token_ref[...].astype(F32).reshape(1, DDIM), 0.0).astype(BF16)
    last = send(z_ref.at[own], z_ref.at[own], row_send.at[LAYERS - 1], row_recv.at[LAYERS - 1], sib)
    to_peer.wait_send()
    to_sib.wait_send()
    relay.wait_send()
    pos_peer.wait_send()
    pos_sib.wait()
    pos_diag.wait()
    last.wait()


def encode(mask, bpe, token, patches, enc_pos, wpe, dec_pos, wed, qkv_t, proj, up, down):
    return pl.pallas_call(
        encoder_kernel,
        out_shape=(
            jax.ShapeDtypeStruct((ROWS + 2 * HEAD, DDIM), BF16),
            jax.ShapeDtypeStruct((CLIPS * SP, TOK), jnp.int32),
            jax.ShapeDtypeStruct((SP - 1, TOK, DDIM), BF16),
        ),
        in_specs=[VMEM] * 3 + [ANY] * 4 + [VMEM] + [ANY] * 4,
        out_specs=(VMEM, VMEM, ANY),
        scratch_shapes=[
            pltpu.VMEM((CLIPS, TOK, PATCH), BF16),
            pltpu.VMEM((TOK, DIM), BF16),
            pltpu.VMEM((PATCH, DIM), BF16),
            pltpu.VMEM((LAYERS, 3 * DIM, DIM), BF16),
            pltpu.VMEM((LAYERS, DIM, DIM), BF16),
            pltpu.VMEM((LAYERS, DIM, 4 * DIM), BF16),
            pltpu.VMEM((LAYERS, 4 * DIM, DIM), BF16),
            pltpu.VMEM((SP - 1, CLIPS, TOK), jnp.int32),
            pltpu.VMEM((WIN, DIM), BF16),
            pltpu.VMEM((SP, WIN, DIM), BF16),
            pltpu.VMEM((ROWS, DIM), BF16),
            pltpu.VMEM((MINE, DIM), BF16),
            pltpu.VMEM((LAYERS, ROWS, DIM), BF16),
            pltpu.VMEM((Q_PAD, DIM), BF16),
            pltpu.VMEM((DIM, Q_PAD), BF16),
            pltpu.VMEM((ROWS, DIM), BF16),
            pltpu.VMEM((DIM, ROWS), BF16),
            pltpu.VMEM((DIM, Q_PAD), BF16),
            pltpu.SemaphoreType.DMA((3,)),
            pltpu.SemaphoreType.DMA((LAYERS * 4,)),
            pltpu.SemaphoreType.DMA((SP - 1,)),
            pltpu.SemaphoreType.DMA((SP - 1,)),
            pltpu.SemaphoreType.DMA((3,)),
            pltpu.SemaphoreType.DMA((3,)),
            pltpu.SemaphoreType.DMA((3,)),
            pltpu.SemaphoreType.DMA((3,)),
            pltpu.SemaphoreType.DMA((LAYERS,)),
            pltpu.SemaphoreType.DMA((LAYERS,)),
        ],
        compiler_params=pltpu.CompilerParams(collective_id=0, has_side_effects=True, vmem_limit_bytes=58 * 2 ** 20),
        cost_estimate=pl.CostEstimate(flops=12 * 10 ** 9, bytes_accessed=4 * 10 ** 7, transcendentals=0),
        name='encoder',
    )(mask, bpe, token, patches, enc_pos, wpe, dec_pos, wed, qkv_t, proj, up, down)


Q_BLK = 512
K_BLK = 256
CHUNK = 256
WIDE = 512
PAIR = 2 * HEAD
MIN_SUM = 2.0 ** -64


def fill_rows(start, count, step, body):
    def run(i, carry):
        body(pl.ds(pl.multiple_of(start + i * step, step), step))
        return carry

    lax.fori_loop(0, count // step, run, 0)


def make_queries(rows, norm, w_q, q_3, q_sq):
    q = dot_nt(w_q, norm[rows, :]).astype(BF16).astype(F32) * EXP_SCALE
    hi = q.astype(BF16)
    rest = q - hi.astype(F32)
    mid = rest.astype(BF16)
    low = (rest - mid.astype(F32)).astype(BF16)
    zero = jnp.zeros((HEAD, q.shape[1]), BF16)
    square = q * q
    for head in range(DEC_HEADS):
        part = slice(head * HEAD, (head + 1) * HEAD)
        for idx, val in enumerate((hi[part], mid[part], low[part], zero)):
            q_3[head, idx * HEAD:(idx + 1) * HEAD, rows] = val
        q_sq[head:head + 1, rows] = col_sum(square[part])


def set_shifts(q_3, q_sq, k_sq):
    for head in range(DEC_HEADS):
        bound = 1.02 * lax.sqrt(q_sq[head:head + 1, :] * k_sq[0:1, head:head + 1])
        first = lax.broadcasted_iota(jnp.int32, (16, OWN), 0) == 0
        q_3[head, 3 * HEAD:3 * HEAD + 16, :] = jnp.where(first, -bound, 0.0).astype(BF16)


def make_keys(rows, norm, w_k, w_v, k_one, k_dup, v_t):
    a = norm[rows, :]
    k = dot_nt(a, w_k).astype(BF16).astype(F32)
    count = k.shape[0]
    lane = lax.broadcasted_iota(jnp.int32, (count, PAIR), 1)
    first = lane < HEAD
    ones = jnp.where(lane == HEAD, 1.0, 0.0)
    for pair in range(DEC_HEADS // 2):
        both = k[:, pair * PAIR:(pair + 1) * PAIR]
        turned = pltpu.roll(both, HEAD, axis=1)
        for odd, (low, high) in enumerate(((both, turned), (turned, both))):
            k_dup[2 * pair + odd, rows, :] = jnp.where(first, low, high).astype(BF16)
            k_one[2 * pair + odd, rows, :] = jnp.where(first, low, ones).astype(BF16)
    v_t[:, rows] = dot_nt(w_v, a).astype(BF16)
    owner = lax.broadcasted_iota(jnp.int32, (DDIM, PAIR), 0) // HEAD
    pick = jnp.where(owner == lax.broadcasted_iota(jnp.int32, (DDIM, PAIR), 1), 1.0, 0.0).astype(BF16)
    norms = dot((k * k).astype(BF16), pick) * 1.02
    return jnp.max(norms.reshape(count // 8, 8, PAIR), axis=0)


def attention(start, count, q_3, k_one, k_dup, v_t, o_t, least):
    blocks = count // Q_BLK

    def body(unit, least):
        head = unit // blocks
        cols = pl.ds(pl.multiple_of(start + (unit - head * blocks) * Q_BLK, Q_BLK), Q_BLK)
        q = q_3[head, :, cols]
        v_rows = pl.ds(pl.multiple_of(head * HEAD, HEAD), HEAD)

        def scores(idx):
            rows = slice(idx * K_BLK, (idx + 1) * K_BLK)
            return dot(jnp.concatenate([k_dup[head, rows, :], k_one[head, rows, :]], axis=1), q)

        ahead = scores(0)
        total = acc = None
        for idx in range(SEQ // K_BLK):
            s = ahead
            if idx + 1 < SEQ // K_BLK:
                ahead = scores(idx + 1)
            e = jnp.exp2(s)
            t = jnp.sum(e.reshape(K_BLK // 8, 8, Q_BLK), axis=0)
            total = t if total is None else total + t
            o = dot(v_t[v_rows, idx * K_BLK:(idx + 1) * K_BLK], e.astype(BF16))
            acc = o if acc is None else acc + o
        total = col_sum(total)
        o_t[v_rows, cols] = (acc * (1.0 / total)).astype(BF16)
        return jnp.where(total >= MIN_SUM, least, 0.0)

    return lax.fori_loop(0, DEC_HEADS * blocks, body, least)


X_BLK = 256


def attention_exact(start, count, q_3, k_one, k_dup, v_t, o_t, s_buf):
    blocks = count // X_BLK

    def body(unit, carry):
        head = unit // blocks
        cols = pl.ds(pl.multiple_of(start + (unit - head * blocks) * X_BLK, X_BLK), X_BLK)
        q = q_3[head, :, cols]
        v_rows = pl.ds(pl.multiple_of(head * HEAD, HEAD), HEAD)

        def measure(i, peak):
            rows = pl.ds(pl.multiple_of(i * K_BLK, K_BLK), K_BLK)
            s = dot(jnp.concatenate([k_dup[head, rows, :], k_one[head, rows, :]], axis=1), q)
            s_buf[rows, :] = s
            return jnp.maximum(peak, jnp.max(s.reshape(K_BLK // 8, 8, X_BLK), axis=0))

        shift = col_max(lax.fori_loop(0, SEQ // K_BLK, measure, jnp.full((8, X_BLK), -jnp.inf, F32)))

        def weigh(i, sums):
            rows = pl.ds(pl.multiple_of(i * K_BLK, K_BLK), K_BLK)
            e = jnp.exp2(s_buf[rows, :] - shift)
            total = sums[0] + jnp.sum(e.reshape(K_BLK // 8, 8, X_BLK), axis=0)
            return total, sums[1] + dot(v_t[v_rows, rows], e.astype(BF16))

        total, acc = lax.fori_loop(0, SEQ // K_BLK, weigh, (jnp.zeros((8, X_BLK), F32), jnp.zeros((HEAD, X_BLK), F32)))
        o_t[v_rows, cols] = (acc * (1.0 / col_sum(total))).astype(BF16)
        return carry

    lax.fori_loop(0, DEC_HEADS * blocks, body, 0)


def mlp(rows, hid, o_t, w_proj, w_up, w_down):
    mid = (hid[rows, :].astype(F32) + dot_tn(o_t[:, rows], w_proj)).astype(BF16)
    act = gelu(dot(layer_norm(mid), w_up))
    return (mid.astype(F32) + dot(act, w_down)).astype(BF16)


def decoder_kernel(exact, z_ref, rank_ref, pos_me, pos_x, qkv_hbm, proj_hbm, up_hbm, down_hbm, far_ref, hid_out, o_out, least_ref,
                   qkv, proj, up, down, hid, norm, fin, q_3, q_sq, k_sq, k_one, k_dup, v_t, o_t, s_buf, least_mine, least_all, w_sem, least_send, least_recv, ready, row_send, row_recv, fin_send, fin_recv, out_sem):
    me = lax.axis_index('sp')
    chip = me // 2
    core = me - 2 * chip
    peer = lax.rem(me + 2, SP)
    sib = me + 1 - 2 * core
    diag = lax.rem(sib + 2, SP)

    copies = []
    for layer in range(LAYERS):
        for idx, (src, dst) in enumerate(((qkv_hbm, qkv), (proj_hbm, proj), (up_hbm, up), (down_hbm, down))):
            copy = pltpu.make_async_copy(src.at[layer], dst.at[layer], w_sem.at[layer * 4 + idx])
            copy.start()
            copies.append(copy)
    barrier = pltpu.get_barrier_semaphore()
    for other in (peer, sib, diag):
        pl.semaphore_signal(barrier, inc=1, device_id={'sp': other}, device_id_type=MESH)
    pl.semaphore_wait(barrier, 3)

    def tokens(dev, pos):
        slot = lax.rem(me - dev + SP, SP)
        rank = rank_ref[pl.ds(2 * slot + chip, 1), :]
        rank_col = jnp.transpose(jnp.broadcast_to(rank.astype(F32), (8, TOK)))[:, 0:1]
        lanes = lax.broadcasted_iota(jnp.int32, (TOK, ROWS + 2 * HEAD), 1).astype(F32)
        select = jnp.where(lanes == rank_col, 1.0, 0.0).astype(BF16)
        return (dot(select, z_ref[...]) + pos.astype(F32)).astype(BF16)

    hid[0:TOK] = tokens(peer, pos_x[0])
    hid[TOK:OWN] = tokens(me, pos_me[...])
    norm[OWN:OWN + TOK] = layer_norm(tokens(diag, pos_x[2]))
    norm[OWN + TOK:SEQ] = layer_norm(tokens(sib, pos_x[1]))

    def own_norm(rows):
        norm[rows, :] = layer_norm(hid[rows, :])

    fill_rows(0, OWN, CHUNK, own_norm)

    wide = CHUNK if exact else WIDE

    def queries(layer):
        fill_rows(0, OWN, wide, lambda rows: make_queries(rows, norm, qkv[layer, 0:DDIM], q_3, q_sq))

    def keys(layer, start, count):
        def run(i, carry):
            rows = pl.ds(pl.multiple_of(start + i * wide, wide), wide)
            norms = make_keys(rows, norm, qkv[layer, DDIM:2 * DDIM], qkv[layer, 2 * DDIM:3 * DDIM], k_one, k_dup, v_t)
            return jnp.maximum(carry, norms)

        return lax.fori_loop(0, count // wide, run, jnp.zeros((8, PAIR), F32))

    def shifts(norms):
        if not exact:
            k_sq[...] = jnp.broadcast_to(col_max(norms), (8, PAIR))
            set_shifts(q_3, q_sq, k_sq)

    def attend(start, count, least):
        if exact:
            attention_exact(start, count, q_3, k_one, k_dup, v_t, o_t, s_buf)
            return least
        return attention(start, count, q_3, k_one, k_dup, v_t, o_t, least)

    least = jnp.ones((1, Q_BLK), F32)
    copies[0].wait()
    queries(0)
    shifts(keys(0, 0, SEQ))
    pl.semaphore_signal(ready, inc=1, device_id={'sp': sib}, device_id_type=MESH)
    least = attend(0, OWN, least)
    pl.semaphore_wait(ready, 1)
    for copy in copies[1:]:
        copy.wait()
    steps = OWN // CHUNK

    def row_copy(i):
        src = pl.ds(pl.multiple_of(i * CHUNK, CHUNK), CHUNK)
        dst = pl.ds(pl.multiple_of(OWN + i * CHUNK, CHUNK), CHUNK)
        return pltpu.make_async_remote_copy(
            src_ref=norm.at[src], dst_ref=norm.at[dst], send_sem=row_send.at[i], recv_sem=row_recv.at[i],
            device_id={'sp': sib}, device_id_type=MESH)

    def first_mlp(i, carry):
        rows = pl.ds(pl.multiple_of(i * CHUNK, CHUNK), CHUNK)
        val = mlp(rows, hid, o_t, proj[0], up[0], down[0])
        hid[rows, :] = val
        norm[rows, :] = layer_norm(val)

        @pl.when(i > 0)
        def _():
            row_copy(i - 1).start()

        return carry

    lax.fori_loop(0, steps, first_mlp, 0)
    queries(1)
    row_copy(steps - 1).start()
    norms = keys(1, 0, OWN)
    for i in range(steps):
        row_copy(i).wait()
    shifts(jnp.maximum(norms, keys(1, OWN, OWN)))

    keep = pltpu.make_async_copy(hid.at[pl.ds(TOK, TOK)], hid_out, out_sem.at[0])
    keep.start()
    early = 2 * Q_BLK
    least = attend(0, early, least)
    pieces = TOK // CHUNK

    def fin_copy(i):
        rows = pl.ds(pl.multiple_of(i * CHUNK, CHUNK), CHUNK)
        return pltpu.make_async_remote_copy(
            src_ref=fin.at[rows], dst_ref=far_ref.at[rows], send_sem=fin_send.at[i], recv_sem=fin_recv.at[i],
            device_id={'sp': peer}, device_id_type=MESH)

    def peer_mlp(i, carry):
        rows = pl.ds(pl.multiple_of(i * CHUNK, CHUNK), CHUNK)
        fin[rows, :] = layer_norm(mlp(rows, hid, o_t, proj[1], up[1], down[1]))

        @pl.when(i > 0)
        def _():
            fin_copy(i - 1).start()

        return carry

    lax.fori_loop(0, pieces, peer_mlp, 0)
    fin_copy(pieces - 1).start()
    least = attend(early, OWN - early, least)
    least_mine[...] = jnp.broadcast_to(jnp.min(least, axis=1, keepdims=True), (8, PAIR))
    shares = []
    for step in range(1, SP):
        share = pltpu.make_async_remote_copy(
            src_ref=least_mine, dst_ref=least_all.at[step - 1], send_sem=least_send.at[step - 1], recv_sem=least_recv.at[step - 1],
            device_id={'sp': lax.rem(me + step, SP)}, device_id_type=MESH)
        shares.append(share)
    give = pltpu.make_async_copy(o_t.at[:, pl.ds(TOK, TOK)], o_out, out_sem.at[1])
    give.start()
    for share in shares:
        share.start()
    for i in range(pieces):
        fin_copy(i).wait()
    for share in shares:
        share.wait()
    low = least_mine[...]
    for k in range(SP - 1):
        low = low * least_all[k]
    least_ref[...] = low
    keep.wait()
    give.wait()


def decode(exact, z, rank, pos, pos_x, wqkv, wproj, wup, wdown):
    return pl.pallas_call(
        functools.partial(decoder_kernel, exact),
        out_shape=(
            jax.ShapeDtypeStruct((TOK, DDIM), BF16),
            jax.ShapeDtypeStruct((TOK, DDIM), BF16),
            jax.ShapeDtypeStruct((DDIM, TOK), BF16),
            jax.ShapeDtypeStruct((8, PAIR), F32),
        ),
        in_specs=[VMEM] * 4 + [ANY] * 4,
        out_specs=(VMEM, ANY, ANY, VMEM),
        scratch_shapes=[
            pltpu.VMEM((LAYERS, 3 * DDIM, DDIM), BF16),
            pltpu.VMEM((LAYERS, DDIM, DDIM), BF16),
            pltpu.VMEM((LAYERS, DDIM, 4 * DDIM), BF16),
            pltpu.VMEM((LAYERS, 4 * DDIM, DDIM), BF16),
            pltpu.VMEM((OWN, DDIM), BF16),
            pltpu.VMEM((SEQ, DDIM), BF16),
            pltpu.VMEM((TOK, DDIM), BF16),
            pltpu.VMEM((DEC_HEADS, 4 * HEAD, OWN), BF16),
            pltpu.VMEM((8, OWN), F32),
            pltpu.VMEM((8, PAIR), F32),
            pltpu.VMEM((DEC_HEADS, SEQ, PAIR), BF16),
            pltpu.VMEM((DEC_HEADS, SEQ, PAIR), BF16),
            pltpu.VMEM((DDIM, SEQ), BF16),
            pltpu.VMEM((DDIM, OWN), BF16),
            pltpu.VMEM((SEQ if exact else 8, X_BLK), F32),
            pltpu.VMEM((8, PAIR), F32),
            pltpu.VMEM((SP - 1, 8, PAIR), F32),
            pltpu.SemaphoreType.DMA((LAYERS * 4,)),
            pltpu.SemaphoreType.DMA((SP - 1,)),
            pltpu.SemaphoreType.DMA((SP - 1,)),
            pltpu.SemaphoreType.REGULAR,
            pltpu.SemaphoreType.DMA((OWN // CHUNK,)),
            pltpu.SemaphoreType.DMA((OWN // CHUNK,)),
            pltpu.SemaphoreType.DMA((TOK // CHUNK,)),
            pltpu.SemaphoreType.DMA((TOK // CHUNK,)),
            pltpu.SemaphoreType.DMA((2,)),
        ],
        compiler_params=pltpu.CompilerParams(collective_id=2 if exact else 1, has_side_effects=True, vmem_limit_bytes=58 * 2 ** 20),
        cost_estimate=pl.CostEstimate(flops=60 * 10 ** 9, bytes_accessed=2 * 10 ** 7, transcendentals=6 * 10 ** 7),
        name='decoder_exact' if exact else 'decoder',
    )(z, rank, pos, pos_x, wqkv, wproj, wup, wdown)


def output_kernel(far_ref, hid, o_t, w_ref, proj_hbm, up_hbm, down_hbm, out_hbm, proj, up, down, buf, w_sem, out_sem):
    chip = lax.axis_index('sp') // 2
    loads = [pltpu.make_async_copy(src.at[LAYERS - 1], dst, w_sem.at[idx])
             for idx, (src, dst) in enumerate(((proj_hbm, proj), (up_hbm, up), (down_hbm, down)))]
    for copy in loads:
        copy.start()
    pieces = TOK // CHUNK

    def out_copy(slot, clip, i):
        rows = pl.ds(pl.multiple_of(i * CHUNK, CHUNK), CHUNK)
        return pltpu.make_async_copy(buf.at[slot], out_hbm.at[clip, rows], out_sem.at[slot])

    def far_rows(i, carry):
        buf[i] = dot(far_ref[pl.ds(pl.multiple_of(i * CHUNK, CHUNK), CHUNK), :], w_ref[...])
        out_copy(i, 1 - chip, i).start()
        return carry

    def near_rows(i, carry):
        rows = pl.ds(pl.multiple_of(i * CHUNK, CHUNK), CHUNK)
        buf[pieces + i] = dot(layer_norm(mlp(rows, hid, o_t, proj[...], up[...], down[...])), w_ref[...])
        out_copy(pieces + i, chip, i).start()
        return carry

    lax.fori_loop(0, pieces, far_rows, 0)
    for copy in loads:
        copy.wait()
    lax.fori_loop(0, pieces, near_rows, 0)
    for i in range(pieces):
        out_copy(i, 1 - chip, i).wait()
        out_copy(pieces + i, chip, i).wait()


def project(far, hid, o_t, w_out, proj, up, down):
    return pl.pallas_call(
        output_kernel,
        out_shape=jax.ShapeDtypeStruct((CLIPS, TOK, PATCH), F32),
        in_specs=[VMEM] * 4 + [ANY] * 3,
        out_specs=ANY,
        scratch_shapes=[
            pltpu.VMEM((DDIM, DDIM), BF16),
            pltpu.VMEM((DDIM, 4 * DDIM), BF16),
            pltpu.VMEM((4 * DDIM, DDIM), BF16),
            pltpu.VMEM((CLIPS * TOK // CHUNK, CHUNK, PATCH), F32),
            pltpu.SemaphoreType.DMA((3,)),
            pltpu.SemaphoreType.DMA((CLIPS * TOK // CHUNK,)),
        ],
        compiler_params=pltpu.CompilerParams(vmem_limit_bytes=62 * 2 ** 20),
        cost_estimate=pl.CostEstimate(flops=5 * 10 ** 9, bytes_accessed=15 * 10 ** 6, transcendentals=0),
        name='output',
    )(far, hid, o_t, w_out, proj, up, down)


def solution(mesh):
    def local_program(patches, vis_mask, enc_pos, dec_pos, w_pe, b_pe, enc_qkv, enc_proj, enc_up, enc_down, w_ed, mask_token, dec_qkv, dec_proj, dec_up, dec_down, w_out):
        enc_qkv_t = jnp.transpose(enc_qkv, (0, 2, 3, 4, 1)).reshape(LAYERS, 3 * DIM, DIM)
        dec_qkv_t = jnp.transpose(dec_qkv, (0, 2, 3, 4, 1)).reshape(LAYERS, 3 * DDIM, DDIM)
        enc_proj2 = enc_proj.reshape(LAYERS, DIM, DIM)
        dec_proj2 = dec_proj.reshape(LAYERS, DDIM, DDIM)
        z, rank, pos_x = encode(vis_mask, b_pe, mask_token, patches, enc_pos, w_pe, dec_pos, w_ed,
                                enc_qkv_t, enc_proj2, enc_up, enc_down)
        args = (z, rank, dec_pos, pos_x, dec_qkv_t, dec_proj2, dec_up, dec_down)
        far, hid, o_t, least = decode(False, *args)
        far, hid, o_t = lax.cond(
            least[0, 0] > 0.5, lambda near, _: near, lambda _, full: tuple(decode(True, *full)[:3]), (far, hid, o_t), args)
        return project(far, hid, o_t, w_out, dec_proj2, dec_up, dec_down)

    row_spec = P('dp', 'sp', None)
    pos_spec = P(('dp', 'sp'), None)
    arg_specs = (row_spec, P('dp', 'sp'), pos_spec, pos_spec) + (P(),) * 13
    return jax.shard_map(local_program, mesh=mesh, in_specs=arg_specs, out_specs=row_spec, check_vma=False)
```

```python
import functools
import math

import jax
import jax.numpy as jnp
from jax import lax
from jax.experimental import pallas as pl
from jax.experimental.pallas import tpu as pltpu
from jax.sharding import PartitionSpec as P

F32 = jnp.float32
BF16 = jnp.bfloat16
MESH = pl.DeviceIdType.MESH
VMEM = pl.BlockSpec(memory_space=pltpu.VMEM)
ANY = pl.BlockSpec(memory_space=pl.ANY)

SP = 4
CLIPS = 2
TOK = 768
PATCH = 1536
DIM = 768
ENC_HEADS = 12
HEAD = 64
DDIM = 384
DEC_HEADS = 6
VIS = 96
WIN = 2 * VIS
ROWS = SP * VIS
OWN = 2 * TOK
SEQ = SP * TOK
LAYERS = 2
EXP_SCALE = HEAD ** -0.5 * math.log2(math.e)


def dot(lhs, rhs):
    return jnp.dot(lhs, rhs, preferred_element_type=F32)


def dot_nt(lhs, rhs):
    return lax.dot_general(lhs, rhs, (((1,), (1,)), ((), ())), preferred_element_type=F32)


def dot_tn(lhs, rhs):
    return lax.dot_general(lhs, rhs, (((0,), (0,)), ((), ())), preferred_element_type=F32)


def layer_norm(hidden):
    hid = hidden.astype(F32)
    centred = hid - jnp.mean(hid, axis=-1, keepdims=True)
    var = jnp.mean(centred * centred, axis=-1, keepdims=True)
    return (centred * lax.rsqrt(var + 1e-6)).astype(BF16)


def gelu(val):
    return (0.5 * val * (1.0 + lax.erf(val * math.sqrt(0.5)))).astype(BF16)


def col_max(val):
    return jnp.max(val, axis=0, keepdims=True)


def col_sum(val):
    return jnp.sum(val, axis=0, keepdims=True)


MINE = ROWS // 2
Q_PAD = 256


def encoder_kernel(mask_ref, bpe_ref, token_ref, patch_hbm, pos_hbm, wpe_hbm, dec_pos_hbm, wed_ref, qkv_hbm, proj_hbm, up_hbm, down_hbm,
                   z_ref, rank_ref, pos_out,
                   patch, pos, wpe, qkv, proj, up, down, masks, sendbuf, win, hall, hid, norm, norm_q, q_t, k_n, v_t, o_t,
                   in_sem, w_sem, mask_send, mask_recv, win_send, win_recv, pos_send, pos_recv, row_send, row_recv):
    me = lax.axis_index('sp')
    chip = me // 2
    core = me - 2 * chip
    peer = lax.rem(me + 2, SP)
    sib = me + 1 - 2 * core
    diag = lax.rem(sib + 2, SP)

    near_load = pltpu.make_async_copy(patch_hbm.at[chip], patch.at[chip], in_sem.at[3])
    loads = [pltpu.make_async_copy(src, dst, in_sem.at[idx])
             for idx, (src, dst) in enumerate(((patch_hbm.at[1 - chip], patch.at[1 - chip]), (wpe_hbm, wpe), (pos_hbm, pos)))]
    for copy in loads:
        copy.start()
    barrier = pltpu.get_barrier_semaphore()
    for other in (peer, sib, diag):
        pl.semaphore_signal(barrier, inc=1, device_id={'sp': other}, device_id_type=MESH)
    order_row = lax.broadcasted_iota(jnp.int32, (TOK, TOK), 0)
    order_col = lax.broadcasted_iota(jnp.int32, (TOK, TOK), 1)
    before = jnp.where(order_row < order_col, 1.0, 0.0).astype(BF16)
    mine = mask_ref[...].astype(F32)
    mine_rank = dot(jnp.concatenate([mine] * SP, axis=0).astype(BF16), before)[0:CLIPS]
    slot_of = jnp.where(mine > 0.0, mine_rank, -1.0)
    pl.semaphore_wait(barrier, 3)

    def send(src, dst, send_sem, recv_sem, dev):
        copy = pltpu.make_async_remote_copy(
            src_ref=src, dst_ref=dst, send_sem=send_sem, recv_sem=recv_sem, device_id={'sp': dev}, device_id_type=MESH)
        copy.start()
        return copy

    mask_copies = [send(mask_ref, masks.at[step - 1], mask_send.at[step - 1], mask_recv.at[step - 1], lax.rem(me + step, SP))
                   for step in range(1, SP)]
    for copy in loads:
        copy.wait()
    near_load.start()
    copies = []
    for layer in range(LAYERS):
        for idx, (src, dst) in enumerate(((qkv_hbm, qkv), (proj_hbm, proj), (up_hbm, up), (down_hbm, down))):
            copy = pltpu.make_async_copy(src.at[layer], dst.at[layer], w_sem.at[layer * 4 + idx])
            copy.start()
            copies.append(copy)

    bias = bpe_ref[...].astype(F32).reshape(1, DIM)

    def window(clip, slots):
        rows = lax.broadcasted_iota(jnp.int32, (WIN, TOK), 0).astype(F32)
        hit = jnp.where(rows == slots, 1.0, 0.0)
        select = hit.astype(BF16)
        moved = dot(select, patch[clip]).astype(BF16)
        occupied = jnp.sum(hit, axis=1, keepdims=True)
        emb = dot(moved, wpe[...]) + occupied * bias + dot(select, pos[...])
        return emb.astype(BF16)

    far = jnp.where(chip == 0, slot_of[1:2], slot_of[0:1])
    near = jnp.where(chip == 0, slot_of[0:1], slot_of[1:2])
    sendbuf[...] = window(1 - chip, far)
    to_peer = send(sendbuf, win.at[1], win_send.at[0], win_recv.at[0], peer)
    near_load.wait()
    win[0] = window(chip, near)
    to_sib = send(win.at[0], win.at[2], win_send.at[1], win_recv.at[1], sib)

    for copy in mask_copies:
        copy.wait()
    stacked = jnp.concatenate([mine] + [masks[k].astype(F32) for k in range(SP - 1)], axis=0)
    local = dot(stacked.astype(BF16), before)
    counts = jnp.sum(stacked, axis=1, keepdims=True)
    row_dev = lax.rem(me - lax.broadcasted_iota(jnp.int32, (CLIPS * SP, 1), 0) // CLIPS + SP, SP)
    base = jnp.zeros((CLIPS * SP, 1), F32)
    for k in range(SP):
        dev_k = lax.rem(me - k + SP, SP)
        tiled = jnp.concatenate([counts[CLIPS * k:CLIPS * k + CLIPS]] * SP, axis=0)
        base = base + jnp.where(dev_k < row_dev, tiled, 0.0)
    rank_ref[...] = jnp.where(stacked > 0.0, local + base, float(ROWS)).astype(jnp.int32)

    def placement(slot):
        def pick(val):
            two = val[CLIPS * slot:CLIPS * slot + CLIPS]
            return jnp.where(chip == 0, two[0:1], two[1:2])

        start, size = pick(base), pick(counts)
        rows = lax.broadcasted_iota(jnp.int32, (ROWS, WIN), 0).astype(F32)
        cols = lax.broadcasted_iota(jnp.int32, (ROWS, WIN), 1).astype(F32)
        return jnp.where((rows == cols + start) & (cols < size), 1.0, 0.0)

    even = core == 0
    left, right = placement(1), placement(3)
    place = [placement(0), placement(2), jnp.where(even, right, left), jnp.where(even, left, right)]
    to_peer.wait_recv()
    relay = send(win.at[1], win.at[3], win_send.at[2], win_recv.at[2], sib)
    pos_peer = send(dec_pos_hbm, pos_out.at[0], pos_send.at[0], pos_recv.at[0], peer)
    pos_sib = send(dec_pos_hbm, pos_out.at[1], pos_send.at[1], pos_recv.at[1], sib)
    total = dot(place[0].astype(BF16), win[0]) + dot(place[1].astype(BF16), win[1])
    to_sib.wait_recv()
    total = total + dot(place[2].astype(BF16), win[2])
    relay.wait_recv()
    total = total + dot(place[3].astype(BF16), win[3])
    hall[...] = total.astype(BF16)
    own = pl.ds(pl.multiple_of(core * MINE, MINE), MINE)
    hid[...] = hall[own, :]
    norm[0] = layer_norm(hall[...])
    norm_q[MINE:] = jnp.zeros((Q_PAD - MINE, DIM), BF16)
    zero = jnp.zeros((HEAD, Q_PAD), BF16)
    pos_diag = swap = None

    for layer in range(LAYERS):
        copies[layer * 4].wait()
        norm_q[0:MINE] = norm[layer, own, :]
        q_t[...] = dot_nt(qkv[layer, 0:DIM], norm_q[...]).astype(BF16)
        if swap is not None:
            swap.wait()
        k_n[...] = dot_nt(norm[layer], qkv[layer, DIM:2 * DIM]).astype(BF16)
        v_t[...] = dot_nt(qkv[layer, 2 * DIM:3 * DIM], norm[layer]).astype(BF16)

        def heads(group, carry):
            scores, weights = [], []
            for pair in range(2):
                lanes = pl.ds(pl.multiple_of((2 * group + pair) * 2 * HEAD, 2 * HEAD), 2 * HEAD)
                for odd in range(2):
                    rows = pl.ds(pl.multiple_of((4 * group + 2 * pair + odd) * HEAD, HEAD), HEAD)
                    q_head = q_t[rows, :]
                    q_both = jnp.concatenate([zero, q_head] if odd else [q_head, zero], axis=0)
                    scores.append(dot(k_n[:, lanes], q_both))
            for s in scores:
                e = jnp.exp2(s * EXP_SCALE - col_max(s) * EXP_SCALE)
                weights.append((e.astype(BF16), 1.0 / col_sum(e)))
            for idx, (e, scale) in enumerate(weights):
                rows = pl.ds(pl.multiple_of((4 * group + idx) * HEAD, HEAD), HEAD)
                o_t[rows, :] = (dot(v_t[rows, :], e) * scale).astype(BF16)
            return carry

        lax.fori_loop(0, ENC_HEADS // 4, heads, 0)
        copies[layer * 4 + 1].wait()
        mid = (hid[...].astype(F32) + dot_tn(o_t[...], proj[layer])[0:MINE]).astype(BF16)
        rows_norm = layer_norm(mid)
        copies[layer * 4 + 2].wait()
        copies[layer * 4 + 3].wait()
        if layer == LAYERS - 1:
            pos_peer.wait_recv()
            pos_diag = send(pos_out.at[0], pos_out.at[2], pos_send.at[2], pos_recv.at[2], sib)
        acc = None
        for lo in range(0, 4 * DIM, DIM):
            act = gelu(dot(rows_norm, up[layer, :, lo:lo + DIM]))
            part = dot(act, down[layer, lo:lo + DIM, :])
            acc = part if acc is None else acc + part
        out = (mid.astype(F32) + acc).astype(BF16)
        if layer < LAYERS - 1:
            hid[...] = out
            norm[layer + 1, own, :] = layer_norm(out)
            swap = send(norm.at[layer + 1, own], norm.at[layer + 1, own], row_send.at[layer], row_recv.at[layer], sib)
    z_ref[own, :] = dot(layer_norm(out), wed_ref[...]).astype(BF16)
    first = lax.broadcasted_iota(jnp.int32, (2 * HEAD, DDIM), 0) == 0
    z_ref[ROWS:] = jnp.where(first, token_ref[...].astype(F32).reshape(1, DDIM), 0.0).astype(BF16)
    last = send(z_ref.at[own], z_ref.at[own], row_send.at[LAYERS - 1], row_recv.at[LAYERS - 1], sib)
    to_peer.wait_send()
    to_sib.wait_send()
    relay.wait_send()
    pos_peer.wait_send()
    pos_sib.wait()
    pos_diag.wait()
    last.wait()


def encode(mask, bpe, token, patches, enc_pos, wpe, dec_pos, wed, qkv_t, proj, up, down):
    return pl.pallas_call(
        encoder_kernel,
        out_shape=(
            jax.ShapeDtypeStruct((ROWS + 2 * HEAD, DDIM), BF16),
            jax.ShapeDtypeStruct((CLIPS * SP, TOK), jnp.int32),
            jax.ShapeDtypeStruct((SP - 1, TOK, DDIM), BF16),
        ),
        in_specs=[VMEM] * 3 + [ANY] * 4 + [VMEM] + [ANY] * 4,
        out_specs=(VMEM, VMEM, ANY),
        scratch_shapes=[
            pltpu.VMEM((CLIPS, TOK, PATCH), BF16),
            pltpu.VMEM((TOK, DIM), BF16),
            pltpu.VMEM((PATCH, DIM), BF16),
            pltpu.VMEM((LAYERS, 3 * DIM, DIM), BF16),
            pltpu.VMEM((LAYERS, DIM, DIM), BF16),
            pltpu.VMEM((LAYERS, DIM, 4 * DIM), BF16),
            pltpu.VMEM((LAYERS, 4 * DIM, DIM), BF16),
            pltpu.VMEM((SP - 1, CLIPS, TOK), jnp.int32),
            pltpu.VMEM((WIN, DIM), BF16),
            pltpu.VMEM((SP, WIN, DIM), BF16),
            pltpu.VMEM((ROWS, DIM), BF16),
            pltpu.VMEM((MINE, DIM), BF16),
            pltpu.VMEM((LAYERS, ROWS, DIM), BF16),
            pltpu.VMEM((Q_PAD, DIM), BF16),
            pltpu.VMEM((DIM, Q_PAD), BF16),
            pltpu.VMEM((ROWS, DIM), BF16),
            pltpu.VMEM((DIM, ROWS), BF16),
            pltpu.VMEM((DIM, Q_PAD), BF16),
            pltpu.SemaphoreType.DMA((4,)),
            pltpu.SemaphoreType.DMA((LAYERS * 4,)),
            pltpu.SemaphoreType.DMA((SP - 1,)),
            pltpu.SemaphoreType.DMA((SP - 1,)),
            pltpu.SemaphoreType.DMA((3,)),
            pltpu.SemaphoreType.DMA((3,)),
            pltpu.SemaphoreType.DMA((3,)),
            pltpu.SemaphoreType.DMA((3,)),
            pltpu.SemaphoreType.DMA((LAYERS,)),
            pltpu.SemaphoreType.DMA((LAYERS,)),
        ],
        compiler_params=pltpu.CompilerParams(collective_id=0, has_side_effects=True, vmem_limit_bytes=58 * 2 ** 20),
        cost_estimate=pl.CostEstimate(flops=12 * 10 ** 9, bytes_accessed=4 * 10 ** 7, transcendentals=0),
        name='encoder',
    )(mask, bpe, token, patches, enc_pos, wpe, dec_pos, wed, qkv_t, proj, up, down)


Q_BLK = 256
K_BLK = 256
CHUNK = 256
WIDE = 512
PAIR = 2 * HEAD


def fill_rows(start, count, step, body):
    def run(i, carry):
        body(pl.ds(pl.multiple_of(start + i * step, step), step))
        return carry

    lax.fori_loop(0, count // step, run, 0)


def make_queries(rows, norm, w_q, q_3):
    q = dot_nt(w_q, norm[rows, :]).astype(BF16).astype(F32) * EXP_SCALE
    hi = q.astype(BF16)
    rest = q - hi.astype(F32)
    mid = rest.astype(BF16)
    low = (rest - mid.astype(F32)).astype(BF16)
    zero = jnp.zeros((HEAD, q.shape[1]), BF16)
    for head in range(DEC_HEADS):
        part = slice(head * HEAD, (head + 1) * HEAD)
        tail = (low[part], zero) if head % 2 == 0 else (zero, low[part])
        for idx, val in enumerate((hi[part], mid[part]) + tail):
            q_3[head, idx * HEAD:(idx + 1) * HEAD, rows] = val


def make_keys(rows, norm, w_k, w_v, k_n, k_dup, v_t):
    a = norm[rows, :]
    k = dot_nt(a, w_k)
    first = lax.broadcasted_iota(jnp.int32, (k.shape[0], PAIR), 1) < HEAD
    for pair in range(DEC_HEADS // 2):
        both = k[:, pair * PAIR:(pair + 1) * PAIR]
        turned = pltpu.roll(both, HEAD, axis=1)
        k_n[pair, rows, :] = both.astype(BF16)
        k_dup[2 * pair, rows, :] = jnp.where(first, both, turned).astype(BF16)
        k_dup[2 * pair + 1, rows, :] = jnp.where(first, turned, both).astype(BF16)
    v_t[:, rows] = dot_nt(w_v, a).astype(BF16)


def attention(start, count, q_3, k_n, k_dup, v_t, o_t, s_even, s_odd):
    blocks = count // Q_BLK
    units = DEC_HEADS * blocks

    def place(unit):
        head = unit // blocks
        return head, pl.ds(pl.multiple_of(start + (unit - head * blocks) * Q_BLK, Q_BLK), Q_BLK)

    def mixed(unit_q, s_q, unit_p, s_p, max8):
        if unit_q is not None:
            head_q, cols_q = place(unit_q)
            q = q_3[head_q, :, cols_q]
        if unit_p is not None:
            head_p, cols_p = place(unit_p)
            shift = col_max(max8)
            v_rows = pl.ds(pl.multiple_of(head_p * HEAD, HEAD), HEAD)
        new_max = total = acc = None
        for idx in range(SEQ // K_BLK):
            rows = slice(idx * K_BLK, (idx + 1) * K_BLK)
            if unit_p is not None:
                e = jnp.exp2(s_p[rows, :] - shift)
                t = jnp.sum(e.reshape(K_BLK // 8, 8, Q_BLK), axis=0)
                total = t if total is None else total + t
                o = dot(v_t[v_rows, rows], e.astype(BF16))
                acc = o if acc is None else acc + o
            if unit_q is not None:
                keys = jnp.concatenate([k_dup[head_q, rows, :], k_n[head_q // 2, rows, :]], axis=1)
                s = dot(keys, q)
                s_q[rows, :] = s
                m = jnp.max(s.reshape(K_BLK // 8, 8, Q_BLK), axis=0)
                new_max = m if new_max is None else jnp.maximum(new_max, m)
        if unit_p is not None:
            o_t[v_rows, cols_p] = (acc * (1.0 / col_sum(total))).astype(BF16)
        return new_max

    first = mixed(0, s_even, None, None, None)

    def body(i, max8):
        unit = 2 * i
        max_odd = mixed(unit + 1, s_odd, unit, s_even, max8)
        return mixed(jnp.minimum(unit + 2, units - 1), s_even, unit + 1, s_odd, max_odd)

    lax.fori_loop(0, units // 2, body, first)


def mlp(rows, hid, o_t, w_proj, w_up, w_down):
    mid = (hid[rows, :].astype(F32) + dot_tn(o_t[:, rows], w_proj)).astype(BF16)
    act = gelu(dot(layer_norm(mid), w_up))
    return (mid.astype(F32) + dot(act, w_down)).astype(BF16)


def decoder_kernel(z_ref, rank_ref, pos_me, pos_x, qkv_hbm, proj_hbm, up_hbm, down_hbm, both_ref,
                   qkv, proj, up, down, hid, norm, fin, q_3, k_n, k_dup, v_t, o_t, s_even, s_odd, w_sem, ready, row_send, row_recv, fin_send, fin_recv, pos, pos_sem):
    me = lax.axis_index('sp')
    chip = me // 2
    core = me - 2 * chip
    peer = lax.rem(me + 2, SP)
    sib = me + 1 - 2 * core
    diag = lax.rem(sib + 2, SP)

    fetch = [pltpu.make_async_copy(src, pos.at[idx], pos_sem.at[idx])
             for idx, src in enumerate((pos_me, pos_x.at[0], pos_x.at[1], pos_x.at[2]))]
    for copy in fetch:
        copy.start()
    copies = []
    for layer in range(LAYERS):
        for idx, (src, dst) in enumerate(((qkv_hbm, qkv), (proj_hbm, proj), (up_hbm, up), (down_hbm, down))):
            copy = pltpu.make_async_copy(src.at[layer], dst.at[layer], w_sem.at[layer * 4 + idx])
            copy.start()
            copies.append(copy)
    barrier = pltpu.get_barrier_semaphore()
    for other in (peer, sib):
        pl.semaphore_signal(barrier, inc=1, device_id={'sp': other}, device_id_type=MESH)
    pl.semaphore_wait(barrier, 2)

    def tokens(dev, idx):
        slot = lax.rem(me - dev + SP, SP)
        rank = rank_ref[pl.ds(2 * slot + chip, 1), :]
        rank_col = jnp.transpose(jnp.broadcast_to(rank.astype(F32), (8, TOK)))[:, 0:1]
        lanes = lax.broadcasted_iota(jnp.int32, (TOK, ROWS + 2 * HEAD), 1).astype(F32)
        select = jnp.where(lanes == rank_col, 1.0, 0.0).astype(BF16)
        fetch[idx].wait()
        return (dot(select, z_ref[...]) + pos[idx].astype(F32)).astype(BF16)

    hid[0:TOK] = tokens(peer, 1)
    hid[TOK:OWN] = tokens(me, 0)
    norm[OWN:OWN + TOK] = layer_norm(tokens(diag, 3))
    norm[OWN + TOK:SEQ] = layer_norm(tokens(sib, 2))

    def own_norm(rows):
        norm[rows, :] = layer_norm(hid[rows, :])

    fill_rows(0, OWN, CHUNK, own_norm)

    def queries(layer):
        fill_rows(0, OWN, WIDE, lambda rows: make_queries(rows, norm, qkv[layer, 0:DDIM], q_3))

    def keys(layer, start, count):
        fill_rows(start, count, WIDE, lambda rows: make_keys(
            rows, norm, qkv[layer, DDIM:2 * DDIM], qkv[layer, 2 * DDIM:3 * DDIM], k_n, k_dup, v_t))

    copies[0].wait()
    queries(0)
    keys(0, 0, SEQ)
    pl.semaphore_signal(ready, inc=1, device_id={'sp': sib}, device_id_type=MESH)
    attention(0, OWN, q_3, k_n, k_dup, v_t, o_t, s_even, s_odd)
    pl.semaphore_wait(ready, 1)
    for copy in copies[1:]:
        copy.wait()
    steps = OWN // CHUNK

    def row_copy(i):
        src = pl.ds(pl.multiple_of(i * CHUNK, CHUNK), CHUNK)
        dst = pl.ds(pl.multiple_of(OWN + i * CHUNK, CHUNK), CHUNK)
        return pltpu.make_async_remote_copy(
            src_ref=norm.at[src], dst_ref=norm.at[dst], send_sem=row_send.at[i], recv_sem=row_recv.at[i],
            device_id={'sp': sib}, device_id_type=MESH)

    def first_mlp(i, carry):
        rows = pl.ds(pl.multiple_of(i * CHUNK, CHUNK), CHUNK)
        val = mlp(rows, hid, o_t, proj[0], up[0], down[0])
        hid[rows, :] = val
        norm[rows, :] = layer_norm(val)

        @pl.when(i > 0)
        def _():
            row_copy(i - 1).start()

        return carry

    lax.fori_loop(0, steps, first_mlp, 0)
    queries(1)
    row_copy(steps - 1).start()
    keys(1, 0, OWN)
    for i in range(steps):
        row_copy(i).wait()
    keys(1, OWN, OWN)

    attention(0, TOK, q_3, k_n, k_dup, v_t, o_t, s_even, s_odd)
    pieces = TOK // CHUNK

    def fin_copy(i):
        rows = pl.ds(pl.multiple_of(i * CHUNK, CHUNK), CHUNK)
        return pltpu.make_async_remote_copy(
            src_ref=fin.at[rows], dst_ref=both_ref.at[chip, rows], send_sem=fin_send.at[i], recv_sem=fin_recv.at[i],
            device_id={'sp': peer}, device_id_type=MESH)

    def last_mlp(i, carry, start):
        src = pl.ds(pl.multiple_of(start + i * CHUNK, CHUNK), CHUNK)
        rows = pl.ds(pl.multiple_of(i * CHUNK, CHUNK), CHUNK)
        val = layer_norm(mlp(src, hid, o_t, proj[1], up[1], down[1]))
        if start == 0:
            fin[rows, :] = val

            @pl.when(i > 0)
            def _():
                fin_copy(i - 1).start()
        else:
            both_ref[chip, rows, :] = val
        return carry

    lax.fori_loop(0, pieces, functools.partial(last_mlp, start=0), 0)
    fin_copy(pieces - 1).start()
    attention(TOK, TOK, q_3, k_n, k_dup, v_t, o_t, s_even, s_odd)
    lax.fori_loop(0, pieces, functools.partial(last_mlp, start=TOK), 0)
    for i in range(pieces):
        fin_copy(i).wait()


def decode(z, rank, pos, pos_x, wqkv, wproj, wup, wdown):
    return pl.pallas_call(
        decoder_kernel,
        out_shape=jax.ShapeDtypeStruct((CLIPS, TOK, DDIM), BF16),
        in_specs=[VMEM] * 2 + [ANY] * 6,
        out_specs=VMEM,
        scratch_shapes=[
            pltpu.VMEM((LAYERS, 3 * DDIM, DDIM), BF16),
            pltpu.VMEM((LAYERS, DDIM, DDIM), BF16),
            pltpu.VMEM((LAYERS, DDIM, 4 * DDIM), BF16),
            pltpu.VMEM((LAYERS, 4 * DDIM, DDIM), BF16),
            pltpu.VMEM((OWN, DDIM), BF16),
            pltpu.VMEM((SEQ, DDIM), BF16),
            pltpu.VMEM((TOK, DDIM), BF16),
            pltpu.VMEM((DEC_HEADS, 4 * HEAD, OWN), BF16),
            pltpu.VMEM((DEC_HEADS // 2, SEQ, PAIR), BF16),
            pltpu.VMEM((DEC_HEADS, SEQ, PAIR), BF16),
            pltpu.VMEM((DDIM, SEQ), BF16),
            pltpu.VMEM((DDIM, OWN), BF16),
            pltpu.VMEM((SEQ, Q_BLK), F32),
            pltpu.VMEM((SEQ, Q_BLK), F32),
            pltpu.SemaphoreType.DMA((LAYERS * 4,)),
            pltpu.SemaphoreType.REGULAR,
            pltpu.SemaphoreType.DMA((OWN // CHUNK,)),
            pltpu.SemaphoreType.DMA((OWN // CHUNK,)),
            pltpu.SemaphoreType.DMA((TOK // CHUNK,)),
            pltpu.SemaphoreType.DMA((TOK // CHUNK,)),
            pltpu.VMEM((SP, TOK, DDIM), BF16),
            pltpu.SemaphoreType.DMA((SP,)),
        ],
        compiler_params=pltpu.CompilerParams(collective_id=1, has_side_effects=True, vmem_limit_bytes=58 * 2 ** 20),
        cost_estimate=pl.CostEstimate(flops=60 * 10 ** 9, bytes_accessed=2 * 10 ** 7, transcendentals=6 * 10 ** 7),
        name='decoder',
    )(z, rank, pos, pos_x, wqkv, wproj, wup, wdown)


def output_kernel(both_ref, w_ref, out_hbm, buf, sem):
    pieces = TOK // CHUNK

    def out_copy(i):
        clip = i // pieces
        rows = pl.ds(pl.multiple_of((i - clip * pieces) * CHUNK, CHUNK), CHUNK)
        return pltpu.make_async_copy(buf.at[i], out_hbm.at[clip, rows], sem.at[i])

    def body(i, carry):
        clip = i // pieces
        rows = pl.ds(pl.multiple_of((i - clip * pieces) * CHUNK, CHUNK), CHUNK)
        buf[i] = dot(both_ref[clip, rows, :], w_ref[...])
        out_copy(i).start()
        return carry

    lax.fori_loop(0, CLIPS * pieces, body, 0)
    for i in range(CLIPS * pieces):
        out_copy(i).wait()


def project(both, w_out):
    return pl.pallas_call(
        output_kernel,
        out_shape=jax.ShapeDtypeStruct((CLIPS, TOK, PATCH), F32),
        in_specs=[VMEM] * 2,
        out_specs=ANY,
        scratch_shapes=[
            pltpu.VMEM((CLIPS * TOK // CHUNK, CHUNK, PATCH), F32),
            pltpu.SemaphoreType.DMA((CLIPS * TOK // CHUNK,)),
        ],
        compiler_params=pltpu.CompilerParams(vmem_limit_bytes=62 * 2 ** 20),
        cost_estimate=pl.CostEstimate(flops=2 * 10 ** 9, bytes_accessed=12 * 10 ** 6, transcendentals=0),
        name='output',
    )(both, w_out)


def solution(mesh):
    def local_program(patches, vis_mask, enc_pos, dec_pos, w_pe, b_pe, enc_qkv, enc_proj, enc_up, enc_down, w_ed, mask_token, dec_qkv, dec_proj, dec_up, dec_down, w_out):
        enc_qkv_t = jnp.transpose(enc_qkv, (0, 2, 3, 4, 1)).reshape(LAYERS, 3 * DIM, DIM)
        dec_qkv_t = jnp.transpose(dec_qkv, (0, 2, 3, 4, 1)).reshape(LAYERS, 3 * DDIM, DDIM)
        enc_proj2 = enc_proj.reshape(LAYERS, DIM, DIM)
        dec_proj2 = dec_proj.reshape(LAYERS, DDIM, DDIM)
        z, rank, pos_x = encode(vis_mask, b_pe, mask_token, patches, enc_pos, w_pe, dec_pos, w_ed,
                                enc_qkv_t, enc_proj2, enc_up, enc_down)
        both = decode(z, rank, dec_pos, pos_x, dec_qkv_t, dec_proj2, dec_up, dec_down)
        return project(both, w_out)

    row_spec = P('dp', 'sp', None)
    pos_spec = P(('dp', 'sp'), None)
    arg_specs = (row_spec, P('dp', 'sp'), pos_spec, pos_spec) + (P(),) * 13
    return jax.shard_map(local_program, mesh=mesh, in_specs=arg_specs, out_specs=row_spec, check_vma=False)
```

```python
import functools
import math

import jax
import jax.numpy as jnp
from jax import lax
from jax.experimental import pallas as pl
from jax.experimental.pallas import tpu as pltpu
from jax.sharding import PartitionSpec as P

F32 = jnp.float32
BF16 = jnp.bfloat16
MESH = pl.DeviceIdType.MESH
VMEM = pl.BlockSpec(memory_space=pltpu.VMEM)
ANY = pl.BlockSpec(memory_space=pl.ANY)

SP = 4
CLIPS = 2
TOK = 768
PATCH = 1536
DIM = 768
ENC_HEADS = 12
HEAD = 64
DDIM = 384
DEC_HEADS = 6
VIS = 96
WIN = 2 * VIS
ROWS = SP * VIS
OWN = 2 * TOK
SEQ = SP * TOK
LAYERS = 2
EXP_SCALE = HEAD ** -0.5 * math.log2(math.e)


def dot(lhs, rhs):
    return jnp.dot(lhs, rhs, preferred_element_type=F32)


def dot_nt(lhs, rhs):
    return lax.dot_general(lhs, rhs, (((1,), (1,)), ((), ())), preferred_element_type=F32)


def dot_tn(lhs, rhs):
    return lax.dot_general(lhs, rhs, (((0,), (0,)), ((), ())), preferred_element_type=F32)


def layer_norm(hidden):
    hid = hidden.astype(F32)
    centred = hid - jnp.mean(hid, axis=-1, keepdims=True)
    var = jnp.mean(centred * centred, axis=-1, keepdims=True)
    return (centred * lax.rsqrt(var + 1e-6)).astype(BF16)


def gelu(val):
    return (0.5 * val * (1.0 + lax.erf(val * math.sqrt(0.5)))).astype(BF16)


def col_max(val):
    return jnp.max(val, axis=0, keepdims=True)


def col_sum(val):
    return jnp.sum(val, axis=0, keepdims=True)


MINE = ROWS // 2
Q_PAD = 256


def encoder_kernel(mask_ref, bpe_ref, token_ref, patch_hbm, pos_hbm, wpe_hbm, dec_pos_hbm, wed_ref, qkv_hbm, proj_hbm, up_hbm, down_hbm,
                   z_ref, rank_ref, pos_out,
                   patch, pos, wpe, qkv, proj, up, down, masks, sendbuf, win, hall, hid, norm, norm_q, q_t, k_n, v_t, o_t,
                   in_sem, w_sem, mask_send, mask_recv, win_send, win_recv, pos_send, pos_recv, row_send, row_recv):
    me = lax.axis_index('sp')
    chip = me // 2
    core = me - 2 * chip
    peer = lax.rem(me + 2, SP)
    sib = me + 1 - 2 * core
    diag = lax.rem(sib + 2, SP)

    near_load = pltpu.make_async_copy(patch_hbm.at[chip], patch.at[chip], in_sem.at[3])
    loads = [pltpu.make_async_copy(src, dst, in_sem.at[idx])
             for idx, (src, dst) in enumerate(((patch_hbm.at[1 - chip], patch.at[1 - chip]), (wpe_hbm, wpe), (pos_hbm, pos)))]
    for copy in loads:
        copy.start()
    barrier = pltpu.get_barrier_semaphore()
    for other in (peer, sib, diag):
        pl.semaphore_signal(barrier, inc=1, device_id={'sp': other}, device_id_type=MESH)
    order_row = lax.broadcasted_iota(jnp.int32, (TOK, TOK), 0)
    order_col = lax.broadcasted_iota(jnp.int32, (TOK, TOK), 1)
    before = jnp.where(order_row < order_col, 1.0, 0.0).astype(BF16)
    mine = mask_ref[...].astype(F32)
    mine_rank = dot(jnp.concatenate([mine] * SP, axis=0).astype(BF16), before)[0:CLIPS]
    slot_of = jnp.where(mine > 0.0, mine_rank, -1.0)
    pl.semaphore_wait(barrier, 3)

    def send(src, dst, send_sem, recv_sem, dev):
        copy = pltpu.make_async_remote_copy(
            src_ref=src, dst_ref=dst, send_sem=send_sem, recv_sem=recv_sem, device_id={'sp': dev}, device_id_type=MESH)
        copy.start()
        return copy

    mask_copies = [send(mask_ref, masks.at[step - 1], mask_send.at[step - 1], mask_recv.at[step - 1], lax.rem(me + step, SP))
                   for step in range(1, SP)]
    for copy in loads:
        copy.wait()
    near_load.start()
    copies = []
    for layer in range(LAYERS):
        for idx, (src, dst) in enumerate(((qkv_hbm, qkv), (proj_hbm, proj), (up_hbm, up), (down_hbm, down))):
            copy = pltpu.make_async_copy(src.at[layer], dst.at[layer], w_sem.at[layer * 4 + idx])
            copy.start()
            copies.append(copy)

    bias = bpe_ref[...].astype(F32).reshape(1, DIM)

    def window(clip, slots):
        rows = lax.broadcasted_iota(jnp.int32, (WIN, TOK), 0).astype(F32)
        hit = jnp.where(rows == slots, 1.0, 0.0)
        select = hit.astype(BF16)
        moved = dot(select, patch[clip]).astype(BF16)
        occupied = jnp.sum(hit, axis=1, keepdims=True)
        emb = dot(moved, wpe[...]) + occupied * bias + dot(select, pos[...])
        return emb.astype(BF16)

    far = jnp.where(chip == 0, slot_of[1:2], slot_of[0:1])
    near = jnp.where(chip == 0, slot_of[0:1], slot_of[1:2])
    sendbuf[...] = window(1 - chip, far)
    to_peer = send(sendbuf, win.at[1], win_send.at[0], win_recv.at[0], peer)
    near_load.wait()
    win[0] = window(chip, near)
    to_sib = send(win.at[0], win.at[2], win_send.at[1], win_recv.at[1], sib)

    for copy in mask_copies:
        copy.wait()
    stacked = jnp.concatenate([mine] + [masks[k].astype(F32) for k in range(SP - 1)], axis=0)
    local = dot(stacked.astype(BF16), before)
    counts = jnp.sum(stacked, axis=1, keepdims=True)
    row_dev = lax.rem(me - lax.broadcasted_iota(jnp.int32, (CLIPS * SP, 1), 0) // CLIPS + SP, SP)
    base = jnp.zeros((CLIPS * SP, 1), F32)
    for k in range(SP):
        dev_k = lax.rem(me - k + SP, SP)
        tiled = jnp.concatenate([counts[CLIPS * k:CLIPS * k + CLIPS]] * SP, axis=0)
        base = base + jnp.where(dev_k < row_dev, tiled, 0.0)
    rank_ref[...] = jnp.where(stacked > 0.0, local + base, float(ROWS)).astype(jnp.int32)

    def placement(slot):
        def pick(val):
            two = val[CLIPS * slot:CLIPS * slot + CLIPS]
            return jnp.where(chip == 0, two[0:1], two[1:2])

        start, size = pick(base), pick(counts)
        rows = lax.broadcasted_iota(jnp.int32, (ROWS, WIN), 0).astype(F32)
        cols = lax.broadcasted_iota(jnp.int32, (ROWS, WIN), 1).astype(F32)
        return jnp.where((rows == cols + start) & (cols < size), 1.0, 0.0)

    even = core == 0
    left, right = placement(1), placement(3)
    place = [placement(0), placement(2), jnp.where(even, right, left), jnp.where(even, left, right)]
    to_peer.wait_recv()
    relay = send(win.at[1], win.at[3], win_send.at[2], win_recv.at[2], sib)
    pos_peer = send(dec_pos_hbm, pos_out.at[0], pos_send.at[0], pos_recv.at[0], peer)
    pos_sib = send(dec_pos_hbm, pos_out.at[1], pos_send.at[1], pos_recv.at[1], sib)
    total = dot(place[0].astype(BF16), win[0]) + dot(place[1].astype(BF16), win[1])
    to_sib.wait_recv()
    total = total + dot(place[2].astype(BF16), win[2])
    relay.wait_recv()
    total = total + dot(place[3].astype(BF16), win[3])
    hall[...] = total.astype(BF16)
    own = pl.ds(pl.multiple_of(core * MINE, MINE), MINE)
    hid[...] = hall[own, :]
    norm[0] = layer_norm(hall[...])
    norm_q[MINE:] = jnp.zeros((Q_PAD - MINE, DIM), BF16)
    zero = jnp.zeros((HEAD, Q_PAD), BF16)
    pos_diag = swap = None

    for layer in range(LAYERS):
        copies[layer * 4].wait()
        norm_q[0:MINE] = norm[layer, own, :]
        q_t[...] = dot_nt(qkv[layer, 0:DIM], norm_q[...]).astype(BF16)
        if swap is not None:
            swap.wait()
        k_n[...] = dot_nt(norm[layer], qkv[layer, DIM:2 * DIM]).astype(BF16)
        v_t[...] = dot_nt(qkv[layer, 2 * DIM:3 * DIM], norm[layer]).astype(BF16)

        def heads(group, carry):
            scores, weights = [], []
            for pair in range(2):
                lanes = pl.ds(pl.multiple_of((2 * group + pair) * 2 * HEAD, 2 * HEAD), 2 * HEAD)
                for odd in range(2):
                    rows = pl.ds(pl.multiple_of((4 * group + 2 * pair + odd) * HEAD, HEAD), HEAD)
                    q_head = q_t[rows, :]
                    q_both = jnp.concatenate([zero, q_head] if odd else [q_head, zero], axis=0)
                    scores.append(dot(k_n[:, lanes], q_both))
            for s in scores:
                e = jnp.exp2(s * EXP_SCALE - col_max(s) * EXP_SCALE)
                weights.append((e.astype(BF16), 1.0 / col_sum(e)))
            for idx, (e, scale) in enumerate(weights):
                rows = pl.ds(pl.multiple_of((4 * group + idx) * HEAD, HEAD), HEAD)
                o_t[rows, :] = (dot(v_t[rows, :], e) * scale).astype(BF16)
            return carry

        lax.fori_loop(0, ENC_HEADS // 4, heads, 0)
        copies[layer * 4 + 1].wait()
        mid = (hid[...].astype(F32) + dot_tn(o_t[...], proj[layer])[0:MINE]).astype(BF16)
        rows_norm = layer_norm(mid)
        copies[layer * 4 + 2].wait()
        copies[layer * 4 + 3].wait()
        if layer == LAYERS - 1:
            pos_peer.wait_recv()
            pos_diag = send(pos_out.at[0], pos_out.at[2], pos_send.at[2], pos_recv.at[2], sib)
        acc = None
        for lo in range(0, 4 * DIM, DIM):
            act = gelu(dot(rows_norm, up[layer, :, lo:lo + DIM]))
            part = dot(act, down[layer, lo:lo + DIM, :])
            acc = part if acc is None else acc + part
        out = (mid.astype(F32) + acc).astype(BF16)
        if layer < LAYERS - 1:
            hid[...] = out
            norm[layer + 1, own, :] = layer_norm(out)
            swap = send(norm.at[layer + 1, own], norm.at[layer + 1, own], row_send.at[layer], row_recv.at[layer], sib)
    z_ref[own, :] = dot(layer_norm(out), wed_ref[...]).astype(BF16)
    first = lax.broadcasted_iota(jnp.int32, (2 * HEAD, DDIM), 0) == 0
    z_ref[ROWS:] = jnp.where(first, token_ref[...].astype(F32).reshape(1, DDIM), 0.0).astype(BF16)
    last = send(z_ref.at[own], z_ref.at[own], row_send.at[LAYERS - 1], row_recv.at[LAYERS - 1], sib)
    to_peer.wait_send()
    to_sib.wait_send()
    relay.wait_send()
    pos_peer.wait_send()
    pos_sib.wait()
    pos_diag.wait()
    last.wait()


def encode(mask, bpe, token, patches, enc_pos, wpe, dec_pos, wed, qkv_t, proj, up, down):
    return pl.pallas_call(
        encoder_kernel,
        out_shape=(
            jax.ShapeDtypeStruct((ROWS + 2 * HEAD, DDIM), BF16),
            jax.ShapeDtypeStruct((CLIPS * SP, TOK), jnp.int32),
            jax.ShapeDtypeStruct((SP - 1, TOK, DDIM), BF16),
        ),
        in_specs=[VMEM] * 3 + [ANY] * 4 + [VMEM] + [ANY] * 4,
        out_specs=(VMEM, VMEM, ANY),
        scratch_shapes=[
            pltpu.VMEM((CLIPS, TOK, PATCH), BF16),
            pltpu.VMEM((TOK, DIM), BF16),
            pltpu.VMEM((PATCH, DIM), BF16),
            pltpu.VMEM((LAYERS, 3 * DIM, DIM), BF16),
            pltpu.VMEM((LAYERS, DIM, DIM), BF16),
            pltpu.VMEM((LAYERS, DIM, 4 * DIM), BF16),
            pltpu.VMEM((LAYERS, 4 * DIM, DIM), BF16),
            pltpu.VMEM((SP - 1, CLIPS, TOK), jnp.int32),
            pltpu.VMEM((WIN, DIM), BF16),
            pltpu.VMEM((SP, WIN, DIM), BF16),
            pltpu.VMEM((ROWS, DIM), BF16),
            pltpu.VMEM((MINE, DIM), BF16),
            pltpu.VMEM((LAYERS, ROWS, DIM), BF16),
            pltpu.VMEM((Q_PAD, DIM), BF16),
            pltpu.VMEM((DIM, Q_PAD), BF16),
            pltpu.VMEM((ROWS, DIM), BF16),
            pltpu.VMEM((DIM, ROWS), BF16),
            pltpu.VMEM((DIM, Q_PAD), BF16),
            pltpu.SemaphoreType.DMA((4,)),
            pltpu.SemaphoreType.DMA((LAYERS * 4,)),
            pltpu.SemaphoreType.DMA((SP - 1,)),
            pltpu.SemaphoreType.DMA((SP - 1,)),
            pltpu.SemaphoreType.DMA((3,)),
            pltpu.SemaphoreType.DMA((3,)),
            pltpu.SemaphoreType.DMA((3,)),
            pltpu.SemaphoreType.DMA((3,)),
            pltpu.SemaphoreType.DMA((LAYERS,)),
            pltpu.SemaphoreType.DMA((LAYERS,)),
        ],
        compiler_params=pltpu.CompilerParams(collective_id=0, has_side_effects=True, vmem_limit_bytes=58 * 2 ** 20),
        cost_estimate=pl.CostEstimate(flops=12 * 10 ** 9, bytes_accessed=4 * 10 ** 7, transcendentals=0),
        name='encoder',
    )(mask, bpe, token, patches, enc_pos, wpe, dec_pos, wed, qkv_t, proj, up, down)


Q_BLK = 256
K_BLK = 256
CHUNK = 256
WIDE = 512
PAIR = 2 * HEAD


def fill_rows(start, count, step, body):
    def run(i, carry):
        body(pl.ds(pl.multiple_of(start + i * step, step), step))
        return carry

    lax.fori_loop(0, count // step, run, 0)


def make_queries(rows, norm, w_q, q_z):
    q = dot_nt(w_q, norm[rows, :]).astype(BF16)
    zero = jnp.zeros((HEAD, q.shape[1]), BF16)
    for head in range(DEC_HEADS):
        q_head = q[head * HEAD:(head + 1) * HEAD]
        low, high = (q_head, zero) if head % 2 == 0 else (zero, q_head)
        q_z[head, 0:HEAD, rows] = low
        q_z[head, HEAD:PAIR, rows] = high


def make_keys(rows, norm, w_k, w_v, k_n, v_t):
    a = norm[rows, :]
    k = dot_nt(a, w_k).astype(BF16)
    for pair in range(DEC_HEADS // 2):
        k_n[pair, rows, :] = k[:, pair * PAIR:(pair + 1) * PAIR]
    v_t[:, rows] = dot_nt(w_v, a).astype(BF16)


def attention(start, count, q_z, k_n, v_t, o_t, s_even, s_odd):
    blocks = count // Q_BLK
    units = DEC_HEADS * blocks

    def place(unit):
        head = unit // blocks
        return head, pl.ds(pl.multiple_of(start + (unit - head * blocks) * Q_BLK, Q_BLK), Q_BLK)

    def mixed(unit_q, s_q, unit_p, s_p, max8):
        if unit_q is not None:
            head_q, cols_q = place(unit_q)
            q = q_z[head_q, :, cols_q]
        if unit_p is not None:
            head_p, cols_p = place(unit_p)
            shift = col_max(max8) * EXP_SCALE
            v_rows = pl.ds(pl.multiple_of(head_p * HEAD, HEAD), HEAD)
        new_max = total = acc = None
        for idx in range(SEQ // K_BLK):
            rows = slice(idx * K_BLK, (idx + 1) * K_BLK)
            if unit_p is not None:
                e = jnp.exp2(s_p[rows, :] * EXP_SCALE - shift)
                t = jnp.sum(e.reshape(K_BLK // 8, 8, Q_BLK), axis=0)
                total = t if total is None else total + t
                o = dot(v_t[v_rows, rows], e.astype(BF16))
                acc = o if acc is None else acc + o
            if unit_q is not None:
                s = dot(k_n[head_q // 2, rows, :], q)
                s_q[rows, :] = s
                m = jnp.max(s.reshape(K_BLK // 8, 8, Q_BLK), axis=0)
                new_max = m if new_max is None else jnp.maximum(new_max, m)
        if unit_p is not None:
            o_t[v_rows, cols_p] = (acc * (1.0 / col_sum(total))).astype(BF16)
        return new_max

    first = mixed(0, s_even, None, None, None)

    def body(i, max8):
        unit = 2 * i
        max_odd = mixed(unit + 1, s_odd, unit, s_even, max8)
        return mixed(jnp.minimum(unit + 2, units - 1), s_even, unit + 1, s_odd, max_odd)

    lax.fori_loop(0, units // 2, body, first)


def mlp(rows, hid, o_t, w_proj, w_up, w_down):
    mid = (hid[rows, :].astype(F32) + dot_tn(o_t[:, rows], w_proj)).astype(BF16)
    act = gelu(dot(layer_norm(mid), w_up))
    return (mid.astype(F32) + dot(act, w_down)).astype(BF16)


def decoder_kernel(z_ref, rank_ref, pos_me, pos_x, qkv_hbm, proj_hbm, up_hbm, down_hbm, both_ref,
                   qkv, proj, up, down, hid, norm, fin, q_z, k_n, v_t, o_t, s_even, s_odd, w_sem, ready, row_send, row_recv, fin_send, fin_recv, pos, pos_sem):
    me = lax.axis_index('sp')
    chip = me // 2
    core = me - 2 * chip
    peer = lax.rem(me + 2, SP)
    sib = me + 1 - 2 * core
    diag = lax.rem(sib + 2, SP)

    fetch = [pltpu.make_async_copy(src, pos.at[idx], pos_sem.at[idx])
             for idx, src in enumerate((pos_me, pos_x.at[0], pos_x.at[1], pos_x.at[2]))]
    for copy in fetch:
        copy.start()
    copies = []
    for layer in range(LAYERS):
        for idx, (src, dst) in enumerate(((qkv_hbm, qkv), (proj_hbm, proj), (up_hbm, up), (down_hbm, down))):
            copy = pltpu.make_async_copy(src.at[layer], dst.at[layer], w_sem.at[layer * 4 + idx])
            copy.start()
            copies.append(copy)
    barrier = pltpu.get_barrier_semaphore()
    for other in (peer, sib):
        pl.semaphore_signal(barrier, inc=1, device_id={'sp': other}, device_id_type=MESH)
    pl.semaphore_wait(barrier, 2)

    def tokens(dev, idx):
        slot = lax.rem(me - dev + SP, SP)
        rank = rank_ref[pl.ds(2 * slot + chip, 1), :]
        rank_col = jnp.transpose(jnp.broadcast_to(rank.astype(F32), (8, TOK)))[:, 0:1]
        lanes = lax.broadcasted_iota(jnp.int32, (TOK, ROWS + 2 * HEAD), 1).astype(F32)
        select = jnp.where(lanes == rank_col, 1.0, 0.0).astype(BF16)
        fetch[idx].wait()
        return (dot(select, z_ref[...]) + pos[idx].astype(F32)).astype(BF16)

    hid[0:TOK] = tokens(peer, 1)
    hid[TOK:OWN] = tokens(me, 0)
    norm[OWN:OWN + TOK] = layer_norm(tokens(diag, 3))
    norm[OWN + TOK:SEQ] = layer_norm(tokens(sib, 2))

    def own_norm(rows):
        norm[rows, :] = layer_norm(hid[rows, :])

    fill_rows(0, OWN, CHUNK, own_norm)

    def queries(layer):
        fill_rows(0, OWN, WIDE, lambda rows: make_queries(rows, norm, qkv[layer, 0:DDIM], q_z))

    def keys(layer, start, count):
        fill_rows(start, count, WIDE, lambda rows: make_keys(
            rows, norm, qkv[layer, DDIM:2 * DDIM], qkv[layer, 2 * DDIM:3 * DDIM], k_n, v_t))

    copies[0].wait()
    queries(0)
    keys(0, 0, SEQ)
    pl.semaphore_signal(ready, inc=1, device_id={'sp': sib}, device_id_type=MESH)
    attention(0, OWN, q_z, k_n, v_t, o_t, s_even, s_odd)
    pl.semaphore_wait(ready, 1)
    for copy in copies[1:]:
        copy.wait()
    steps = OWN // CHUNK

    def row_copy(i):
        src = pl.ds(pl.multiple_of(i * CHUNK, CHUNK), CHUNK)
        dst = pl.ds(pl.multiple_of(OWN + i * CHUNK, CHUNK), CHUNK)
        return pltpu.make_async_remote_copy(
            src_ref=norm.at[src], dst_ref=norm.at[dst], send_sem=row_send.at[i], recv_sem=row_recv.at[i],
            device_id={'sp': sib}, device_id_type=MESH)

    def first_mlp(i, carry):
        rows = pl.ds(pl.multiple_of(i * CHUNK, CHUNK), CHUNK)
        val = mlp(rows, hid, o_t, proj[0], up[0], down[0])
        hid[rows, :] = val
        norm[rows, :] = layer_norm(val)

        @pl.when(i > 0)
        def _():
            row_copy(i - 1).start()

        return carry

    lax.fori_loop(0, steps, first_mlp, 0)
    queries(1)
    row_copy(steps - 1).start()
    keys(1, 0, OWN)
    for i in range(steps):
        row_copy(i).wait()
    keys(1, OWN, OWN)

    attention(0, TOK, q_z, k_n, v_t, o_t, s_even, s_odd)
    pieces = TOK // CHUNK

    def fin_copy(i):
        rows = pl.ds(pl.multiple_of(i * CHUNK, CHUNK), CHUNK)
        return pltpu.make_async_remote_copy(
            src_ref=fin.at[rows], dst_ref=both_ref.at[chip, rows], send_sem=fin_send.at[i], recv_sem=fin_recv.at[i],
            device_id={'sp': peer}, device_id_type=MESH)

    def last_mlp(i, carry, start):
        src = pl.ds(pl.multiple_of(start + i * CHUNK, CHUNK), CHUNK)
        rows = pl.ds(pl.multiple_of(i * CHUNK, CHUNK), CHUNK)
        val = layer_norm(mlp(src, hid, o_t, proj[1], up[1], down[1]))
        if start == 0:
            fin[rows, :] = val

            @pl.when(i > 0)
            def _():
                fin_copy(i - 1).start()
        else:
            both_ref[chip, rows, :] = val
        return carry

    lax.fori_loop(0, pieces, functools.partial(last_mlp, start=0), 0)
    fin_copy(pieces - 1).start()
    attention(TOK, TOK, q_z, k_n, v_t, o_t, s_even, s_odd)
    lax.fori_loop(0, pieces, functools.partial(last_mlp, start=TOK), 0)
    for i in range(pieces):
        fin_copy(i).wait()


def decode(z, rank, pos, pos_x, wqkv, wproj, wup, wdown):
    return pl.pallas_call(
        decoder_kernel,
        out_shape=jax.ShapeDtypeStruct((CLIPS, TOK, DDIM), BF16),
        in_specs=[VMEM] * 2 + [ANY] * 6,
        out_specs=VMEM,
        scratch_shapes=[
            pltpu.VMEM((LAYERS, 3 * DDIM, DDIM), BF16),
            pltpu.VMEM((LAYERS, DDIM, DDIM), BF16),
            pltpu.VMEM((LAYERS, DDIM, 4 * DDIM), BF16),
            pltpu.VMEM((LAYERS, 4 * DDIM, DDIM), BF16),
            pltpu.VMEM((OWN, DDIM), BF16),
            pltpu.VMEM((SEQ, DDIM), BF16),
            pltpu.VMEM((TOK, DDIM), BF16),
            pltpu.VMEM((DEC_HEADS, PAIR, OWN), BF16),
            pltpu.VMEM((DEC_HEADS // 2, SEQ, PAIR), BF16),
            pltpu.VMEM((DDIM, SEQ), BF16),
            pltpu.VMEM((DDIM, OWN), BF16),
            pltpu.VMEM((SEQ, Q_BLK), F32),
            pltpu.VMEM((SEQ, Q_BLK), F32),
            pltpu.SemaphoreType.DMA((LAYERS * 4,)),
            pltpu.SemaphoreType.REGULAR,
            pltpu.SemaphoreType.DMA((OWN // CHUNK,)),
            pltpu.SemaphoreType.DMA((OWN // CHUNK,)),
            pltpu.SemaphoreType.DMA((TOK // CHUNK,)),
            pltpu.SemaphoreType.DMA((TOK // CHUNK,)),
            pltpu.VMEM((SP, TOK, DDIM), BF16),
            pltpu.SemaphoreType.DMA((SP,)),
        ],
        compiler_params=pltpu.CompilerParams(collective_id=1, has_side_effects=True, vmem_limit_bytes=58 * 2 ** 20),
        cost_estimate=pl.CostEstimate(flops=60 * 10 ** 9, bytes_accessed=2 * 10 ** 7, transcendentals=6 * 10 ** 7),
        name='decoder',
    )(z, rank, pos, pos_x, wqkv, wproj, wup, wdown)


def output_kernel(both_ref, w_ref, out_hbm, buf, sem):
    pieces = TOK // CHUNK

    def out_copy(i):
        clip = i // pieces
        rows = pl.ds(pl.multiple_of((i - clip * pieces) * CHUNK, CHUNK), CHUNK)
        return pltpu.make_async_copy(buf.at[i], out_hbm.at[clip, rows], sem.at[i])

    def body(i, carry):
        clip = i // pieces
        rows = pl.ds(pl.multiple_of((i - clip * pieces) * CHUNK, CHUNK), CHUNK)
        buf[i] = dot(both_ref[clip, rows, :], w_ref[...])
        out_copy(i).start()
        return carry

    lax.fori_loop(0, CLIPS * pieces, body, 0)
    for i in range(CLIPS * pieces):
        out_copy(i).wait()


def project(both, w_out):
    return pl.pallas_call(
        output_kernel,
        out_shape=jax.ShapeDtypeStruct((CLIPS, TOK, PATCH), F32),
        in_specs=[VMEM] * 2,
        out_specs=ANY,
        scratch_shapes=[
            pltpu.VMEM((CLIPS * TOK // CHUNK, CHUNK, PATCH), F32),
            pltpu.SemaphoreType.DMA((CLIPS * TOK // CHUNK,)),
        ],
        compiler_params=pltpu.CompilerParams(vmem_limit_bytes=62 * 2 ** 20),
        cost_estimate=pl.CostEstimate(flops=2 * 10 ** 9, bytes_accessed=12 * 10 ** 6, transcendentals=0),
        name='output',
    )(both, w_out)


def solution(mesh):
    def local_program(patches, vis_mask, enc_pos, dec_pos, w_pe, b_pe, enc_qkv, enc_proj, enc_up, enc_down, w_ed, mask_token, dec_qkv, dec_proj, dec_up, dec_down, w_out):
        enc_qkv_t = jnp.transpose(enc_qkv, (0, 2, 3, 4, 1)).reshape(LAYERS, 3 * DIM, DIM)
        dec_qkv_t = jnp.transpose(dec_qkv, (0, 2, 3, 4, 1)).reshape(LAYERS, 3 * DDIM, DDIM)
        enc_proj2 = enc_proj.reshape(LAYERS, DIM, DIM)
        dec_proj2 = dec_proj.reshape(LAYERS, DDIM, DDIM)
        z, rank, pos_x = encode(vis_mask, b_pe, mask_token, patches, enc_pos, w_pe, dec_pos, w_ed,
                                enc_qkv_t, enc_proj2, enc_up, enc_down)
        both = decode(z, rank, dec_pos, pos_x, dec_qkv_t, dec_proj2, dec_up, dec_down)
        return project(both, w_out)

    row_spec = P('dp', 'sp', None)
    pos_spec = P(('dp', 'sp'), None)
    arg_specs = (row_spec, P('dp', 'sp'), pos_spec, pos_spec) + (P(),) * 13
    return jax.shard_map(local_program, mesh=mesh, in_specs=arg_specs, out_specs=row_spec, check_vma=False)
```

```python
import functools
import math

import jax
import jax.numpy as jnp
from jax import lax
from jax.experimental import pallas as pl
from jax.experimental.pallas import tpu as pltpu
from jax.sharding import PartitionSpec as P

F32 = jnp.float32
BF16 = jnp.bfloat16
MESH = pl.DeviceIdType.MESH
VMEM = pl.BlockSpec(memory_space=pltpu.VMEM)
ANY = pl.BlockSpec(memory_space=pl.ANY)

SP = 4
CLIPS = 2
TOK = 768
PATCH = 1536
DIM = 768
ENC_HEADS = 12
HEAD = 64
DDIM = 384
DEC_HEADS = 6
VIS = 96
WIN = 2 * VIS
ROWS = SP * VIS
OWN = 2 * TOK
SEQ = SP * TOK
LAYERS = 2
EXP_SCALE = HEAD ** -0.5 * math.log2(math.e)


def dot(lhs, rhs):
    return jnp.dot(lhs, rhs, preferred_element_type=F32)


def dot_nt(lhs, rhs):
    return lax.dot_general(lhs, rhs, (((1,), (1,)), ((), ())), preferred_element_type=F32)


def dot_tn(lhs, rhs):
    return lax.dot_general(lhs, rhs, (((0,), (0,)), ((), ())), preferred_element_type=F32)


def layer_norm(hidden):
    hid = hidden.astype(F32)
    centred = hid - jnp.mean(hid, axis=-1, keepdims=True)
    var = jnp.mean(centred * centred, axis=-1, keepdims=True)
    return (centred * lax.rsqrt(var + 1e-6)).astype(BF16)


def gelu(val):
    return (0.5 * val * (1.0 + lax.erf(val * math.sqrt(0.5)))).astype(BF16)


def col_max(val):
    return jnp.max(val, axis=0, keepdims=True)


def col_sum(val):
    return jnp.sum(val, axis=0, keepdims=True)


MINE = ROWS // 2
Q_PAD = 256


def encoder_kernel(mask_ref, bpe_ref, token_ref, patch_hbm, pos_hbm, wpe_hbm, dec_pos_hbm, wed_ref, qkv_hbm, proj_hbm, up_hbm, down_hbm,
                   z_ref, rank_ref, pos_out,
                   patch, pos, wpe, qkv, proj, up, down, masks, sendbuf, win, hall, hid, norm, norm_q, q_t, k_n, v_t, o_t,
                   in_sem, w_sem, mask_send, mask_recv, win_send, win_recv, pos_send, pos_recv, row_send, row_recv):
    me = lax.axis_index('sp')
    chip = me // 2
    core = me - 2 * chip
    peer = lax.rem(me + 2, SP)
    sib = me + 1 - 2 * core
    diag = lax.rem(sib + 2, SP)

    near_load = pltpu.make_async_copy(patch_hbm.at[chip], patch.at[chip], in_sem.at[3])
    loads = [pltpu.make_async_copy(src, dst, in_sem.at[idx])
             for idx, (src, dst) in enumerate(((patch_hbm.at[1 - chip], patch.at[1 - chip]), (wpe_hbm, wpe), (pos_hbm, pos)))]
    for copy in loads:
        copy.start()
    barrier = pltpu.get_barrier_semaphore()
    for other in (peer, sib, diag):
        pl.semaphore_signal(barrier, inc=1, device_id={'sp': other}, device_id_type=MESH)
    order_row = lax.broadcasted_iota(jnp.int32, (TOK, TOK), 0)
    order_col = lax.broadcasted_iota(jnp.int32, (TOK, TOK), 1)
    before = jnp.where(order_row < order_col, 1.0, 0.0).astype(BF16)
    mine = mask_ref[...].astype(F32)
    mine_rank = dot(jnp.concatenate([mine] * SP, axis=0).astype(BF16), before)[0:CLIPS]
    slot_of = jnp.where(mine > 0.0, mine_rank, -1.0)
    pl.semaphore_wait(barrier, 3)

    def send(src, dst, send_sem, recv_sem, dev):
        copy = pltpu.make_async_remote_copy(
            src_ref=src, dst_ref=dst, send_sem=send_sem, recv_sem=recv_sem, device_id={'sp': dev}, device_id_type=MESH)
        copy.start()
        return copy

    mask_copies = [send(mask_ref, masks.at[step - 1], mask_send.at[step - 1], mask_recv.at[step - 1], lax.rem(me + step, SP))
                   for step in range(1, SP)]
    for copy in loads:
        copy.wait()
    near_load.start()
    copies = []
    for layer in range(LAYERS):
        for idx, (src, dst) in enumerate(((qkv_hbm, qkv), (proj_hbm, proj), (up_hbm, up), (down_hbm, down))):
            copy = pltpu.make_async_copy(src.at[layer], dst.at[layer], w_sem.at[layer * 4 + idx])
            copy.start()
            copies.append(copy)

    bias = bpe_ref[...].astype(F32).reshape(1, DIM)

    def window(clip, slots):
        rows = lax.broadcasted_iota(jnp.int32, (WIN, TOK), 0).astype(F32)
        hit = jnp.where(rows == slots, 1.0, 0.0)
        select = hit.astype(BF16)
        moved = dot(select, patch[clip]).astype(BF16)
        occupied = jnp.sum(hit, axis=1, keepdims=True)
        emb = dot(moved, wpe[...]) + occupied * bias + dot(select, pos[...])
        return emb.astype(BF16)

    far = jnp.where(chip == 0, slot_of[1:2], slot_of[0:1])
    near = jnp.where(chip == 0, slot_of[0:1], slot_of[1:2])
    sendbuf[...] = window(1 - chip, far)
    to_peer = send(sendbuf, win.at[1], win_send.at[0], win_recv.at[0], peer)
    near_load.wait()
    win[0] = window(chip, near)
    to_sib = send(win.at[0], win.at[2], win_send.at[1], win_recv.at[1], sib)

    for copy in mask_copies:
        copy.wait()
    stacked = jnp.concatenate([mine] + [masks[k].astype(F32) for k in range(SP - 1)], axis=0)
    local = dot(stacked.astype(BF16), before)
    counts = jnp.sum(stacked, axis=1, keepdims=True)
    row_dev = lax.rem(me - lax.broadcasted_iota(jnp.int32, (CLIPS * SP, 1), 0) // CLIPS + SP, SP)
    base = jnp.zeros((CLIPS * SP, 1), F32)
    for k in range(SP):
        dev_k = lax.rem(me - k + SP, SP)
        tiled = jnp.concatenate([counts[CLIPS * k:CLIPS * k + CLIPS]] * SP, axis=0)
        base = base + jnp.where(dev_k < row_dev, tiled, 0.0)
    rank_ref[...] = jnp.where(stacked > 0.0, local + base, float(ROWS)).astype(jnp.int32)

    def placement(slot):
        def pick(val):
            two = val[CLIPS * slot:CLIPS * slot + CLIPS]
            return jnp.where(chip == 0, two[0:1], two[1:2])

        start, size = pick(base), pick(counts)
        rows = lax.broadcasted_iota(jnp.int32, (ROWS, WIN), 0).astype(F32)
        cols = lax.broadcasted_iota(jnp.int32, (ROWS, WIN), 1).astype(F32)
        return jnp.where((rows == cols + start) & (cols < size), 1.0, 0.0)

    even = core == 0
    left, right = placement(1), placement(3)
    place = [placement(0), placement(2), jnp.where(even, right, left), jnp.where(even, left, right)]
    to_peer.wait_recv()
    relay = send(win.at[1], win.at[3], win_send.at[2], win_recv.at[2], sib)
    pos_peer = send(dec_pos_hbm, pos_out.at[0], pos_send.at[0], pos_recv.at[0], peer)
    pos_sib = send(dec_pos_hbm, pos_out.at[1], pos_send.at[1], pos_recv.at[1], sib)
    total = dot(place[0].astype(BF16), win[0]) + dot(place[1].astype(BF16), win[1])
    to_sib.wait_recv()
    total = total + dot(place[2].astype(BF16), win[2])
    relay.wait_recv()
    total = total + dot(place[3].astype(BF16), win[3])
    hall[...] = total.astype(BF16)
    own = pl.ds(pl.multiple_of(core * MINE, MINE), MINE)
    hid[...] = hall[own, :]
    norm[0] = layer_norm(hall[...])
    norm_q[MINE:] = jnp.zeros((Q_PAD - MINE, DIM), BF16)
    zero = jnp.zeros((HEAD, Q_PAD), BF16)
    pos_diag = swap = None

    for layer in range(LAYERS):
        copies[layer * 4].wait()
        norm_q[0:MINE] = norm[layer, own, :]
        q_t[...] = dot_nt(qkv[layer, 0:DIM], norm_q[...]).astype(BF16)
        if swap is not None:
            swap.wait()
        k_n[...] = dot_nt(norm[layer], qkv[layer, DIM:2 * DIM]).astype(BF16)
        v_t[...] = dot_nt(qkv[layer, 2 * DIM:3 * DIM], norm[layer]).astype(BF16)

        def heads(group, carry):
            scores, weights = [], []
            for pair in range(2):
                lanes = pl.ds(pl.multiple_of((2 * group + pair) * 2 * HEAD, 2 * HEAD), 2 * HEAD)
                for odd in range(2):
                    rows = pl.ds(pl.multiple_of((4 * group + 2 * pair + odd) * HEAD, HEAD), HEAD)
                    q_head = q_t[rows, :]
                    q_both = jnp.concatenate([zero, q_head] if odd else [q_head, zero], axis=0)
                    scores.append(dot(k_n[:, lanes], q_both))
            for s in scores:
                e = jnp.exp2(s * EXP_SCALE - col_max(s) * EXP_SCALE)
                weights.append((e.astype(BF16), 1.0 / col_sum(e)))
            for idx, (e, scale) in enumerate(weights):
                rows = pl.ds(pl.multiple_of((4 * group + idx) * HEAD, HEAD), HEAD)
                o_t[rows, :] = (dot(v_t[rows, :], e) * scale).astype(BF16)
            return carry

        lax.fori_loop(0, ENC_HEADS // 4, heads, 0)
        copies[layer * 4 + 1].wait()
        mid = (hid[...].astype(F32) + dot_tn(o_t[...], proj[layer])[0:MINE]).astype(BF16)
        rows_norm = layer_norm(mid)
        copies[layer * 4 + 2].wait()
        copies[layer * 4 + 3].wait()
        if layer == LAYERS - 1:
            pos_peer.wait_recv()
            pos_diag = send(pos_out.at[0], pos_out.at[2], pos_send.at[2], pos_recv.at[2], sib)
        acc = None
        for lo in range(0, 4 * DIM, DIM):
            act = gelu(dot(rows_norm, up[layer, :, lo:lo + DIM]))
            part = dot(act, down[layer, lo:lo + DIM, :])
            acc = part if acc is None else acc + part
        out = (mid.astype(F32) + acc).astype(BF16)
        if layer < LAYERS - 1:
            hid[...] = out
            norm[layer + 1, own, :] = layer_norm(out)
            swap = send(norm.at[layer + 1, own], norm.at[layer + 1, own], row_send.at[layer], row_recv.at[layer], sib)
    z_ref[own, :] = dot(layer_norm(out), wed_ref[...]).astype(BF16)
    first = lax.broadcasted_iota(jnp.int32, (2 * HEAD, DDIM), 0) == 0
    z_ref[ROWS:] = jnp.where(first, token_ref[...].astype(F32).reshape(1, DDIM), 0.0).astype(BF16)
    last = send(z_ref.at[own], z_ref.at[own], row_send.at[LAYERS - 1], row_recv.at[LAYERS - 1], sib)
    to_peer.wait_send()
    to_sib.wait_send()
    relay.wait_send()
    pos_peer.wait_send()
    pos_sib.wait()
    pos_diag.wait()
    last.wait()


def encode(mask, bpe, token, patches, enc_pos, wpe, dec_pos, wed, qkv_t, proj, up, down):
    return pl.pallas_call(
        encoder_kernel,
        out_shape=(
            jax.ShapeDtypeStruct((ROWS + 2 * HEAD, DDIM), BF16),
            jax.ShapeDtypeStruct((CLIPS * SP, TOK), jnp.int32),
            jax.ShapeDtypeStruct((SP - 1, TOK, DDIM), BF16),
        ),
        in_specs=[VMEM] * 3 + [ANY] * 4 + [VMEM] + [ANY] * 4,
        out_specs=(VMEM, VMEM, ANY),
        scratch_shapes=[
            pltpu.VMEM((CLIPS, TOK, PATCH), BF16),
            pltpu.VMEM((TOK, DIM), BF16),
            pltpu.VMEM((PATCH, DIM), BF16),
            pltpu.VMEM((LAYERS, 3 * DIM, DIM), BF16),
            pltpu.VMEM((LAYERS, DIM, DIM), BF16),
            pltpu.VMEM((LAYERS, DIM, 4 * DIM), BF16),
            pltpu.VMEM((LAYERS, 4 * DIM, DIM), BF16),
            pltpu.VMEM((SP - 1, CLIPS, TOK), jnp.int32),
            pltpu.VMEM((WIN, DIM), BF16),
            pltpu.VMEM((SP, WIN, DIM), BF16),
            pltpu.VMEM((ROWS, DIM), BF16),
            pltpu.VMEM((MINE, DIM), BF16),
            pltpu.VMEM((LAYERS, ROWS, DIM), BF16),
            pltpu.VMEM((Q_PAD, DIM), BF16),
            pltpu.VMEM((DIM, Q_PAD), BF16),
            pltpu.VMEM((ROWS, DIM), BF16),
            pltpu.VMEM((DIM, ROWS), BF16),
            pltpu.VMEM((DIM, Q_PAD), BF16),
            pltpu.SemaphoreType.DMA((4,)),
            pltpu.SemaphoreType.DMA((LAYERS * 4,)),
            pltpu.SemaphoreType.DMA((SP - 1,)),
            pltpu.SemaphoreType.DMA((SP - 1,)),
            pltpu.SemaphoreType.DMA((3,)),
            pltpu.SemaphoreType.DMA((3,)),
            pltpu.SemaphoreType.DMA((3,)),
            pltpu.SemaphoreType.DMA((3,)),
            pltpu.SemaphoreType.DMA((LAYERS,)),
            pltpu.SemaphoreType.DMA((LAYERS,)),
        ],
        compiler_params=pltpu.CompilerParams(collective_id=0, has_side_effects=True, vmem_limit_bytes=58 * 2 ** 20),
        cost_estimate=pl.CostEstimate(flops=12 * 10 ** 9, bytes_accessed=4 * 10 ** 7, transcendentals=0),
        name='encoder',
    )(mask, bpe, token, patches, enc_pos, wpe, dec_pos, wed, qkv_t, proj, up, down)


Q_BLK = 512
K_BLK = 256
CHUNK = 256
WIDE = 512
PAIR = 2 * HEAD


def fill_rows(start, count, step, body):
    def run(i, carry):
        body(pl.ds(pl.multiple_of(start + i * step, step), step))
        return carry

    lax.fori_loop(0, count // step, run, 0)


def make_queries(rows, norm, w_q, q_3):
    q = dot_nt(w_q, norm[rows, :]).astype(BF16).astype(F32) * EXP_SCALE
    hi = q.astype(BF16)
    rest = q - hi.astype(F32)
    mid = rest.astype(BF16)
    low = (rest - mid.astype(F32)).astype(BF16)
    zero = jnp.zeros((HEAD, q.shape[1]), BF16)
    for head in range(DEC_HEADS):
        part = slice(head * HEAD, (head + 1) * HEAD)
        tail = (low[part], zero) if head % 2 == 0 else (zero, low[part])
        for idx, val in enumerate((hi[part], mid[part]) + tail):
            q_3[head, idx * HEAD:(idx + 1) * HEAD, rows] = val


def make_keys(rows, norm, w_k, w_v, k_n, k_dup, v_t):
    a = norm[rows, :]
    k = dot_nt(a, w_k)
    first = lax.broadcasted_iota(jnp.int32, (k.shape[0], PAIR), 1) < HEAD
    for pair in range(DEC_HEADS // 2):
        both = k[:, pair * PAIR:(pair + 1) * PAIR]
        turned = pltpu.roll(both, HEAD, axis=1)
        k_n[pair, rows, :] = both.astype(BF16)
        k_dup[2 * pair, rows, :] = jnp.where(first, both, turned).astype(BF16)
        k_dup[2 * pair + 1, rows, :] = jnp.where(first, turned, both).astype(BF16)
    v_t[:, rows] = dot_nt(w_v, a).astype(BF16)


def attention(start, count, q_3, k_n, k_dup, v_t, o_t, s_even, s_odd):
    blocks = count // Q_BLK
    units = DEC_HEADS * blocks

    def place(unit):
        head = unit // blocks
        return head, pl.ds(pl.multiple_of(start + (unit - head * blocks) * Q_BLK, Q_BLK), Q_BLK)

    def mixed(unit_q, s_q, unit_p, s_p, max8):
        if unit_q is not None:
            head_q, cols_q = place(unit_q)
            q = q_3[head_q, :, cols_q]
        if unit_p is not None:
            head_p, cols_p = place(unit_p)
            shift = col_max(max8)
            v_rows = pl.ds(pl.multiple_of(head_p * HEAD, HEAD), HEAD)
        new_max = total = late = None
        accs = [None, None]

        def weigh(idx, weights):
            o = dot(v_t[v_rows, idx * K_BLK:(idx + 1) * K_BLK], weights)
            accs[idx % 2] = o if accs[idx % 2] is None else accs[idx % 2] + o

        for idx in range(SEQ // K_BLK):
            rows = slice(idx * K_BLK, (idx + 1) * K_BLK)
            if unit_p is not None:
                e = jnp.exp2(s_p[rows, :] - shift)
                t = jnp.sum(e.reshape(K_BLK // 8, 8, Q_BLK), axis=0)
                total = t if total is None else total + t
                if late is not None:
                    weigh(*late)
                late = (idx, e.astype(BF16))
            if unit_q is not None:
                keys = jnp.concatenate([k_dup[head_q, rows, :], k_n[head_q // 2, rows, :]], axis=1)
                s = dot(keys, q)
                s_q[rows, :] = s
                m = jnp.max(s.reshape(K_BLK // 8, 8, Q_BLK), axis=0)
                new_max = m if new_max is None else jnp.maximum(new_max, m)
        if unit_p is not None:
            weigh(*late)
            o_t[v_rows, cols_p] = ((accs[0] + accs[1]) * (1.0 / col_sum(total))).astype(BF16)
        return new_max

    first = mixed(0, s_even, None, None, None)

    def body(i, max8):
        unit = 2 * i
        max_odd = mixed(unit + 1, s_odd, unit, s_even, max8)
        return mixed(jnp.minimum(unit + 2, units - 1), s_even, unit + 1, s_odd, max_odd)

    lax.fori_loop(0, units // 2, body, first)


def mlp(rows, hid, o_t, w_proj, w_up, w_down):
    mid = (hid[rows, :].astype(F32) + dot_tn(o_t[:, rows], w_proj)).astype(BF16)
    act = gelu(dot(layer_norm(mid), w_up))
    return (mid.astype(F32) + dot(act, w_down)).astype(BF16)


def decoder_kernel(z_ref, rank_ref, pos_me, pos_x, qkv_hbm, proj_hbm, up_hbm, down_hbm, both_ref,
                   qkv, proj, up, down, hid, norm, fin, q_3, k_n, k_dup, v_t, o_t, s_even, s_odd, w_sem, ready, row_send, row_recv, fin_send, fin_recv, pos, pos_sem):
    me = lax.axis_index('sp')
    chip = me // 2
    core = me - 2 * chip
    peer = lax.rem(me + 2, SP)
    sib = me + 1 - 2 * core
    diag = lax.rem(sib + 2, SP)

    fetch = [pltpu.make_async_copy(src, pos.at[idx], pos_sem.at[idx])
             for idx, src in enumerate((pos_me, pos_x.at[0], pos_x.at[1], pos_x.at[2]))]
    for copy in fetch:
        copy.start()
    copies = []
    for layer in range(LAYERS):
        for idx, (src, dst) in enumerate(((qkv_hbm, qkv), (proj_hbm, proj), (up_hbm, up), (down_hbm, down))):
            copy = pltpu.make_async_copy(src.at[layer], dst.at[layer], w_sem.at[layer * 4 + idx])
            copy.start()
            copies.append(copy)
    barrier = pltpu.get_barrier_semaphore()
    for other in (peer, sib):
        pl.semaphore_signal(barrier, inc=1, device_id={'sp': other}, device_id_type=MESH)
    pl.semaphore_wait(barrier, 2)

    def tokens(dev, idx):
        slot = lax.rem(me - dev + SP, SP)
        rank = rank_ref[pl.ds(2 * slot + chip, 1), :]
        rank_col = jnp.transpose(jnp.broadcast_to(rank.astype(F32), (8, TOK)))[:, 0:1]
        lanes = lax.broadcasted_iota(jnp.int32, (TOK, ROWS + 2 * HEAD), 1).astype(F32)
        select = jnp.where(lanes == rank_col, 1.0, 0.0).astype(BF16)
        fetch[idx].wait()
        return (dot(select, z_ref[...]) + pos[idx].astype(F32)).astype(BF16)

    hid[0:TOK] = tokens(peer, 1)
    hid[TOK:OWN] = tokens(me, 0)
    norm[OWN:OWN + TOK] = layer_norm(tokens(diag, 3))
    norm[OWN + TOK:SEQ] = layer_norm(tokens(sib, 2))

    def own_norm(rows):
        norm[rows, :] = layer_norm(hid[rows, :])

    fill_rows(0, OWN, CHUNK, own_norm)

    def queries(layer):
        fill_rows(0, OWN, WIDE, lambda rows: make_queries(rows, norm, qkv[layer, 0:DDIM], q_3))

    def keys(layer, start, count):
        fill_rows(start, count, WIDE, lambda rows: make_keys(
            rows, norm, qkv[layer, DDIM:2 * DDIM], qkv[layer, 2 * DDIM:3 * DDIM], k_n, k_dup, v_t))

    copies[0].wait()
    queries(0)
    keys(0, 0, SEQ)
    pl.semaphore_signal(ready, inc=1, device_id={'sp': sib}, device_id_type=MESH)
    attention(0, OWN, q_3, k_n, k_dup, v_t, o_t, s_even, s_odd)
    pl.semaphore_wait(ready, 1)
    for copy in copies[1:]:
        copy.wait()
    steps = OWN // CHUNK

    def row_copy(i):
        src = pl.ds(pl.multiple_of(i * CHUNK, CHUNK), CHUNK)
        dst = pl.ds(pl.multiple_of(OWN + i * CHUNK, CHUNK), CHUNK)
        return pltpu.make_async_remote_copy(
            src_ref=norm.at[src], dst_ref=norm.at[dst], send_sem=row_send.at[i], recv_sem=row_recv.at[i],
            device_id={'sp': sib}, device_id_type=MESH)

    def first_mlp(i, carry):
        rows = pl.ds(pl.multiple_of(i * CHUNK, CHUNK), CHUNK)
        val = mlp(rows, hid, o_t, proj[0], up[0], down[0])
        hid[rows, :] = val
        norm[rows, :] = layer_norm(val)

        @pl.when(i > 0)
        def _():
            row_copy(i - 1).start()

        return carry

    lax.fori_loop(0, steps, first_mlp, 0)
    queries(1)
    row_copy(steps - 1).start()
    keys(1, 0, OWN)
    for i in range(steps):
        row_copy(i).wait()
    keys(1, OWN, OWN)

    early = 2 * Q_BLK
    attention(0, early, q_3, k_n, k_dup, v_t, o_t, s_even, s_odd)
    pieces = TOK // CHUNK

    def fin_copy(i):
        rows = pl.ds(pl.multiple_of(i * CHUNK, CHUNK), CHUNK)
        return pltpu.make_async_remote_copy(
            src_ref=fin.at[rows], dst_ref=both_ref.at[chip, rows], send_sem=fin_send.at[i], recv_sem=fin_recv.at[i],
            device_id={'sp': peer}, device_id_type=MESH)

    def last_mlp(i, carry, start):
        src = pl.ds(pl.multiple_of(start + i * CHUNK, CHUNK), CHUNK)
        rows = pl.ds(pl.multiple_of(i * CHUNK, CHUNK), CHUNK)
        val = layer_norm(mlp(src, hid, o_t, proj[1], up[1], down[1]))
        if start == 0:
            fin[rows, :] = val

            @pl.when(i > 0)
            def _():
                fin_copy(i - 1).start()
        else:
            both_ref[chip, rows, :] = val
        return carry

    lax.fori_loop(0, pieces, functools.partial(last_mlp, start=0), 0)
    fin_copy(pieces - 1).start()
    attention(early, OWN - early, q_3, k_n, k_dup, v_t, o_t, s_even, s_odd)
    lax.fori_loop(0, pieces, functools.partial(last_mlp, start=TOK), 0)
    for i in range(pieces):
        fin_copy(i).wait()


def decode(z, rank, pos, pos_x, wqkv, wproj, wup, wdown):
    return pl.pallas_call(
        decoder_kernel,
        out_shape=jax.ShapeDtypeStruct((CLIPS, TOK, DDIM), BF16),
        in_specs=[VMEM] * 2 + [ANY] * 6,
        out_specs=VMEM,
        scratch_shapes=[
            pltpu.VMEM((LAYERS, 3 * DDIM, DDIM), BF16),
            pltpu.VMEM((LAYERS, DDIM, DDIM), BF16),
            pltpu.VMEM((LAYERS, DDIM, 4 * DDIM), BF16),
            pltpu.VMEM((LAYERS, 4 * DDIM, DDIM), BF16),
            pltpu.VMEM((OWN, DDIM), BF16),
            pltpu.VMEM((SEQ, DDIM), BF16),
            pltpu.VMEM((TOK, DDIM), BF16),
            pltpu.VMEM((DEC_HEADS, 4 * HEAD, OWN), BF16),
            pltpu.VMEM((DEC_HEADS // 2, SEQ, PAIR), BF16),
            pltpu.VMEM((DEC_HEADS, SEQ, PAIR), BF16),
            pltpu.VMEM((DDIM, SEQ), BF16),
            pltpu.VMEM((DDIM, OWN), BF16),
            pltpu.VMEM((SEQ, Q_BLK), F32),
            pltpu.VMEM((SEQ, Q_BLK), F32),
            pltpu.SemaphoreType.DMA((LAYERS * 4,)),
            pltpu.SemaphoreType.REGULAR,
            pltpu.SemaphoreType.DMA((OWN // CHUNK,)),
            pltpu.SemaphoreType.DMA((OWN // CHUNK,)),
            pltpu.SemaphoreType.DMA((TOK // CHUNK,)),
            pltpu.SemaphoreType.DMA((TOK // CHUNK,)),
            pltpu.VMEM((SP, TOK, DDIM), BF16),
            pltpu.SemaphoreType.DMA((SP,)),
        ],
        compiler_params=pltpu.CompilerParams(collective_id=1, has_side_effects=True, vmem_limit_bytes=58 * 2 ** 20),
        cost_estimate=pl.CostEstimate(flops=60 * 10 ** 9, bytes_accessed=2 * 10 ** 7, transcendentals=6 * 10 ** 7),
        name='decoder',
    )(z, rank, pos, pos_x, wqkv, wproj, wup, wdown)


def output_kernel(both_ref, w_ref, out_hbm, buf, sem):
    pieces = TOK // CHUNK

    def out_copy(i):
        clip = i // pieces
        rows = pl.ds(pl.multiple_of((i - clip * pieces) * CHUNK, CHUNK), CHUNK)
        return pltpu.make_async_copy(buf.at[i], out_hbm.at[clip, rows], sem.at[i])

    def body(i, carry):
        clip = i // pieces
        rows = pl.ds(pl.multiple_of((i - clip * pieces) * CHUNK, CHUNK), CHUNK)
        buf[i] = dot(both_ref[clip, rows, :], w_ref[...])
        out_copy(i).start()
        return carry

    lax.fori_loop(0, CLIPS * pieces, body, 0)
    for i in range(CLIPS * pieces):
        out_copy(i).wait()


def project(both, w_out):
    return pl.pallas_call(
        output_kernel,
        out_shape=jax.ShapeDtypeStruct((CLIPS, TOK, PATCH), F32),
        in_specs=[VMEM] * 2,
        out_specs=ANY,
        scratch_shapes=[
            pltpu.VMEM((CLIPS * TOK // CHUNK, CHUNK, PATCH), F32),
            pltpu.SemaphoreType.DMA((CLIPS * TOK // CHUNK,)),
        ],
        compiler_params=pltpu.CompilerParams(vmem_limit_bytes=62 * 2 ** 20),
        cost_estimate=pl.CostEstimate(flops=2 * 10 ** 9, bytes_accessed=12 * 10 ** 6, transcendentals=0),
        name='output',
    )(both, w_out)


def solution(mesh):
    def local_program(patches, vis_mask, enc_pos, dec_pos, w_pe, b_pe, enc_qkv, enc_proj, enc_up, enc_down, w_ed, mask_token, dec_qkv, dec_proj, dec_up, dec_down, w_out):
        enc_qkv_t = jnp.transpose(enc_qkv, (0, 2, 3, 4, 1)).reshape(LAYERS, 3 * DIM, DIM)
        dec_qkv_t = jnp.transpose(dec_qkv, (0, 2, 3, 4, 1)).reshape(LAYERS, 3 * DDIM, DDIM)
        enc_proj2 = enc_proj.reshape(LAYERS, DIM, DIM)
        dec_proj2 = dec_proj.reshape(LAYERS, DDIM, DDIM)
        z, rank, pos_x = encode(vis_mask, b_pe, mask_token, patches, enc_pos, w_pe, dec_pos, w_ed,
                                enc_qkv_t, enc_proj2, enc_up, enc_down)
        both = decode(z, rank, dec_pos, pos_x, dec_qkv_t, dec_proj2, dec_up, dec_down)
        return project(both, w_out)

    row_spec = P('dp', 'sp', None)
    pos_spec = P(('dp', 'sp'), None)
    arg_specs = (row_spec, P('dp', 'sp'), pos_spec, pos_spec) + (P(),) * 13
    return jax.shard_map(local_program, mesh=mesh, in_specs=arg_specs, out_specs=row_spec, check_vma=False)
```

```python
import functools
import math

import jax
import jax.numpy as jnp
from jax import lax
from jax.experimental import pallas as pl
from jax.experimental.pallas import tpu as pltpu
from jax.sharding import PartitionSpec as P

F32 = jnp.float32
BF16 = jnp.bfloat16
MESH = pl.DeviceIdType.MESH
VMEM = pl.BlockSpec(memory_space=pltpu.VMEM)
ANY = pl.BlockSpec(memory_space=pl.ANY)

SP = 4
CLIPS = 2
TOK = 768
PATCH = 1536
DIM = 768
ENC_HEADS = 12
HEAD = 64
DDIM = 384
DEC_HEADS = 6
VIS = 96
WIN = 2 * VIS
ROWS = SP * VIS
OWN = 2 * TOK
SEQ = SP * TOK
LAYERS = 2
EXP_SCALE = HEAD ** -0.5 * math.log2(math.e)


def dot(lhs, rhs):
    return jnp.dot(lhs, rhs, preferred_element_type=F32)


def dot_nt(lhs, rhs):
    return lax.dot_general(lhs, rhs, (((1,), (1,)), ((), ())), preferred_element_type=F32)


def dot_tn(lhs, rhs):
    return lax.dot_general(lhs, rhs, (((0,), (0,)), ((), ())), preferred_element_type=F32)


def layer_norm(hidden):
    hid = hidden.astype(F32)
    centred = hid - jnp.mean(hid, axis=-1, keepdims=True)
    var = jnp.mean(centred * centred, axis=-1, keepdims=True)
    return (centred * lax.rsqrt(var + 1e-6)).astype(BF16)


def gelu(val):
    return (0.5 * val * (1.0 + lax.erf(val * math.sqrt(0.5)))).astype(BF16)


def col_max(val):
    return jnp.max(val, axis=0, keepdims=True)


def col_sum(val):
    return jnp.sum(val, axis=0, keepdims=True)


MINE = ROWS // 2
Q_PAD = 256


def encoder_kernel(mask_ref, bpe_ref, token_ref, patch_hbm, pos_hbm, wpe_hbm, dec_pos_hbm, wed_ref, qkv_hbm, proj_hbm, up_hbm, down_hbm,
                   z_ref, rank_ref, pos_out,
                   patch, pos, wpe, qkv, proj, up, down, masks, sendbuf, win, hall, hid, norm, norm_q, q_t, k_n, v_t, o_t,
                   in_sem, w_sem, mask_send, mask_recv, win_send, win_recv, pos_send, pos_recv, row_send, row_recv):
    me = lax.axis_index('sp')
    chip = me // 2
    core = me - 2 * chip
    peer = lax.rem(me + 2, SP)
    sib = me + 1 - 2 * core
    diag = lax.rem(sib + 2, SP)

    near_load = pltpu.make_async_copy(patch_hbm.at[chip], patch.at[chip], in_sem.at[3])
    loads = [pltpu.make_async_copy(src, dst, in_sem.at[idx])
             for idx, (src, dst) in enumerate(((patch_hbm.at[1 - chip], patch.at[1 - chip]), (wpe_hbm, wpe), (pos_hbm, pos)))]
    for copy in loads:
        copy.start()
    barrier = pltpu.get_barrier_semaphore()
    for other in (peer, sib, diag):
        pl.semaphore_signal(barrier, inc=1, device_id={'sp': other}, device_id_type=MESH)
    order_row = lax.broadcasted_iota(jnp.int32, (TOK, TOK), 0)
    order_col = lax.broadcasted_iota(jnp.int32, (TOK, TOK), 1)
    before = jnp.where(order_row < order_col, 1.0, 0.0).astype(BF16)
    mine = mask_ref[...].astype(F32)
    mine_rank = dot(jnp.concatenate([mine] * SP, axis=0).astype(BF16), before)[0:CLIPS]
    slot_of = jnp.where(mine > 0.0, mine_rank, -1.0)
    pl.semaphore_wait(barrier, 3)

    def send(src, dst, send_sem, recv_sem, dev):
        copy = pltpu.make_async_remote_copy(
            src_ref=src, dst_ref=dst, send_sem=send_sem, recv_sem=recv_sem, device_id={'sp': dev}, device_id_type=MESH)
        copy.start()
        return copy

    mask_copies = [send(mask_ref, masks.at[step - 1], mask_send.at[step - 1], mask_recv.at[step - 1], lax.rem(me + step, SP))
                   for step in range(1, SP)]
    for copy in loads:
        copy.wait()
    near_load.start()
    copies = []
    for layer in range(LAYERS):
        for idx, (src, dst) in enumerate(((qkv_hbm, qkv), (proj_hbm, proj), (up_hbm, up), (down_hbm, down))):
            copy = pltpu.make_async_copy(src.at[layer], dst.at[layer], w_sem.at[layer * 4 + idx])
            copy.start()
            copies.append(copy)

    bias = bpe_ref[...].astype(F32).reshape(1, DIM)

    def window(clip, slots, low, count):
        rows = (lax.broadcasted_iota(jnp.int32, (count, TOK), 0) + low).astype(F32)
        hit = jnp.where(rows == slots, 1.0, 0.0)
        select = hit.astype(BF16)
        moved = dot(select, patch[clip]).astype(BF16)
        occupied = jnp.sum(hit, axis=1, keepdims=True)
        emb = dot(moved, wpe[...]) + occupied * bias + dot(select, pos[...])
        return emb.astype(BF16)

    far = jnp.where(chip == 0, slot_of[1:2], slot_of[0:1])
    near = jnp.where(chip == 0, slot_of[0:1], slot_of[1:2])
    halves = [pl.ds(0, VIS), pl.ds(VIS, VIS)]
    to_peer = []
    for idx, part in enumerate(halves):
        sendbuf[idx * VIS:(idx + 1) * VIS] = window(1 - chip, far, idx * VIS, VIS)
        to_peer.append(send(sendbuf.at[part], win.at[1, part], win_send.at[idx], win_recv.at[idx], peer))
    near_load.wait()
    win[0] = window(chip, near, 0, WIN)
    to_sib = send(win.at[0], win.at[2], win_send.at[2], win_recv.at[2], sib)

    for copy in mask_copies:
        copy.wait()
    stacked = jnp.concatenate([mine] + [masks[k].astype(F32) for k in range(SP - 1)], axis=0)
    local = dot(stacked.astype(BF16), before)
    counts = jnp.sum(stacked, axis=1, keepdims=True)
    row_dev = lax.rem(me - lax.broadcasted_iota(jnp.int32, (CLIPS * SP, 1), 0) // CLIPS + SP, SP)
    base = jnp.zeros((CLIPS * SP, 1), F32)
    for k in range(SP):
        dev_k = lax.rem(me - k + SP, SP)
        tiled = jnp.concatenate([counts[CLIPS * k:CLIPS * k + CLIPS]] * SP, axis=0)
        base = base + jnp.where(dev_k < row_dev, tiled, 0.0)
    rank_ref[...] = jnp.where(stacked > 0.0, local + base, float(ROWS)).astype(jnp.int32)

    def placement(slot):
        def pick(val):
            two = val[CLIPS * slot:CLIPS * slot + CLIPS]
            return jnp.where(chip == 0, two[0:1], two[1:2])

        start, size = pick(base), pick(counts)
        rows = lax.broadcasted_iota(jnp.int32, (ROWS, WIN), 0).astype(F32)
        cols = lax.broadcasted_iota(jnp.int32, (ROWS, WIN), 1).astype(F32)
        return jnp.where((rows == cols + start) & (cols < size), 1.0, 0.0)

    even = core == 0
    left, right = placement(1), placement(3)
    place = [placement(0), placement(2), jnp.where(even, right, left), jnp.where(even, left, right)]
    relay = []
    for idx, part in enumerate(halves):
        to_peer[idx].wait_recv()
        relay.append(send(win.at[1, part], win.at[3, part], win_send.at[3 + idx], win_recv.at[3 + idx], sib))
    pos_peer = send(dec_pos_hbm, pos_out.at[0], pos_send.at[0], pos_recv.at[0], peer)
    pos_sib = send(dec_pos_hbm, pos_out.at[1], pos_send.at[1], pos_recv.at[1], sib)
    total = dot(place[0].astype(BF16), win[0]) + dot(place[1].astype(BF16), win[1])
    to_sib.wait_recv()
    total = total + dot(place[2].astype(BF16), win[2])
    for copy in relay:
        copy.wait_recv()
    total = total + dot(place[3].astype(BF16), win[3])
    hall[...] = total.astype(BF16)
    own = pl.ds(pl.multiple_of(core * MINE, MINE), MINE)
    hid[...] = hall[own, :]
    norm[0] = layer_norm(hall[...])
    norm_q[MINE:] = jnp.zeros((Q_PAD - MINE, DIM), BF16)
    zero = jnp.zeros((HEAD, Q_PAD), BF16)
    pos_diag = swap = None

    for layer in range(LAYERS):
        copies[layer * 4].wait()
        norm_q[0:MINE] = norm[layer, own, :]
        q_t[...] = dot_nt(qkv[layer, 0:DIM], norm_q[...]).astype(BF16)
        if swap is not None:
            swap.wait()
        k_n[...] = dot_nt(norm[layer], qkv[layer, DIM:2 * DIM]).astype(BF16)
        v_t[...] = dot_nt(qkv[layer, 2 * DIM:3 * DIM], norm[layer]).astype(BF16)

        def heads(group, carry):
            scores, weights = [], []
            for pair in range(2):
                lanes = pl.ds(pl.multiple_of((2 * group + pair) * 2 * HEAD, 2 * HEAD), 2 * HEAD)
                for odd in range(2):
                    rows = pl.ds(pl.multiple_of((4 * group + 2 * pair + odd) * HEAD, HEAD), HEAD)
                    q_head = q_t[rows, :]
                    q_both = jnp.concatenate([zero, q_head] if odd else [q_head, zero], axis=0)
                    scores.append(dot(k_n[:, lanes], q_both))
            for s in scores:
                e = jnp.exp2(s * EXP_SCALE - col_max(s) * EXP_SCALE)
                weights.append((e.astype(BF16), 1.0 / col_sum(e)))
            for idx, (e, scale) in enumerate(weights):
                rows = pl.ds(pl.multiple_of((4 * group + idx) * HEAD, HEAD), HEAD)
                o_t[rows, :] = (dot(v_t[rows, :], e) * scale).astype(BF16)
            return carry

        lax.fori_loop(0, ENC_HEADS // 4, heads, 0)
        copies[layer * 4 + 1].wait()
        mid = (hid[...].astype(F32) + dot_tn(o_t[...], proj[layer])[0:MINE]).astype(BF16)
        rows_norm = layer_norm(mid)
        copies[layer * 4 + 2].wait()
        copies[layer * 4 + 3].wait()
        if layer == LAYERS - 1:
            pos_peer.wait_recv()
            pos_diag = send(pos_out.at[0], pos_out.at[2], pos_send.at[2], pos_recv.at[2], sib)
        acc = None
        for lo in range(0, 4 * DIM, DIM):
            act = gelu(dot(rows_norm, up[layer, :, lo:lo + DIM]))
            part = dot(act, down[layer, lo:lo + DIM, :])
            acc = part if acc is None else acc + part
        out = (mid.astype(F32) + acc).astype(BF16)
        if layer < LAYERS - 1:
            hid[...] = out
            norm[layer + 1, own, :] = layer_norm(out)
            swap = send(norm.at[layer + 1, own], norm.at[layer + 1, own], row_send.at[layer], row_recv.at[layer], sib)
    z_ref[own, :] = dot(layer_norm(out), wed_ref[...]).astype(BF16)
    first = lax.broadcasted_iota(jnp.int32, (2 * HEAD, DDIM), 0) == 0
    z_ref[ROWS:] = jnp.where(first, token_ref[...].astype(F32).reshape(1, DDIM), 0.0).astype(BF16)
    last = send(z_ref.at[own], z_ref.at[own], row_send.at[LAYERS - 1], row_recv.at[LAYERS - 1], sib)
    for copy in (*to_peer, to_sib, *relay):
        copy.wait_send()
    pos_peer.wait_send()
    pos_sib.wait()
    pos_diag.wait()
    last.wait()


def encode(mask, bpe, token, patches, enc_pos, wpe, dec_pos, wed, qkv_t, proj, up, down):
    return pl.pallas_call(
        encoder_kernel,
        out_shape=(
            jax.ShapeDtypeStruct((ROWS + 2 * HEAD, DDIM), BF16),
            jax.ShapeDtypeStruct((CLIPS * SP, TOK), jnp.int32),
            jax.ShapeDtypeStruct((SP - 1, TOK, DDIM), BF16),
        ),
        in_specs=[VMEM] * 3 + [ANY] * 4 + [VMEM] + [ANY] * 4,
        out_specs=(VMEM, VMEM, ANY),
        scratch_shapes=[
            pltpu.VMEM((CLIPS, TOK, PATCH), BF16),
            pltpu.VMEM((TOK, DIM), BF16),
            pltpu.VMEM((PATCH, DIM), BF16),
            pltpu.VMEM((LAYERS, 3 * DIM, DIM), BF16),
            pltpu.VMEM((LAYERS, DIM, DIM), BF16),
            pltpu.VMEM((LAYERS, DIM, 4 * DIM), BF16),
            pltpu.VMEM((LAYERS, 4 * DIM, DIM), BF16),
            pltpu.VMEM((SP - 1, CLIPS, TOK), jnp.int32),
            pltpu.VMEM((WIN, DIM), BF16),
            pltpu.VMEM((SP, WIN, DIM), BF16),
            pltpu.VMEM((ROWS, DIM), BF16),
            pltpu.VMEM((MINE, DIM), BF16),
            pltpu.VMEM((LAYERS, ROWS, DIM), BF16),
            pltpu.VMEM((Q_PAD, DIM), BF16),
            pltpu.VMEM((DIM, Q_PAD), BF16),
            pltpu.VMEM((ROWS, DIM), BF16),
            pltpu.VMEM((DIM, ROWS), BF16),
            pltpu.VMEM((DIM, Q_PAD), BF16),
            pltpu.SemaphoreType.DMA((4,)),
            pltpu.SemaphoreType.DMA((LAYERS * 4,)),
            pltpu.SemaphoreType.DMA((SP - 1,)),
            pltpu.SemaphoreType.DMA((SP - 1,)),
            pltpu.SemaphoreType.DMA((5,)),
            pltpu.SemaphoreType.DMA((5,)),
            pltpu.SemaphoreType.DMA((3,)),
            pltpu.SemaphoreType.DMA((3,)),
            pltpu.SemaphoreType.DMA((LAYERS,)),
            pltpu.SemaphoreType.DMA((LAYERS,)),
        ],
        compiler_params=pltpu.CompilerParams(collective_id=0, has_side_effects=True, vmem_limit_bytes=58 * 2 ** 20),
        cost_estimate=pl.CostEstimate(flops=12 * 10 ** 9, bytes_accessed=4 * 10 ** 7, transcendentals=0),
        name='encoder',
    )(mask, bpe, token, patches, enc_pos, wpe, dec_pos, wed, qkv_t, proj, up, down)


Q_BLK = 512
K_BLK = 256
CHUNK = 256
WIDE = 512
PAIR = 2 * HEAD


def fill_rows(start, count, step, body):
    def run(i, carry):
        body(pl.ds(pl.multiple_of(start + i * step, step), step))
        return carry

    lax.fori_loop(0, count // step, run, 0)


def make_queries(rows, norm, w_q, q_3):
    q = dot_nt(w_q, norm[rows, :]).astype(BF16).astype(F32) * EXP_SCALE
    hi = q.astype(BF16)
    rest = q - hi.astype(F32)
    mid = rest.astype(BF16)
    low = (rest - mid.astype(F32)).astype(BF16)
    zero = jnp.zeros((HEAD, q.shape[1]), BF16)
    for head in range(DEC_HEADS):
        part = slice(head * HEAD, (head + 1) * HEAD)
        tail = (low[part], zero) if head % 2 == 0 else (zero, low[part])
        for idx, val in enumerate((hi[part], mid[part]) + tail):
            q_3[head, idx * HEAD:(idx + 1) * HEAD, rows] = val


def make_keys(rows, norm, w_k, w_v, k_n, k_dup, v_t):
    a = norm[rows, :]
    k = dot_nt(a, w_k)
    first = lax.broadcasted_iota(jnp.int32, (k.shape[0], PAIR), 1) < HEAD
    for pair in range(DEC_HEADS // 2):
        both = k[:, pair * PAIR:(pair + 1) * PAIR]
        turned = pltpu.roll(both, HEAD, axis=1)
        k_n[pair, rows, :] = both.astype(BF16)
        k_dup[2 * pair, rows, :] = jnp.where(first, both, turned).astype(BF16)
        k_dup[2 * pair + 1, rows, :] = jnp.where(first, turned, both).astype(BF16)
    v_t[:, rows] = dot_nt(w_v, a).astype(BF16)


def attention(start, count, q_3, k_n, k_dup, v_t, o_t, s_even, s_odd, first=None, follow=None):
    blocks = count // Q_BLK
    units = DEC_HEADS * blocks

    def place(unit):
        head = unit // blocks
        offset = start + (unit - head * blocks) * Q_BLK
        if follow is not None:
            past = unit >= units
            head = jnp.where(past, 0, head)
            offset = jnp.where(past, follow, offset)
        return head, pl.ds(pl.multiple_of(offset, Q_BLK), Q_BLK)

    def mixed(unit_q, s_q, unit_p, s_p, max8):
        if unit_q is not None:
            head_q, cols_q = place(unit_q)
            q = q_3[head_q, :, cols_q]
        if unit_p is not None:
            head_p, cols_p = place(unit_p)
            shift = col_max(max8)
            v_rows = pl.ds(pl.multiple_of(head_p * HEAD, HEAD), HEAD)
        new_max = total = late = None
        accs = [None, None]

        def weigh(idx, weights):
            o = dot(v_t[v_rows, idx * K_BLK:(idx + 1) * K_BLK], weights)
            accs[idx % 2] = o if accs[idx % 2] is None else accs[idx % 2] + o

        for idx in range(SEQ // K_BLK):
            rows = slice(idx * K_BLK, (idx + 1) * K_BLK)
            if unit_p is not None:
                e = jnp.exp2(s_p[rows, :] - shift)
                t = jnp.sum(e.reshape(K_BLK // 8, 8, Q_BLK), axis=0)
                total = t if total is None else total + t
                if late is not None:
                    weigh(*late)
                late = (idx, e.astype(BF16))
            if unit_q is not None:
                keys = jnp.concatenate([k_dup[head_q, rows, :], k_n[head_q // 2, rows, :]], axis=1)
                s = dot(keys, q)
                s_q[rows, :] = s
                m = jnp.max(s.reshape(K_BLK // 8, 8, Q_BLK), axis=0)
                new_max = m if new_max is None else jnp.maximum(new_max, m)
        if unit_p is not None:
            weigh(*late)
            o_t[v_rows, cols_p] = ((accs[0] + accs[1]) * (1.0 / col_sum(total))).astype(BF16)
        return new_max

    if first is None:
        first = mixed(0, s_even, None, None, None)

    def body(i, max8):
        unit = 2 * i
        max_odd = mixed(unit + 1, s_odd, unit, s_even, max8)
        following = unit + 2 if follow is not None else jnp.minimum(unit + 2, units - 1)
        return mixed(following, s_even, unit + 1, s_odd, max_odd)

    return lax.fori_loop(0, units // 2, body, first)


def mlp(rows, hid, o_t, w_proj, w_up, w_down):
    mid = (hid[rows, :].astype(F32) + dot_tn(o_t[:, rows], w_proj)).astype(BF16)
    act = gelu(dot(layer_norm(mid), w_up))
    return (mid.astype(F32) + dot(act, w_down)).astype(BF16)


def decoder_kernel(z_ref, rank_ref, pos_me, pos_x, qkv_hbm, proj_hbm, up_hbm, down_hbm, both_ref,
                   qkv, proj, up, down, hid, norm, fin, q_3, k_n, k_dup, v_t, o_t, s_even, s_odd, w_sem, ready, row_send, row_recv, fin_send, fin_recv, pos, pos_sem):
    me = lax.axis_index('sp')
    chip = me // 2
    core = me - 2 * chip
    peer = lax.rem(me + 2, SP)
    sib = me + 1 - 2 * core
    diag = lax.rem(sib + 2, SP)

    fetch = [pltpu.make_async_copy(src, pos.at[idx], pos_sem.at[idx])
             for idx, src in enumerate((pos_me, pos_x.at[0], pos_x.at[1], pos_x.at[2]))]
    for copy in fetch:
        copy.start()
    copies = []
    for layer in range(LAYERS):
        for idx, (src, dst) in enumerate(((qkv_hbm, qkv), (proj_hbm, proj), (up_hbm, up), (down_hbm, down))):
            copy = pltpu.make_async_copy(src.at[layer], dst.at[layer], w_sem.at[layer * 4 + idx])
            copy.start()
            copies.append(copy)
    barrier = pltpu.get_barrier_semaphore()
    for other in (peer, sib):
        pl.semaphore_signal(barrier, inc=1, device_id={'sp': other}, device_id_type=MESH)
    pl.semaphore_wait(barrier, 2)

    def tokens(dev, idx):
        slot = lax.rem(me - dev + SP, SP)
        rank = rank_ref[pl.ds(2 * slot + chip, 1), :]
        rank_col = jnp.transpose(jnp.broadcast_to(rank.astype(F32), (8, TOK)))[:, 0:1]
        lanes = lax.broadcasted_iota(jnp.int32, (TOK, ROWS + 2 * HEAD), 1).astype(F32)
        select = jnp.where(lanes == rank_col, 1.0, 0.0).astype(BF16)
        fetch[idx].wait()
        return (dot(select, z_ref[...]) + pos[idx].astype(F32)).astype(BF16)

    hid[0:TOK] = tokens(peer, 1)
    hid[TOK:OWN] = tokens(me, 0)
    norm[OWN:OWN + TOK] = layer_norm(tokens(diag, 3))
    norm[OWN + TOK:SEQ] = layer_norm(tokens(sib, 2))

    def own_norm(rows):
        norm[rows, :] = layer_norm(hid[rows, :])

    fill_rows(0, OWN, CHUNK, own_norm)

    def queries(layer):
        fill_rows(0, OWN, WIDE, lambda rows: make_queries(rows, norm, qkv[layer, 0:DDIM], q_3))

    def keys(layer, start, count):
        fill_rows(start, count, WIDE, lambda rows: make_keys(
            rows, norm, qkv[layer, DDIM:2 * DDIM], qkv[layer, 2 * DDIM:3 * DDIM], k_n, k_dup, v_t))

    copies[0].wait()
    queries(0)
    keys(0, 0, SEQ)
    pl.semaphore_signal(ready, inc=1, device_id={'sp': sib}, device_id_type=MESH)
    attention(0, OWN, q_3, k_n, k_dup, v_t, o_t, s_even, s_odd)
    pl.semaphore_wait(ready, 1)
    for copy in copies[1:]:
        copy.wait()
    steps = OWN // CHUNK

    def row_copy(i):
        src = pl.ds(pl.multiple_of(i * CHUNK, CHUNK), CHUNK)
        dst = pl.ds(pl.multiple_of(OWN + i * CHUNK, CHUNK), CHUNK)
        return pltpu.make_async_remote_copy(
            src_ref=norm.at[src], dst_ref=norm.at[dst], send_sem=row_send.at[i], recv_sem=row_recv.at[i],
            device_id={'sp': sib}, device_id_type=MESH)

    def first_mlp(i, carry):
        rows = pl.ds(pl.multiple_of(i * CHUNK, CHUNK), CHUNK)
        val = mlp(rows, hid, o_t, proj[0], up[0], down[0])
        hid[rows, :] = val
        norm[rows, :] = layer_norm(val)

        @pl.when(i > 0)
        def _():
            row_copy(i - 1).start()

        return carry

    lax.fori_loop(0, steps, first_mlp, 0)
    queries(1)
    row_copy(steps - 1).start()
    keys(1, 0, OWN)
    for i in range(steps):
        row_copy(i).wait()
    keys(1, OWN, OWN)

    early = 2 * Q_BLK
    scored = attention(0, early, q_3, k_n, k_dup, v_t, o_t, s_even, s_odd, follow=early)
    pieces = TOK // CHUNK

    def fin_copy(i):
        rows = pl.ds(pl.multiple_of(i * CHUNK, CHUNK), CHUNK)
        return pltpu.make_async_remote_copy(
            src_ref=fin.at[rows], dst_ref=both_ref.at[chip, rows], send_sem=fin_send.at[i], recv_sem=fin_recv.at[i],
            device_id={'sp': peer}, device_id_type=MESH)

    def last_mlp(i, carry, start):
        src = pl.ds(pl.multiple_of(start + i * CHUNK, CHUNK), CHUNK)
        rows = pl.ds(pl.multiple_of(i * CHUNK, CHUNK), CHUNK)
        val = layer_norm(mlp(src, hid, o_t, proj[1], up[1], down[1]))
        if start == 0:
            fin[rows, :] = val

            @pl.when(i > 0)
            def _():
                fin_copy(i - 1).start()
        else:
            both_ref[chip, rows, :] = val
        return carry

    lax.fori_loop(0, pieces, functools.partial(last_mlp, start=0), 0)
    fin_copy(pieces - 1).start()
    attention(early, OWN - early, q_3, k_n, k_dup, v_t, o_t, s_even, s_odd, first=scored)
    lax.fori_loop(0, pieces, functools.partial(last_mlp, start=TOK), 0)
    for i in range(pieces):
        fin_copy(i).wait()


def decode(z, rank, pos, pos_x, wqkv, wproj, wup, wdown):
    return pl.pallas_call(
        decoder_kernel,
        out_shape=jax.ShapeDtypeStruct((CLIPS, TOK, DDIM), BF16),
        in_specs=[VMEM] * 2 + [ANY] * 6,
        out_specs=VMEM,
        scratch_shapes=[
            pltpu.VMEM((LAYERS, 3 * DDIM, DDIM), BF16),
            pltpu.VMEM((LAYERS, DDIM, DDIM), BF16),
            pltpu.VMEM((LAYERS, DDIM, 4 * DDIM), BF16),
            pltpu.VMEM((LAYERS, 4 * DDIM, DDIM), BF16),
            pltpu.VMEM((OWN, DDIM), BF16),
            pltpu.VMEM((SEQ, DDIM), BF16),
            pltpu.VMEM((TOK, DDIM), BF16),
            pltpu.VMEM((DEC_HEADS, 4 * HEAD, OWN), BF16),
            pltpu.VMEM((DEC_HEADS // 2, SEQ, PAIR), BF16),
            pltpu.VMEM((DEC_HEADS, SEQ, PAIR), BF16),
            pltpu.VMEM((DDIM, SEQ), BF16),
            pltpu.VMEM((DDIM, OWN), BF16),
            pltpu.VMEM((SEQ, Q_BLK), F32),
            pltpu.VMEM((SEQ, Q_BLK), F32),
            pltpu.SemaphoreType.DMA((LAYERS * 4,)),
            pltpu.SemaphoreType.REGULAR,
            pltpu.SemaphoreType.DMA((OWN // CHUNK,)),
            pltpu.SemaphoreType.DMA((OWN // CHUNK,)),
            pltpu.SemaphoreType.DMA((TOK // CHUNK,)),
            pltpu.SemaphoreType.DMA((TOK // CHUNK,)),
            pltpu.VMEM((SP, TOK, DDIM), BF16),
            pltpu.SemaphoreType.DMA((SP,)),
        ],
        compiler_params=pltpu.CompilerParams(collective_id=1, has_side_effects=True, vmem_limit_bytes=58 * 2 ** 20),
        cost_estimate=pl.CostEstimate(flops=60 * 10 ** 9, bytes_accessed=2 * 10 ** 7, transcendentals=6 * 10 ** 7),
        name='decoder',
    )(z, rank, pos, pos_x, wqkv, wproj, wup, wdown)


def output_kernel(both_ref, w_ref, out_hbm, buf, sem):
    pieces = TOK // CHUNK

    def out_copy(i):
        clip = i // pieces
        rows = pl.ds(pl.multiple_of((i - clip * pieces) * CHUNK, CHUNK), CHUNK)
        return pltpu.make_async_copy(buf.at[i], out_hbm.at[clip, rows], sem.at[i])

    def body(i, carry):
        clip = i // pieces
        rows = pl.ds(pl.multiple_of((i - clip * pieces) * CHUNK, CHUNK), CHUNK)
        buf[i] = dot(both_ref[clip, rows, :], w_ref[...])
        out_copy(i).start()
        return carry

    lax.fori_loop(0, CLIPS * pieces, body, 0)
    for i in range(CLIPS * pieces):
        out_copy(i).wait()


def project(both, w_out):
    return pl.pallas_call(
        output_kernel,
        out_shape=jax.ShapeDtypeStruct((CLIPS, TOK, PATCH), F32),
        in_specs=[VMEM] * 2,
        out_specs=ANY,
        scratch_shapes=[
            pltpu.VMEM((CLIPS * TOK // CHUNK, CHUNK, PATCH), F32),
            pltpu.SemaphoreType.DMA((CLIPS * TOK // CHUNK,)),
        ],
        compiler_params=pltpu.CompilerParams(vmem_limit_bytes=62 * 2 ** 20),
        cost_estimate=pl.CostEstimate(flops=2 * 10 ** 9, bytes_accessed=12 * 10 ** 6, transcendentals=0),
        name='output',
    )(both, w_out)


def solution(mesh):
    def local_program(patches, vis_mask, enc_pos, dec_pos, w_pe, b_pe, enc_qkv, enc_proj, enc_up, enc_down, w_ed, mask_token, dec_qkv, dec_proj, dec_up, dec_down, w_out):
        enc_qkv_t = jnp.transpose(enc_qkv, (0, 2, 3, 4, 1)).reshape(LAYERS, 3 * DIM, DIM)
        dec_qkv_t = jnp.transpose(dec_qkv, (0, 2, 3, 4, 1)).reshape(LAYERS, 3 * DDIM, DDIM)
        enc_proj2 = enc_proj.reshape(LAYERS, DIM, DIM)
        dec_proj2 = dec_proj.reshape(LAYERS, DDIM, DDIM)
        z, rank, pos_x = encode(vis_mask, b_pe, mask_token, patches, enc_pos, w_pe, dec_pos, w_ed,
                                enc_qkv_t, enc_proj2, enc_up, enc_down)
        both = decode(z, rank, dec_pos, pos_x, dec_qkv_t, dec_proj2, dec_up, dec_down)
        return project(both, w_out)

    row_spec = P('dp', 'sp', None)
    pos_spec = P(('dp', 'sp'), None)
    arg_specs = (row_spec, P('dp', 'sp'), pos_spec, pos_spec) + (P(),) * 13
    return jax.shard_map(local_program, mesh=mesh, in_specs=arg_specs, out_specs=row_spec, check_vma=False)
```

```python
import functools
import math

import jax
import jax.numpy as jnp
from jax import lax
from jax.experimental import pallas as pl
from jax.experimental.pallas import tpu as pltpu
from jax.sharding import PartitionSpec as P

F32 = jnp.float32
BF16 = jnp.bfloat16
MESH = pl.DeviceIdType.MESH
VMEM = pl.BlockSpec(memory_space=pltpu.VMEM)
ANY = pl.BlockSpec(memory_space=pl.ANY)

SP = 4
CLIPS = 2
TOK = 768
PATCH = 1536
DIM = 768
ENC_HEADS = 12
HEAD = 64
DDIM = 384
DEC_HEADS = 6
VIS = 96
WIN = 2 * VIS
ROWS = SP * VIS
OWN = 2 * TOK
SEQ = SP * TOK
LAYERS = 2
EXP_SCALE = HEAD ** -0.5 * math.log2(math.e)


def dot(lhs, rhs):
    return jnp.dot(lhs, rhs, preferred_element_type=F32)


def dot_nt(lhs, rhs):
    return lax.dot_general(lhs, rhs, (((1,), (1,)), ((), ())), preferred_element_type=F32)


def dot_tn(lhs, rhs):
    return lax.dot_general(lhs, rhs, (((0,), (0,)), ((), ())), preferred_element_type=F32)


def layer_norm(hidden):
    hid = hidden.astype(F32)
    centred = hid - jnp.mean(hid, axis=-1, keepdims=True)
    var = jnp.mean(centred * centred, axis=-1, keepdims=True)
    return (centred * lax.rsqrt(var + 1e-6)).astype(BF16)


def gelu(val):
    return (0.5 * val * (1.0 + lax.erf(val * math.sqrt(0.5)))).astype(BF16)


def col_max(val):
    return jnp.max(val, axis=0, keepdims=True)


def col_sum(val):
    return jnp.sum(val, axis=0, keepdims=True)


MINE = ROWS // 2
Q_PAD = 256


def encoder_kernel(mask_ref, bpe_ref, token_ref, patch_hbm, pos_hbm, wpe_hbm, dec_pos_hbm, wed_ref, qkv_hbm, proj_hbm, up_hbm, down_hbm,
                   z_ref, rank_ref, pos_out,
                   patch, pos, wpe, qkv, proj, up, down, masks, sendbuf, win, hall, hid, norm, norm_q, q_t, k_n, v_t, o_t,
                   in_sem, w_sem, mask_send, mask_recv, win_send, win_recv, pos_send, pos_recv, row_send, row_recv):
    me = lax.axis_index('sp')
    chip = me // 2
    core = me - 2 * chip
    peer = lax.rem(me + 2, SP)
    sib = me + 1 - 2 * core
    diag = lax.rem(sib + 2, SP)

    near_load = pltpu.make_async_copy(patch_hbm.at[chip], patch.at[chip], in_sem.at[3])
    loads = [pltpu.make_async_copy(src, dst, in_sem.at[idx])
             for idx, (src, dst) in enumerate(((patch_hbm.at[1 - chip], patch.at[1 - chip]), (wpe_hbm, wpe), (pos_hbm, pos)))]
    for copy in loads:
        copy.start()
    barrier = pltpu.get_barrier_semaphore()
    for other in (peer, sib, diag):
        pl.semaphore_signal(barrier, inc=1, device_id={'sp': other}, device_id_type=MESH)
    order_row = lax.broadcasted_iota(jnp.int32, (TOK, TOK), 0)
    order_col = lax.broadcasted_iota(jnp.int32, (TOK, TOK), 1)
    before = jnp.where(order_row < order_col, 1.0, 0.0).astype(BF16)
    mine = mask_ref[...].astype(F32)
    mine_rank = dot(jnp.concatenate([mine] * SP, axis=0).astype(BF16), before)[0:CLIPS]
    slot_of = jnp.where(mine > 0.0, mine_rank, -1.0)
    pl.semaphore_wait(barrier, 3)

    def send(src, dst, send_sem, recv_sem, dev):
        copy = pltpu.make_async_remote_copy(
            src_ref=src, dst_ref=dst, send_sem=send_sem, recv_sem=recv_sem, device_id={'sp': dev}, device_id_type=MESH)
        copy.start()
        return copy

    mask_copies = [send(mask_ref, masks.at[step - 1], mask_send.at[step - 1], mask_recv.at[step - 1], lax.rem(me + step, SP))
                   for step in range(1, SP)]
    for copy in loads:
        copy.wait()
    near_load.start()
    copies = []
    for layer in range(LAYERS):
        for idx, (src, dst) in enumerate(((qkv_hbm, qkv), (proj_hbm, proj), (up_hbm, up), (down_hbm, down))):
            copy = pltpu.make_async_copy(src.at[layer], dst.at[layer], w_sem.at[layer * 4 + idx])
            copy.start()
            copies.append(copy)

    bias = bpe_ref[...].astype(F32).reshape(1, DIM)

    def window(clip, slots, low, count):
        rows = (lax.broadcasted_iota(jnp.int32, (count, TOK), 0) + low).astype(F32)
        hit = jnp.where(rows == slots, 1.0, 0.0)
        select = hit.astype(BF16)
        moved = dot(select, patch[clip]).astype(BF16)
        occupied = jnp.sum(hit, axis=1, keepdims=True)
        emb = dot(moved, wpe[...]) + occupied * bias + dot(select, pos[...])
        return emb.astype(BF16)

    far = jnp.where(chip == 0, slot_of[1:2], slot_of[0:1])
    near = jnp.where(chip == 0, slot_of[0:1], slot_of[1:2])
    halves = [pl.ds(0, VIS), pl.ds(VIS, VIS)]
    to_peer = []
    for idx, part in enumerate(halves):
        sendbuf[idx * VIS:(idx + 1) * VIS] = window(1 - chip, far, idx * VIS, VIS)
        to_peer.append(send(sendbuf.at[part], win.at[1, part], win_send.at[idx], win_recv.at[idx], peer))
    near_load.wait()
    win[0] = window(chip, near, 0, WIN)
    to_sib = send(win.at[0], win.at[2], win_send.at[2], win_recv.at[2], sib)

    for copy in mask_copies:
        copy.wait()
    stacked = jnp.concatenate([mine] + [masks[k].astype(F32) for k in range(SP - 1)], axis=0)
    local = dot(stacked.astype(BF16), before)
    counts = jnp.sum(stacked, axis=1, keepdims=True)
    row_dev = lax.rem(me - lax.broadcasted_iota(jnp.int32, (CLIPS * SP, 1), 0) // CLIPS + SP, SP)
    base = jnp.zeros((CLIPS * SP, 1), F32)
    for k in range(SP):
        dev_k = lax.rem(me - k + SP, SP)
        tiled = jnp.concatenate([counts[CLIPS * k:CLIPS * k + CLIPS]] * SP, axis=0)
        base = base + jnp.where(dev_k < row_dev, tiled, 0.0)
    rank_ref[...] = jnp.where(stacked > 0.0, local + base, float(ROWS)).astype(jnp.int32)

    def placement(slot):
        def pick(val):
            two = val[CLIPS * slot:CLIPS * slot + CLIPS]
            return jnp.where(chip == 0, two[0:1], two[1:2])

        start, size = pick(base), pick(counts)
        rows = lax.broadcasted_iota(jnp.int32, (ROWS, WIN), 0).astype(F32)
        cols = lax.broadcasted_iota(jnp.int32, (ROWS, WIN), 1).astype(F32)
        return jnp.where((rows == cols + start) & (cols < size), 1.0, 0.0)

    even = core == 0
    left, right = placement(1), placement(3)
    place = [placement(0), placement(2), jnp.where(even, right, left), jnp.where(even, left, right)]
    relay = []
    for idx, part in enumerate(halves):
        to_peer[idx].wait_recv()
        relay.append(send(win.at[1, part], win.at[3, part], win_send.at[3 + idx], win_recv.at[3 + idx], sib))
    pos_peer = send(dec_pos_hbm, pos_out.at[0], pos_send.at[0], pos_recv.at[0], peer)
    pos_sib = send(dec_pos_hbm, pos_out.at[1], pos_send.at[1], pos_recv.at[1], sib)
    total = dot(place[0].astype(BF16), win[0]) + dot(place[1].astype(BF16), win[1])
    to_sib.wait_recv()
    total = total + dot(place[2].astype(BF16), win[2])
    for copy in relay:
        copy.wait_recv()
    total = total + dot(place[3].astype(BF16), win[3])
    hall[...] = total.astype(BF16)
    own = pl.ds(pl.multiple_of(core * MINE, MINE), MINE)
    hid[...] = hall[own, :]
    norm[0] = layer_norm(hall[...])
    norm_q[MINE:] = jnp.zeros((Q_PAD - MINE, DIM), BF16)
    zero = jnp.zeros((HEAD, Q_PAD), BF16)
    pos_diag = swap = None

    for layer in range(LAYERS):
        copies[layer * 4].wait()
        norm_q[0:MINE] = norm[layer, own, :]
        q_t[...] = dot_nt(qkv[layer, 0:DIM], norm_q[...]).astype(BF16)
        if swap is not None:
            swap.wait()
        k_n[...] = dot_nt(norm[layer], qkv[layer, DIM:2 * DIM]).astype(BF16)
        v_t[...] = dot_nt(qkv[layer, 2 * DIM:3 * DIM], norm[layer]).astype(BF16)

        def heads(group, carry):
            scores, weights = [], []
            for pair in range(2):
                lanes = pl.ds(pl.multiple_of((2 * group + pair) * 2 * HEAD, 2 * HEAD), 2 * HEAD)
                for odd in range(2):
                    rows = pl.ds(pl.multiple_of((4 * group + 2 * pair + odd) * HEAD, HEAD), HEAD)
                    q_head = q_t[rows, :]
                    q_both = jnp.concatenate([zero, q_head] if odd else [q_head, zero], axis=0)
                    scores.append(dot(k_n[:, lanes], q_both))
            for s in scores:
                e = jnp.exp2(s * EXP_SCALE - col_max(s) * EXP_SCALE)
                weights.append((e.astype(BF16), 1.0 / col_sum(e)))
            for idx, (e, scale) in enumerate(weights):
                rows = pl.ds(pl.multiple_of((4 * group + idx) * HEAD, HEAD), HEAD)
                o_t[rows, :] = (dot(v_t[rows, :], e) * scale).astype(BF16)
            return carry

        lax.fori_loop(0, ENC_HEADS // 4, heads, 0)
        copies[layer * 4 + 1].wait()
        mid = (hid[...].astype(F32) + dot_tn(o_t[...], proj[layer])[0:MINE]).astype(BF16)
        rows_norm = layer_norm(mid)
        copies[layer * 4 + 2].wait()
        copies[layer * 4 + 3].wait()
        if layer == LAYERS - 1:
            pos_peer.wait_recv()
            pos_diag = send(pos_out.at[0], pos_out.at[2], pos_send.at[2], pos_recv.at[2], sib)
        acc = None
        for lo in range(0, 4 * DIM, DIM):
            act = gelu(dot(rows_norm, up[layer, :, lo:lo + DIM]))
            part = dot(act, down[layer, lo:lo + DIM, :])
            acc = part if acc is None else acc + part
        out = (mid.astype(F32) + acc).astype(BF16)
        if layer < LAYERS - 1:
            hid[...] = out
            norm[layer + 1, own, :] = layer_norm(out)
            swap = send(norm.at[layer + 1, own], norm.at[layer + 1, own], row_send.at[layer], row_recv.at[layer], sib)
    z_ref[own, :] = dot(layer_norm(out), wed_ref[...]).astype(BF16)
    first = lax.broadcasted_iota(jnp.int32, (2 * HEAD, DDIM), 0) == 0
    z_ref[ROWS:] = jnp.where(first, token_ref[...].astype(F32).reshape(1, DDIM), 0.0).astype(BF16)
    last = send(z_ref.at[own], z_ref.at[own], row_send.at[LAYERS - 1], row_recv.at[LAYERS - 1], sib)
    for copy in (*to_peer, to_sib, *relay):
        copy.wait_send()
    pos_peer.wait_send()
    pos_sib.wait()
    pos_diag.wait()
    last.wait()


def encode(mask, bpe, token, patches, enc_pos, wpe, dec_pos, wed, qkv_t, proj, up, down):
    return pl.pallas_call(
        encoder_kernel,
        out_shape=(
            jax.ShapeDtypeStruct((ROWS + 2 * HEAD, DDIM), BF16),
            jax.ShapeDtypeStruct((CLIPS * SP, TOK), jnp.int32),
            jax.ShapeDtypeStruct((SP - 1, TOK, DDIM), BF16),
        ),
        in_specs=[VMEM] * 3 + [ANY] * 4 + [VMEM] + [ANY] * 4,
        out_specs=(VMEM, VMEM, ANY),
        scratch_shapes=[
            pltpu.VMEM((CLIPS, TOK, PATCH), BF16),
            pltpu.VMEM((TOK, DIM), BF16),
            pltpu.VMEM((PATCH, DIM), BF16),
            pltpu.VMEM((LAYERS, 3 * DIM, DIM), BF16),
            pltpu.VMEM((LAYERS, DIM, DIM), BF16),
            pltpu.VMEM((LAYERS, DIM, 4 * DIM), BF16),
            pltpu.VMEM((LAYERS, 4 * DIM, DIM), BF16),
            pltpu.VMEM((SP - 1, CLIPS, TOK), jnp.int32),
            pltpu.VMEM((WIN, DIM), BF16),
            pltpu.VMEM((SP, WIN, DIM), BF16),
            pltpu.VMEM((ROWS, DIM), BF16),
            pltpu.VMEM((MINE, DIM), BF16),
            pltpu.VMEM((LAYERS, ROWS, DIM), BF16),
            pltpu.VMEM((Q_PAD, DIM), BF16),
            pltpu.VMEM((DIM, Q_PAD), BF16),
            pltpu.VMEM((ROWS, DIM), BF16),
            pltpu.VMEM((DIM, ROWS), BF16),
            pltpu.VMEM((DIM, Q_PAD), BF16),
            pltpu.SemaphoreType.DMA((4,)),
            pltpu.SemaphoreType.DMA((LAYERS * 4,)),
            pltpu.SemaphoreType.DMA((SP - 1,)),
            pltpu.SemaphoreType.DMA((SP - 1,)),
            pltpu.SemaphoreType.DMA((5,)),
            pltpu.SemaphoreType.DMA((5,)),
            pltpu.SemaphoreType.DMA((3,)),
            pltpu.SemaphoreType.DMA((3,)),
            pltpu.SemaphoreType.DMA((LAYERS,)),
            pltpu.SemaphoreType.DMA((LAYERS,)),
        ],
        compiler_params=pltpu.CompilerParams(collective_id=0, has_side_effects=True, vmem_limit_bytes=58 * 2 ** 20),
        cost_estimate=pl.CostEstimate(flops=12 * 10 ** 9, bytes_accessed=4 * 10 ** 7, transcendentals=0),
        name='encoder',
    )(mask, bpe, token, patches, enc_pos, wpe, dec_pos, wed, qkv_t, proj, up, down)


Q_BLK = 512
K_BLK = 256
CHUNK = 256
WIDE = 512
PAIR = 2 * HEAD


def fill_rows(start, count, step, body):
    def run(i, carry):
        body(pl.ds(pl.multiple_of(start + i * step, step), step))
        return carry

    lax.fori_loop(0, count // step, run, 0)


def make_queries(rows, norm, w_q, q_3):
    q = dot_nt(w_q, norm[rows, :]).astype(BF16).astype(F32) * EXP_SCALE
    hi = q.astype(BF16)
    rest = q - hi.astype(F32)
    mid = rest.astype(BF16)
    low = (rest - mid.astype(F32)).astype(BF16)
    zero = jnp.zeros((HEAD, q.shape[1]), BF16)
    for head in range(DEC_HEADS):
        part = slice(head * HEAD, (head + 1) * HEAD)
        tail = (low[part], zero) if head % 2 == 0 else (zero, low[part])
        for idx, val in enumerate((hi[part], mid[part]) + tail):
            q_3[head, idx * HEAD:(idx + 1) * HEAD, rows] = val


def make_keys(rows, norm, w_k, w_v, k_n, k_dup, v_t):
    a = norm[rows, :]
    k = dot_nt(a, w_k)
    first = lax.broadcasted_iota(jnp.int32, (k.shape[0], PAIR), 1) < HEAD
    for pair in range(DEC_HEADS // 2):
        both = k[:, pair * PAIR:(pair + 1) * PAIR]
        turned = pltpu.roll(both, HEAD, axis=1)
        k_n[pair, rows, :] = both.astype(BF16)
        k_dup[2 * pair, rows, :] = jnp.where(first, both, turned).astype(BF16)
        k_dup[2 * pair + 1, rows, :] = jnp.where(first, turned, both).astype(BF16)
    v_t[:, rows] = dot_nt(w_v, a).astype(BF16)


def attention(start, count, q_3, k_n, k_dup, v_t, o_t, s_even, s_odd, first=None, follow=None):
    blocks = count // Q_BLK
    units = DEC_HEADS * blocks

    def place(unit):
        head = unit // blocks
        offset = start + (unit - head * blocks) * Q_BLK
        if follow is not None:
            past = unit >= units
            head = jnp.where(past, 0, head)
            offset = jnp.where(past, follow, offset)
        return head, pl.ds(pl.multiple_of(offset, Q_BLK), Q_BLK)

    def mixed(unit_q, s_q, unit_p, s_p, max8):
        if unit_q is not None:
            head_q, cols_q = place(unit_q)
            q = q_3[head_q, :, cols_q]
        if unit_p is not None:
            head_p, cols_p = place(unit_p)
            shift = col_max(max8)
            v_rows = pl.ds(pl.multiple_of(head_p * HEAD, HEAD), HEAD)
        new_max = total = late = None
        accs = [None, None]

        def weigh(idx, weights):
            o = dot(v_t[v_rows, idx * K_BLK:(idx + 1) * K_BLK], weights)
            accs[idx % 2] = o if accs[idx % 2] is None else accs[idx % 2] + o

        for idx in range(SEQ // K_BLK):
            rows = slice(idx * K_BLK, (idx + 1) * K_BLK)
            if unit_p is not None:
                e = jnp.exp2(s_p[rows, :] - shift)
                t = jnp.sum(e.reshape(K_BLK // 8, 8, Q_BLK), axis=0)
                total = t if total is None else total + t
                if late is not None:
                    weigh(*late)
                late = (idx, e.astype(BF16))
            if unit_q is not None:
                keys = jnp.concatenate([k_dup[head_q, rows, :], k_n[head_q // 2, rows, :]], axis=1)
                s = dot(keys, q)
                s_q[rows, :] = s
                m = jnp.max(s.reshape(K_BLK // 8, 8, Q_BLK), axis=0)
                new_max = m if new_max is None else jnp.maximum(new_max, m)
        if unit_p is not None:
            weigh(*late)
            o_t[v_rows, cols_p] = ((accs[0] + accs[1]) * (1.0 / col_sum(total))).astype(BF16)
        return new_max

    if first is None:
        first = mixed(0, s_even, None, None, None)

    def body(i, max8):
        unit = 2 * i
        max_odd = mixed(unit + 1, s_odd, unit, s_even, max8)
        following = unit + 2 if follow is not None else jnp.minimum(unit + 2, units - 1)
        return mixed(following, s_even, unit + 1, s_odd, max_odd)

    return lax.fori_loop(0, units // 2, body, first)


def mlp(rows, hid, o_t, w_proj, w_up, w_down):
    mid = (hid[rows, :].astype(F32) + dot_tn(o_t[:, rows], w_proj)).astype(BF16)
    act = gelu(dot(layer_norm(mid), w_up))
    return (mid.astype(F32) + dot(act, w_down)).astype(BF16)


def decoder_kernel(z_ref, rank_ref, pos_me, pos_x, qkv_hbm, proj_hbm, up_hbm, down_hbm, both_ref,
                   qkv, proj, up, down, hid, norm, fin, q_3, k_n, k_dup, v_t, o_t, s_even, s_odd, w_sem, ready, row_send, row_recv, fin_send, fin_recv, pos, pos_sem):
    me = lax.axis_index('sp')
    chip = me // 2
    core = me - 2 * chip
    peer = lax.rem(me + 2, SP)
    sib = me + 1 - 2 * core
    diag = lax.rem(sib + 2, SP)

    fetch = [pltpu.make_async_copy(src, pos.at[idx], pos_sem.at[idx])
             for idx, src in enumerate((pos_me, pos_x.at[0], pos_x.at[1], pos_x.at[2]))]
    for copy in fetch:
        copy.start()
    copies = []
    for layer in range(LAYERS):
        for idx, (src, dst) in enumerate(((qkv_hbm, qkv), (proj_hbm, proj), (up_hbm, up), (down_hbm, down))):
            copy = pltpu.make_async_copy(src.at[layer], dst.at[layer], w_sem.at[layer * 4 + idx])
            copy.start()
            copies.append(copy)
    barrier = pltpu.get_barrier_semaphore()
    for other in (peer, sib):
        pl.semaphore_signal(barrier, inc=1, device_id={'sp': other}, device_id_type=MESH)
    pl.semaphore_wait(barrier, 2)

    def tokens(dev, idx):
        slot = lax.rem(me - dev + SP, SP)
        rank = rank_ref[pl.ds(2 * slot + chip, 1), :]
        rank_col = jnp.transpose(jnp.broadcast_to(rank.astype(F32), (8, TOK)))[:, 0:1]
        lanes = lax.broadcasted_iota(jnp.int32, (TOK, ROWS + 2 * HEAD), 1).astype(F32)
        select = jnp.where(lanes == rank_col, 1.0, 0.0).astype(BF16)
        fetch[idx].wait()
        return (dot(select, z_ref[...]) + pos[idx].astype(F32)).astype(BF16)

    hid[0:TOK] = tokens(peer, 1)
    hid[TOK:OWN] = tokens(me, 0)
    norm[OWN:OWN + TOK] = layer_norm(tokens(diag, 3))
    norm[OWN + TOK:SEQ] = layer_norm(tokens(sib, 2))

    def own_norm(rows):
        norm[rows, :] = layer_norm(hid[rows, :])

    fill_rows(0, OWN, CHUNK, own_norm)

    def queries(layer):
        fill_rows(0, OWN, WIDE, lambda rows: make_queries(rows, norm, qkv[layer, 0:DDIM], q_3))

    def keys(layer, start, count):
        fill_rows(start, count, WIDE, lambda rows: make_keys(
            rows, norm, qkv[layer, DDIM:2 * DDIM], qkv[layer, 2 * DDIM:3 * DDIM], k_n, k_dup, v_t))

    copies[0].wait()
    queries(0)
    keys(0, 0, SEQ)
    pl.semaphore_signal(ready, inc=1, device_id={'sp': sib}, device_id_type=MESH)
    attention(0, OWN, q_3, k_n, k_dup, v_t, o_t, s_even, s_odd)
    pl.semaphore_wait(ready, 1)
    for copy in copies[1:]:
        copy.wait()
    steps = OWN // CHUNK

    def row_copy(i):
        src = pl.ds(pl.multiple_of(i * CHUNK, CHUNK), CHUNK)
        dst = pl.ds(pl.multiple_of(OWN + i * CHUNK, CHUNK), CHUNK)
        return pltpu.make_async_remote_copy(
            src_ref=norm.at[src], dst_ref=norm.at[dst], send_sem=row_send.at[i], recv_sem=row_recv.at[i],
            device_id={'sp': sib}, device_id_type=MESH)

    def first_mlp(i, carry):
        rows = pl.ds(pl.multiple_of(i * CHUNK, CHUNK), CHUNK)
        val = mlp(rows, hid, o_t, proj[0], up[0], down[0])
        hid[rows, :] = val
        norm[rows, :] = layer_norm(val)

        @pl.when(i > 0)
        def _():
            row_copy(i - 1).start()

        return carry

    lax.fori_loop(0, steps, first_mlp, 0)
    queries(1)
    row_copy(steps - 1).start()
    keys(1, 0, OWN)
    for i in range(steps):
        row_copy(i).wait()
    keys(1, OWN, OWN)

    early = 2 * Q_BLK
    scored = attention(0, early, q_3, k_n, k_dup, v_t, o_t, s_even, s_odd, follow=early)
    pieces = TOK // CHUNK

    def fin_copy(i):
        rows = pl.ds(pl.multiple_of(i * CHUNK, CHUNK), CHUNK)
        return pltpu.make_async_remote_copy(
            src_ref=fin.at[rows], dst_ref=both_ref.at[chip, rows], send_sem=fin_send.at[i], recv_sem=fin_recv.at[i],
            device_id={'sp': peer}, device_id_type=MESH)

    def last_mlp(i, carry, start):
        src = pl.ds(pl.multiple_of(start + i * CHUNK, CHUNK), CHUNK)
        rows = pl.ds(pl.multiple_of(i * CHUNK, CHUNK), CHUNK)
        val = layer_norm(mlp(src, hid, o_t, proj[1], up[1], down[1]))
        if start == 0:
            fin[rows, :] = val

            @pl.when(i > 0)
            def _():
                fin_copy(i - 1).start()
        else:
            both_ref[chip, rows, :] = val
        return carry

    lax.fori_loop(0, pieces, functools.partial(last_mlp, start=0), 0)
    fin_copy(pieces - 1).start()
    attention(early, OWN - early, q_3, k_n, k_dup, v_t, o_t, s_even, s_odd, first=scored)
    lax.fori_loop(0, pieces, functools.partial(last_mlp, start=TOK), 0)
    for i in range(pieces):
        fin_copy(i).wait()


def decode(z, rank, pos, pos_x, wqkv, wproj, wup, wdown):
    return pl.pallas_call(
        decoder_kernel,
        out_shape=jax.ShapeDtypeStruct((CLIPS, TOK, DDIM), BF16),
        in_specs=[VMEM] * 2 + [ANY] * 6,
        out_specs=VMEM,
        scratch_shapes=[
            pltpu.VMEM((LAYERS, 3 * DDIM, DDIM), BF16),
            pltpu.VMEM((LAYERS, DDIM, DDIM), BF16),
            pltpu.VMEM((LAYERS, DDIM, 4 * DDIM), BF16),
            pltpu.VMEM((LAYERS, 4 * DDIM, DDIM), BF16),
            pltpu.VMEM((OWN, DDIM), BF16),
            pltpu.VMEM((SEQ, DDIM), BF16),
            pltpu.VMEM((TOK, DDIM), BF16),
            pltpu.VMEM((DEC_HEADS, 4 * HEAD, OWN), BF16),
            pltpu.VMEM((DEC_HEADS // 2, SEQ, PAIR), BF16),
            pltpu.VMEM((DEC_HEADS, SEQ, PAIR), BF16),
            pltpu.VMEM((DDIM, SEQ), BF16),
            pltpu.VMEM((DDIM, OWN), BF16),
            pltpu.VMEM((SEQ, Q_BLK), F32),
            pltpu.VMEM((SEQ, Q_BLK), F32),
            pltpu.SemaphoreType.DMA((LAYERS * 4,)),
            pltpu.SemaphoreType.REGULAR,
            pltpu.SemaphoreType.DMA((OWN // CHUNK,)),
            pltpu.SemaphoreType.DMA((OWN // CHUNK,)),
            pltpu.SemaphoreType.DMA((TOK // CHUNK,)),
            pltpu.SemaphoreType.DMA((TOK // CHUNK,)),
            pltpu.VMEM((SP, TOK, DDIM), BF16),
            pltpu.SemaphoreType.DMA((SP,)),
        ],
        compiler_params=pltpu.CompilerParams(collective_id=1, has_side_effects=True, vmem_limit_bytes=54 * 2 ** 20),
        cost_estimate=pl.CostEstimate(flops=60 * 10 ** 9, bytes_accessed=2 * 10 ** 7, transcendentals=6 * 10 ** 7),
        name='decoder',
    )(z, rank, pos, pos_x, wqkv, wproj, wup, wdown)


def output_kernel(both_hbm, w_ref, out_hbm, both, buf, in_sem, sem):
    pieces = TOK // CHUNK

    def out_copy(i):
        clip = i // pieces
        rows = pl.ds(pl.multiple_of((i - clip * pieces) * CHUNK, CHUNK), CHUNK)
        return pltpu.make_async_copy(buf.at[i], out_hbm.at[clip, rows], sem.at[i])

    def in_copy(i):
        clip = i // pieces
        rows = pl.ds(pl.multiple_of((i - clip * pieces) * CHUNK, CHUNK), CHUNK)
        return pltpu.make_async_copy(both_hbm.at[clip, rows], both.at[i], in_sem.at[i])

    for i in range(CLIPS * pieces):
        in_copy(i).start()

    def body(i, carry):
        in_copy(i).wait()
        buf[i] = dot(both[i], w_ref[...])
        out_copy(i).start()
        return carry

    lax.fori_loop(0, CLIPS * pieces, body, 0)
    for i in range(CLIPS * pieces):
        out_copy(i).wait()


def project(both, w_out):
    return pl.pallas_call(
        output_kernel,
        out_shape=jax.ShapeDtypeStruct((CLIPS, TOK, PATCH), F32),
        in_specs=[pl.BlockSpec(memory_space=pltpu.HBM), VMEM],
        out_specs=ANY,
        scratch_shapes=[
            pltpu.VMEM((CLIPS * TOK // CHUNK, CHUNK, DDIM), BF16),
            pltpu.VMEM((CLIPS * TOK // CHUNK, CHUNK, PATCH), F32),
            pltpu.SemaphoreType.DMA((CLIPS * TOK // CHUNK,)),
            pltpu.SemaphoreType.DMA((CLIPS * TOK // CHUNK,)),
        ],
        compiler_params=pltpu.CompilerParams(vmem_limit_bytes=20 * 2 ** 20),
        cost_estimate=pl.CostEstimate(flops=2 * 10 ** 9, bytes_accessed=12 * 10 ** 6, transcendentals=0),
        name='output',
    )(both, w_out)


def solution(mesh):
    def local_program(patches, vis_mask, enc_pos, dec_pos, w_pe, b_pe, enc_qkv, enc_proj, enc_up, enc_down, w_ed, mask_token, dec_qkv, dec_proj, dec_up, dec_down, w_out):
        enc_qkv_t = jnp.transpose(enc_qkv, (0, 2, 3, 4, 1)).reshape(LAYERS, 3 * DIM, DIM)
        dec_qkv_t = jnp.transpose(dec_qkv, (0, 2, 3, 4, 1)).reshape(LAYERS, 3 * DDIM, DDIM)
        enc_proj2 = enc_proj.reshape(LAYERS, DIM, DIM)
        dec_proj2 = dec_proj.reshape(LAYERS, DDIM, DDIM)
        z, rank, pos_x = encode(vis_mask, b_pe, mask_token, patches, enc_pos, w_pe, dec_pos, w_ed,
                                enc_qkv_t, enc_proj2, enc_up, enc_down)
        both = decode(z, rank, dec_pos, pos_x, dec_qkv_t, dec_proj2, dec_up, dec_down)
        return project(both, w_out)

    row_spec = P('dp', 'sp', None)
    pos_spec = P(('dp', 'sp'), None)
    arg_specs = (row_spec, P('dp', 'sp'), pos_spec, pos_spec) + (P(),) * 13
    return jax.shard_map(local_program, mesh=mesh, in_specs=arg_specs, out_specs=row_spec, check_vma=False)
```
